32 devices in a mesh: dp: 8 (over z, x), col: 4 (over y, core).
Axes of the slice: x: 2, y: 2, z: 4, core: 2. Of those that a mesh axis runs over, the one named last changes fastest.
Arguments:
- activations: bfloat16 [2, 7168, 8192], P(None, 'dp', 'col'), may hold values from -40 to 40
- cotangent: bfloat16 [2, 7168, 2048], P(None, 'dp'), may hold values from -40 to 40
- master_weights: float32 [2, 2048, 8192], P(None, 'dp', 'col'), may hold values from -6 to 6
- moment_codes: bfloat16 [2, 2048, 8192], P(None, 'dp', 'col'), may hold values from -1 to 1
- square_codes: bfloat16 [2, 2048, 8192], P(None, 'dp', 'col'), may hold values from 0.049804688 to 1
- moment_scales: float32 [2, 2048, 4], P(None, 'dp'), may hold values from 0.05 to 0.5
- square_scales: float32 [2, 2048, 4], P(None, 'dp'), may hold values from 0.005 to 0.05
Outputs:
- new_weights: float32 [2, 2048, 8192], P(None, 'dp', 'col')
- new_moment_codes: bfloat16 [2, 2048, 8192], P(None, 'dp', 'col')
- new_square_codes: bfloat16 [2, 2048, 8192], P(None, 'dp', 'col')
- new_moment_scales: float32 [2, 2048, 4], P(None, 'dp')
- new_square_scales: float32 [2, 2048, 4], P(None, 'dp')
The draws below stay inside these ranges and needn't reach their ends.
All inputs are finite; a program needn't handle non-finite values. Where the reference program divides by a largest or mean magnitude, that divisor is 1e-20 or more.
Results may differ from the reference program's by a relative error of at most 0.001.
Values sent between devices are 32-bit elements; how exact they have to be, the bound alone decides.
A program may use at most 128 MiB of HBM per device.

```python
import math
import jax
import jax.numpy as jnp
from jax import lax

D = 8192
KV = 2048
BLOCK = 2048
LAYERS = 2
STEP = 10
TOK_DEV = 896
TOKENS = 7168
NB = 4
N_DP = 8


def scaled_values(key, width):
    keys = jax.random.split(key, 2)
    position = jnp.arange(width, dtype=jnp.float32) / width
    col_scale = jnp.exp(jnp.log(3.0) * position + jnp.log(3.4) * jax.random.uniform(keys[1], (width,)))
    values = jax.random.normal(keys[0], (LAYERS, TOKENS, width)) * col_scale
    return jnp.clip(values, -40.0, 40.0).astype(jnp.bfloat16)


def draw_activations(key, part):
    return scaled_values(jax.random.fold_in(key, 11), D)


def draw_cotangent(key, part):
    return scaled_values(jax.random.fold_in(key, 23), KV)


def shard_levels(stream_key, shape, cuts, smallest, high):
    def one(axis_at, parts):
        heights = jax.random.uniform(jax.random.fold_in(jax.random.fold_in(stream_key, 6), axis_at), (parts,), jnp.float32, smallest / len(cuts), high / len(cuts))
        return jnp.repeat(jnp.exp(heights), shape[axis_at] // parts).reshape((-1,) + (1,) * (len(shape) - axis_at - 1))

    gain = one(*cuts[0])
    for cut in cuts[1:]:
        gain = gain * one(*cut)
    return gain


def normal_values(stream_key, shape, scale, limit, shards=(), kind=jnp.bfloat16):
    array = scale * jax.random.normal(stream_key, shape, jnp.float32)
    if shards:
        array = array * shard_levels(stream_key, shape, shards, -0.22, 0.18)
    return jnp.clip(array, -limit, limit).astype(kind)


def setup_inputs(seed: int = 0) -> dict:
    arg_keys = jax.random.split(jax.random.key(seed), 8)
    return {
        "activations": draw_activations(jax.random.fold_in(arg_keys[7], 71), 0),
        "cotangent": draw_cotangent(jax.random.fold_in(arg_keys[7], 71), 0),
        "master_weights": normal_values(arg_keys[2], (LAYERS, KV, D), 1.0, 6.0, ((1, 8), (2, 4)), jnp.float32),
        "moment_codes": jnp.clip(jax.random.uniform(arg_keys[3], (LAYERS, KV, D), jnp.float32, -1.0, 1.0) * shard_levels(arg_keys[3], (LAYERS, KV, D), ((1, 8), (2, 4)), -0.4, 0.0), -1.0, 1.0).astype(jnp.bfloat16),
        "square_codes": jnp.clip(0.049804688 + 0.9501953 * jax.random.uniform(arg_keys[4], (LAYERS, KV, D), jnp.float32) ** shard_levels(arg_keys[4], (LAYERS, KV, D), ((1, 8), (2, 4)), -0.2, 0.2), 0.049804688, 1.0).astype(jnp.bfloat16),
        "moment_scales": jnp.clip(jnp.exp(math.log(0.5) - 2.3025851 * jax.random.uniform(arg_keys[5], (LAYERS, KV, NB), jnp.float32) ** shard_levels(arg_keys[5], (LAYERS, KV, NB), ((1, 8),), -0.2, 0.2)), 0.05, 0.5),
        "square_scales": jnp.clip(jnp.exp(math.log(0.05) - 2.3025851 * jax.random.uniform(arg_keys[6], (LAYERS, KV, NB), jnp.float32) ** shard_levels(arg_keys[6], (LAYERS, KV, NB), ((1, 8),), -0.2, 0.2)), 0.005, 0.05),
    }


beta_one = 0.9
beta_two = 0.999
learn_rate = 0.001
decay_rate = 0.1
adam_eps = 1e-08
scale_eps = 1e-06
norm_eps = 1e-06

def layer_gradient(layer_acts, layer_cot):
    grouped_acts = layer_acts.reshape(N_DP, TOK_DEV, D)
    grouped_cot = layer_cot.reshape(N_DP, TOK_DEV, KV)

    def accumulate(total, pair):
        group_acts, group_cot = pair
        partial_sum = lax.dot_general(group_cot, group_acts, (((0,), (0,)), ((), ())), preferred_element_type=jnp.float32)
        return (total + partial_sum, None)
    total, unused = lax.scan(accumulate, jnp.zeros((KV, D), jnp.float32), (grouped_acts, grouped_cot))
    return total

def reference(activations, cotangent, master_weights, moment_codes, square_codes, moment_scales, square_scales):
    gradients = [layer_gradient(activations[index], cotangent[index]) for index in range(LAYERS)]
    total_sq = jnp.float32(0.0)
    for gradient in gradients:
        total_sq = total_sq + jnp.sum(gradient * gradient)
    rms = jnp.sqrt(total_sq / float(LAYERS * KV * D) + norm_eps)
    clip_factor = jnp.minimum(1.0, 1.0 / rms)
    correct_one = 1.0 - beta_one ** STEP
    correct_two = 1.0 - beta_two ** STEP
    outs_weights, outs_mcode, outs_scode, outs_mscale, outs_sscale = ([], [], [], [], [])
    for index in range(LAYERS):
        old_moment = moment_codes[index].astype(jnp.float32).reshape(KV, NB, BLOCK) * moment_scales[index][:, :, None]
        old_square = square_codes[index].astype(jnp.float32).reshape(KV, NB, BLOCK) * square_scales[index][:, :, None]
        grad_now = (clip_factor * gradients[index]).reshape(KV, NB, BLOCK)
        moment = beta_one * old_moment + (1.0 - beta_one) * grad_now
        square = beta_two * old_square + (1.0 - beta_two) * grad_now * grad_now
        moment_max = lax.optimization_barrier(jnp.max(jnp.abs(moment), axis=2))
        square_max = lax.optimization_barrier(jnp.max(square, axis=2))
        outs_mcode.append((moment / (moment_max[:, :, None] + scale_eps)).astype(jnp.bfloat16).reshape(KV, D))
        outs_scode.append((square / (square_max[:, :, None] + scale_eps)).astype(jnp.bfloat16).reshape(KV, D))
        outs_mscale.append(moment_max)
        outs_sscale.append(square_max)
        ratio = (moment / correct_one / (jnp.sqrt(square / correct_two) + adam_eps)).reshape(KV, D)
        weights = master_weights[index]
        outs_weights.append(weights - learn_rate * (decay_rate * weights + ratio))
    return (jnp.stack(outs_weights), jnp.stack(outs_mcode), jnp.stack(outs_scode), jnp.stack(outs_mscale), jnp.stack(outs_sscale))
```

```python
import functools

import jax
import jax.numpy as jnp
from jax import lax
from jax.experimental import pallas as pl
from jax.experimental.pallas import tpu as pltpu
from jax.sharding import PartitionSpec as P

D = 8192
KV = 2048
BLOCK = 2048
LAYERS = 2
STEP = 10


beta_one = 0.9
beta_two = 0.999
learn_rate = 0.001
decay_rate = 0.1
adam_eps = 1e-08
scale_eps = 1e-06
norm_eps = 1e-06

LANES = 128
AHEAD = 3
XSLOTS = 4


def reduce_kernel(
    count, col_count, cot_ref, act_ref, out_ref, sq_ref,
    xs, xr, part, arr, bs, br, own_sq, sum_sq, col_sq, dp_sq,
    xs_sem, xr_sem, rs_sem, rr_sem, ls_sem, ll_sem, bs_sem, br_sem,
    cs_sem, cr_sem, ds_sem, dr_sem, x_free, from_right, from_left,
):
    layers, pairs, line, rows, tokens = cot_ref.shape
    cols = act_ref.shape[2]
    slots = part.shape[0]
    wide_per = cols // (2 * LANES) - 1
    per_layer = wide_per + 2
    period = (per_layer + 1) // 2
    items = layers * per_layer
    wides = layers * wide_per
    me = lax.axis_index("dp")
    z = me // 2
    x = me % 2
    peer = 2 * z + 1 - x
    right = jnp.minimum(z + 1, line - 1) * 2 + x
    left = jnp.maximum(z - 1, 0) * 2 + x
    has_right = z < line - 1
    has_left = z > 0
    mirror = line - 1 - z

    def signal(sem, where):
        pl.semaphore_signal(
            sem, inc=1, device_id={"dp": where}, device_id_type=pl.DeviceIdType.MESH
        )

    barrier = pltpu.get_barrier_semaphore()
    mine = lax.axis_index("col")
    for offset in range(1, count):
        signal(barrier, lax.rem(me + offset, count))
    for offset in range(1, col_count):
        pl.semaphore_signal(
            barrier, inc=1, device_id={"col": lax.rem(mine + offset, col_count)},
            device_id_type=pl.DeviceIdType.MESH,
        )
    pl.semaphore_wait(barrier, count + col_count - 2)

    def remote(src, dst, send, recv, where):
        return pltpu.make_async_remote_copy(
            src_ref=src, dst_ref=dst, send_sem=send, recv_sem=recv,
            device_id={"dp": where}, device_id_type=pl.DeviceIdType.MESH,
        )

    def describe(item):
        layer = item // per_layer
        place = item % per_layer
        narrow = place % period == 0
        wide_at = place - (place + period - 1) // period
        narrow_at = place // period
        return layer, narrow, wide_at, narrow_at

    def x_copy(number):
        slot = number % XSLOTS
        return remote(xs.at[slot], xr.at[slot], xs_sem.at[slot], xr_sem.at[slot], peer)

    def r_copy(slot, target):
        return remote(
            part.at[slot, target], arr.at[slot, target + 1],
            rs_sem.at[slot, target], rr_sem.at[slot, target], right,
        )

    def l_copy(slot, target):
        return remote(
            part.at[slot, target], arr.at[slot, target],
            ls_sem.at[slot, target], ll_sem.at[slot, target], left,
        )

    def b_copy(number):
        return remote(
            bs.at[number], br.at[number], bs_sem.at[number], br_sem.at[number], peer
        )

    def product(layer, pair, target, start, width):
        return jnp.dot(
            cot_ref[layer, pair, target],
            act_ref[layer, :, pl.ds(pl.multiple_of(start, LANES), width)],
            preferred_element_type=jnp.float32,
        )

    def send_wide(item):
        layer, narrow, wide_at, _ = describe(item)

        @pl.when(jnp.logical_not(narrow))
        def _():
            number = layer * wide_per + wide_at
            slot = number % XSLOTS

            @pl.loop(0, line)
            def _(target):
                value = product(layer, 1 - x, target, wide_at * 2 * LANES, 2 * LANES)
                xs[slot, target, 0] = value[:, :LANES]
                xs[slot, target, 1] = value[:, LANES:]

            @pl.when(number >= XSLOTS)
            def _():
                pl.semaphore_wait(x_free, 1)

            x_copy(number).start()

    def form(item):
        layer, narrow, wide_at, narrow_at = describe(item)
        here = item % slots

        @pl.when(item >= slots)
        def _():
            @pl.when(has_right)
            def _():
                pl.semaphore_wait(from_right, 1)

            @pl.when(has_left)
            def _():
                pl.semaphore_wait(from_left, 1)

        @pl.when(narrow)
        def _():
            start = wide_per * 2 * LANES + narrow_at * LANES

            @pl.loop(0, line)
            def _(target):
                part[here, target, 0] = product(layer, 0, target, start, LANES)
                part[here, target, 1] = product(layer, 1, target, start, LANES)

        @pl.when(jnp.logical_not(narrow))
        def _():
            number = layer * wide_per + wide_at
            slot = number % XSLOTS
            x_copy(number).wait()

            @pl.loop(0, line)
            def _(target):
                value = product(layer, x, target, wide_at * 2 * LANES, 2 * LANES)
                part[here, target, 0] = value[:, :LANES] + xr[slot, target, 0]
                part[here, target, 1] = value[:, LANES:] + xr[slot, target, 1]

            @pl.when(number + XSLOTS < wides)
            def _():
                signal(x_free, peer)

    def hop(item, stage):
        here = item % slots

        @pl.when(z <= stage)
        def _():
            target = line - 1 - stage + z
            if stage > 0:
                @pl.when(has_left)
                def _():
                    r_copy(here, target).wait_recv()
                    part[here, target] += arr[here, target + 1]

            r_copy(here, target).start()

        @pl.when(mirror <= stage)
        def _():
            target = stage - mirror
            if stage > 0:
                @pl.when(has_right)
                def _():
                    l_copy(here, target).wait_recv()
                    part[here, target] += arr[here, target]

            l_copy(here, target).start()

    def finish(item):
        layer, narrow, wide_at, narrow_at = describe(item)
        here = item % slots

        @pl.when(has_left)
        def _():
            r_copy(here, z).wait_recv()
            part[here, z] += arr[here, z + 1]

        @pl.when(has_right)
        def _():
            l_copy(here, z).wait_recv()
            part[here, z] += arr[here, z]

        for target in range(line):
            @pl.when(target > z)
            def _(target=target):
                r_copy(here, target).wait_send()

            @pl.when(target < z)
            def _(target=target):
                l_copy(here, target).wait_send()

        @pl.when(narrow)
        def _():
            number = layer * 2 + narrow_at
            start = wide_per * 2 * LANES + narrow_at * LANES
            bs[number] = part[here, z, 1 - x]
            b_copy(number).start()
            out_ref[layer, :, pl.ds(pl.multiple_of(start, LANES), LANES)] = part[here, z, x]

        @pl.when(jnp.logical_not(narrow))
        def _():
            for half in range(2):
                start = wide_at * 2 * LANES + half * LANES
                out_ref[layer, :, pl.ds(pl.multiple_of(start, LANES), LANES)] = part[here, z, half]

        @pl.when(item + slots < items)
        def _():
            @pl.when(has_left)
            def _():
                signal(from_right, left)

            @pl.when(has_right)
            def _():
                signal(from_left, right)

    for item in range(1, AHEAD):
        send_wide(jnp.int32(item))

    @pl.loop(0, items + line - 1)
    def _(step):
        def guard(item, action):
            pl.when(jnp.logical_and(item >= 0, item < items))(lambda: action(item))

        guard(step + AHEAD, send_wide)
        guard(step - (line - 1), finish)
        for stage in reversed(range(1, line - 1)):
            guard(step - stage, functools.partial(hop, stage=stage))

        def begin(item):
            form(item)
            hop(item, 0)

        guard(step, begin)

    for number in range(2 * layers):
        b_copy(number).wait()
        start = wide_per * 2 * LANES + (number % 2) * LANES
        out_ref[number // 2, :, start : start + LANES] += br[number]

    def square_rows(index, total):
        layer = index // (rows // 8)
        at = pl.multiple_of(index % (rows // 8) * 8, 8)
        for piece in range(cols // LANES):
            value = out_ref[layer, pl.ds(at, 8), piece * LANES : (piece + 1) * LANES]
            total = total + value * value
        return total

    def spread(src, landing, send, recv, axis, index, size):
        copies = []
        for offset in range(1, size):
            copies.append(
                pltpu.make_async_remote_copy(
                    src_ref=src, dst_ref=landing.at[offset - 1],
                    send_sem=send.at[offset - 1], recv_sem=recv.at[offset - 1],
                    device_id={axis: lax.rem(index + offset, size)},
                    device_id_type=pl.DeviceIdType.MESH,
                )
            )
        for copy in copies:
            copy.start()
        for copy in copies:
            copy.wait()
        total = src[...]
        for offset in range(1, size):
            total = total + landing[offset - 1]
        return total

    own_sq[...] = lax.fori_loop(
        0, layers * rows // 8, square_rows, jnp.zeros((8, LANES), jnp.float32)
    )
    sum_sq[...] = spread(own_sq, col_sq, cs_sem, cr_sem, "col", mine, col_count)
    sq_ref[...] = spread(sum_sq, dp_sq, ds_sem, dr_sem, "dp", me, count)


def reduced_gradient(activations, cotangent, mesh_shape):
    count = mesh_shape["dp"]
    col_count = mesh_shape["col"]
    layers, tokens, cols = activations.shape
    line = count // 2
    rows = cotangent.shape[2] // count
    slots = line + 2
    cot = cotangent.reshape(layers, tokens, line, 2, rows).transpose(0, 3, 2, 4, 1)
    block = (line, 2, rows, LANES)
    dma = pltpu.SemaphoreType.DMA
    vmem = pl.BlockSpec(memory_space=pltpu.VMEM)
    return pl.pallas_call(
        functools.partial(reduce_kernel, count, col_count),
        out_shape=(
            jax.ShapeDtypeStruct((layers, rows, cols), jnp.float32),
            jax.ShapeDtypeStruct((8, LANES), jnp.float32),
        ),
        in_specs=[vmem, vmem],
        out_specs=(vmem, vmem),
        scratch_shapes=[
            pltpu.VMEM((XSLOTS,) + block, jnp.float32),
            pltpu.VMEM((XSLOTS,) + block, jnp.float32),
            pltpu.VMEM((slots,) + block, jnp.float32),
            pltpu.VMEM((slots, line + 1) + block[1:], jnp.float32),
            pltpu.VMEM((2 * layers, rows, LANES), jnp.float32),
            pltpu.VMEM((2 * layers, rows, LANES), jnp.float32),
            pltpu.VMEM((8, LANES), jnp.float32),
            pltpu.VMEM((8, LANES), jnp.float32),
            pltpu.VMEM((col_count - 1, 8, LANES), jnp.float32),
            pltpu.VMEM((count - 1, 8, LANES), jnp.float32),
            dma((XSLOTS,)), dma((XSLOTS,)),
            dma((slots, line)), dma((slots, line)), dma((slots, line)), dma((slots, line)),
            dma((2 * layers,)), dma((2 * layers,)),
            dma((col_count - 1,)), dma((col_count - 1,)), dma((count - 1,)), dma((count - 1,)),
            pltpu.SemaphoreType.REGULAR, pltpu.SemaphoreType.REGULAR, pltpu.SemaphoreType.REGULAR,
        ],
        compiler_params=pltpu.CompilerParams(
            collective_id=0, has_side_effects=True, vmem_limit_bytes=62 * 2**20
        ),
    )(cot, activations)


AHEAD_UNITS = 5
SEND_SLOTS = 6
ACT_SLOTS = 5
NARROW = 2


def factor_kernel(
    count, col_count, cot_hbm, act_hbm, out_ref, sq_ref,
    cot_raw, act_raw, narrow_act, cot_t, act_cat, xs, xr, crx, part, arr, narrow_in,
    own_sq, sum_sq, col_sq, dp_sq,
    ld_sem, xs_sem, xr_sem, pr_sem, cs_sem, cr_sem, rs_sem, rr_sem, ls_sem, ll_sem, fs_sem, fr_sem,
    qs_sem, qr_sem, ds_sem, dr_sem, act_free, cot_free, from_right, from_left,
):
    layers, tokens, cols = act_hbm.shape
    half = cols // 2
    line = count // 2
    pair_rows = part.shape[2]
    rows = pair_rows // 2
    slots = part.shape[0]
    chunks = half // LANES
    first_chunks = chunks - NARROW // 2
    wides = first_chunks + (layers - 1) * chunks
    items = NARROW + wides
    first_units = first_chunks + line
    layer_units = chunks + line
    units = first_units + (layers - 1) * layer_units
    own = col_count - 1
    me = lax.axis_index("dp")
    mine = lax.axis_index("col")
    z = me // 2
    x = me % 2
    peer = 2 * z + 1 - x
    right = jnp.minimum(z + 1, line - 1) * 2 + x
    left = jnp.maximum(z - 1, 0) * 2 + x
    has_right = z < line - 1
    has_left = z > 0
    mirror = line - 1 - z
    own_half = pl.multiple_of(x * half, LANES)
    peer_half = pl.multiple_of((1 - x) * half, LANES)

    def lanes(start, width=LANES):
        return pl.ds(pl.multiple_of(start, LANES), width)

    def signal(sem, where):
        pl.semaphore_signal(
            sem, inc=1, device_id={"dp": where}, device_id_type=pl.DeviceIdType.MESH
        )

    loads = []

    def load(src, dst):
        copy = pltpu.make_async_copy(src, dst, ld_sem.at[len(loads)])
        copy.start()
        loads.append(copy)

    load(cot_hbm.at[0], cot_raw.at[0])
    for index in range(NARROW):
        start = (index % 2) * half + (chunks - 1 - index // 2) * LANES
        load(act_hbm.at[0, :, lanes(start)], narrow_act.at[index])
    for layer in range(layers):
        if layer > 0:
            load(cot_hbm.at[layer], cot_raw.at[layer])
        load(act_hbm.at[layer, :, pl.ds(peer_half, half)], act_raw.at[layer])
        load(act_hbm.at[layer, :, pl.ds(own_half, half)], act_cat.at[layer, pl.ds(0, tokens)])

    barrier = pltpu.get_barrier_semaphore()
    for offset in range(1, count):
        signal(barrier, lax.rem(me + offset, count))
    for offset in range(1, col_count):
        pl.semaphore_signal(
            barrier, inc=1, device_id={"col": lax.rem(mine + offset, col_count)},
            device_id_type=pl.DeviceIdType.MESH,
        )
    pl.semaphore_wait(barrier, count + col_count - 2)

    def remote(src, dst, send, recv, where):
        return pltpu.make_async_remote_copy(
            src_ref=src, dst_ref=dst, send_sem=send, recv_sem=recv,
            device_id={"dp": where}, device_id_type=pl.DeviceIdType.MESH,
        )

    def block_target(place):
        after = line - 1 - z
        rising = jnp.where(place < after, line - 1 - place, place - after)
        falling = jnp.where(place < z, place, line - 1 - (place - z))
        other = jnp.where(z < line // 2, rising, falling)
        return jnp.where(place < line - 1, other, z)

    def describe(item):
        number = item - NARROW
        narrow = item < NARROW
        later = jnp.maximum(number - first_chunks, 0)
        layer = jnp.where(number < first_chunks, 0, 1 + later // chunks)
        chunk = jnp.where(number < first_chunks, number, later % chunks)
        return layer, narrow, chunk

    def unit_base(layer):
        return jnp.where(layer == 0, 0, first_units + (layer - 1) * layer_units)

    def act_number(layer, chunk):
        return jnp.where(layer == 0, chunk, first_chunks + (layer - 1) * chunks + chunk)

    def act_copy(unit, number):
        here = unit % SEND_SLOTS
        slot = number % ACT_SLOTS
        return remote(xs.at[here], xr.at[slot], xs_sem.at[here], xr_sem.at[slot], peer)

    def cot_copy(unit, place):
        here = unit % SEND_SLOTS
        return remote(xs.at[here], crx.at[place, own], xs_sem.at[here], pr_sem.at[place], peer)

    def col_copy(place, offset):
        return pltpu.make_async_remote_copy(
            src_ref=crx.at[place, own], dst_ref=crx.at[place, offset - 1],
            send_sem=cs_sem.at[place, offset - 1], recv_sem=cr_sem.at[place, offset - 1],
            device_id={"col": lax.rem(mine + offset, col_count)},
            device_id_type=pl.DeviceIdType.MESH,
        )

    def r_copy(slot, target):
        return remote(
            part.at[slot, target], arr.at[slot, target + 1],
            rs_sem.at[slot, target], rr_sem.at[slot, target], right,
        )

    def l_copy(slot, target):
        return remote(
            part.at[slot, target], arr.at[slot, target],
            ls_sem.at[slot, target], ll_sem.at[slot, target], left,
        )

    def row_source(slot):
        return part.at[slot, z, pl.ds(pl.multiple_of((1 - x) * rows, 8), rows)]

    def n_copy(item):
        slot = item % slots
        return remote(
            row_source(slot), narrow_in.at[jnp.minimum(item, NARROW - 1)],
            fs_sem.at[slot], fr_sem.at[item], peer,
        )

    def f_copy(item, side):
        layer, narrow, chunk = describe(item)
        slot = item % slots
        where = out_ref.at[layer, :, lanes(side * half + chunk * LANES)]
        return remote(row_source(slot), where, fs_sem.at[slot], fr_sem.at[item], peer)

    def send(unit):
        @pl.when(unit < units)
        def _():
            layer = jnp.where(unit < first_units, 0, 1 + (unit - first_units) // layer_units)
            index = unit - unit_base(layer)
            is_cot = jnp.logical_or(index < line - 1, index == 2 * line - 2)
            here = unit % SEND_SLOTS

            @pl.when(unit >= SEND_SLOTS)
            def _():
                act_copy(unit, 0).wait_send()

            @pl.when(is_cot)
            def _():
                place = jnp.minimum(index, line - 1)
                start = block_target(place) * pair_rows + mine * LANES
                xs[here] = cot_raw[layer, :, lanes(start)].astype(jnp.float32)

                @pl.when(layer > 0)
                def _():
                    pl.semaphore_wait(cot_free.at[place], 1)

                cot_copy(unit, place).start()

            @pl.when(jnp.logical_not(is_cot))
            def _():
                chunk = jnp.where(index < 2 * line - 2, index - (line - 1), index - line)
                number = act_number(layer, chunk)
                xs[here] = act_raw[layer, :, lanes(chunk * LANES)].astype(jnp.float32)

                @pl.when(number >= ACT_SLOTS)
                def _():
                    pl.semaphore_wait(act_free.at[number % ACT_SLOTS], 1)

                act_copy(unit, number).start()

    def forward(layer, place):
        cot_copy(0, place).wait_recv()
        for offset in range(1, col_count):
            col_copy(place, offset).start()
        send(unit_base(layer) + jnp.where(place < line - 1, place, 2 * line - 2) + AHEAD_UNITS)

    def prepare(layer, place):
        base = block_target(place) * pair_rows

        @pl.loop(0, col_count)
        def _(member):
            start = base + member * LANES
            value = cot_raw[layer, :, lanes(start)].astype(jnp.float32)
            cot_t[layer, lanes(start), pl.ds(0, tokens)] = value.T.astype(jnp.bfloat16)

    def absorb(layer, place):
        @pl.when(layer > 0)
        def _():
            prepare(layer, place)

        base = block_target(place) * pair_rows
        for offset in range(col_count):
            if offset > 0:
                col_copy(place, offset).wait_recv()
            source = crx[place, offset - 1 if offset > 0 else own]
            owner = lax.rem(mine - offset + col_count, col_count)
            cot_t[layer, lanes(base + owner * LANES), pl.ds(tokens, tokens)] = source.T.astype(jnp.bfloat16)
        for offset in range(1, col_count):
            col_copy(place, offset).wait_send()

        @pl.when(layer < layers - 1)
        def _():
            signal(cot_free.at[place], peer)

    def take(layer, chunk):
        number = act_number(layer, chunk)
        slot = number % ACT_SLOTS
        act_copy(0, number).wait_recv()
        act_cat[layer, pl.ds(tokens, tokens), lanes(chunk * LANES)] = xr[slot].astype(jnp.bfloat16)

        @pl.when(number + ACT_SLOTS < wides)
        def _():
            signal(act_free.at[slot], peer)

        index = jnp.where(chunk < line - 1, chunk + line - 1, chunk + line)
        send(unit_base(layer) + index + AHEAD_UNITS)

    def form(item, target):
        layer, narrow, chunk = describe(item)
        here = item % slots
        at = pl.ds(pl.multiple_of(target * pair_rows, LANES), pair_rows)

        @pl.when(narrow)
        def _():
            part[here, target] = jnp.dot(
                cot_t[0, at, pl.ds(0, tokens)], narrow_act[jnp.minimum(item, NARROW - 1)],
                preferred_element_type=jnp.float32,
            )

        @pl.when(jnp.logical_not(narrow))
        def _():
            part[here, target] = jnp.dot(
                cot_t[layer, at, :], act_cat[layer, :, lanes(chunk * LANES)],
                preferred_element_type=jnp.float32,
            )

    def opens(item):
        layer, narrow, chunk = describe(item)
        return layer, jnp.logical_and(jnp.logical_not(narrow), chunk == 0)

    def ready(item, place):
        @pl.when(item == 0)
        def _():
            prepare(0, place)

        layer, first = opens(item)

        @pl.when(first)
        def _():
            if place == 0:
                for early in range(2, line - 1):
                    forward(layer, early)
            absorb(layer, place)

    def hop(item, stage):
        here = item % slots

        @pl.when(z <= stage)
        def _():
            target = line - 1 - stage + z
            form(item, target)
            if stage > 0:
                @pl.when(has_left)
                def _():
                    r_copy(here, target).wait_recv()
                    part[here, target] += arr[here, target + 1]

            r_copy(here, target).start()

        @pl.when(mirror <= stage)
        def _():
            target = stage - mirror
            form(item, target)
            if stage > 0:
                @pl.when(has_right)
                def _():
                    l_copy(here, target).wait_recv()
                    part[here, target] += arr[here, target]

            l_copy(here, target).start()

    def begin(item):
        layer, narrow, chunk = describe(item)
        ready(item, 0)

        @pl.when(jnp.logical_not(narrow))
        def _():
            take(layer, chunk)

        @pl.when(item >= slots)
        def _():
            @pl.when(has_right)
            def _():
                pl.semaphore_wait(from_right, 1)

            @pl.when(has_left)
            def _():
                pl.semaphore_wait(from_left, 1)

        hop(item, 0)
        next_layer, next_first = opens(item + 1)

        @pl.when(jnp.logical_and(next_first, item + 1 < items))
        def _():
            for place in range(2):
                forward(next_layer, place)

        @pl.when(jnp.logical_and(jnp.logical_not(narrow), chunk == line - 2))
        def _():
            forward(layer, line - 1)

    def middle(item, stage):
        ready(item, stage)
        hop(item, stage)

    def finish(item):
        layer, narrow, chunk = describe(item)
        here = item % slots
        ready(item, line - 1)

        @pl.when(item >= slots)
        def _():
            n_copy(item - slots).wait_send()

        form(item, z)

        @pl.when(has_left)
        def _():
            r_copy(here, z).wait_recv()
            part[here, z] += arr[here, z + 1]

        @pl.when(has_right)
        def _():
            l_copy(here, z).wait_recv()
            part[here, z] += arr[here, z]

        for target in range(line):
            @pl.when(target > z)
            def _(target=target):
                r_copy(here, target).wait_send()

            @pl.when(target < z)
            def _(target=target):
                l_copy(here, target).wait_send()

        kept = pl.ds(pl.multiple_of(x * rows, 8), rows)

        @pl.when(narrow)
        def _():
            n_copy(item).start()
            start = (item % 2) * half + (chunks - 1 - item // 2) * LANES
            out_ref[0, :, lanes(start)] = part[here, z, kept]

        @pl.when(jnp.logical_not(narrow))
        def _():
            f_copy(item, x).start()
            out_ref[layer, :, lanes(own_half + chunk * LANES)] = part[here, z, kept]

        @pl.when(item + slots < items)
        def _():
            @pl.when(has_left)
            def _():
                signal(from_right, left)

            @pl.when(has_right)
            def _():
                signal(from_left, right)

    for copy in loads[: 2 + NARROW]:
        copy.wait()

    @pl.loop(0, AHEAD_UNITS)
    def _(unit):
        send(unit)

    for copy in loads[2 + NARROW :]:
        copy.wait()

    @pl.loop(0, items + line - 1)
    def _(step):
        def guard(item, action):
            pl.when(jnp.logical_and(item >= 0, item < items))(lambda: action(item))

        for stage in reversed(range(1, line - 1)):
            guard(step - stage, functools.partial(middle, stage=stage))
        guard(step, begin)
        guard(step - (line - 1), finish)

    @pl.loop(units - SEND_SLOTS, units)
    def _(unit):
        act_copy(unit, 0).wait_send()

    @pl.loop(items - slots, items)
    def _(item):
        n_copy(item).wait_send()

    for item in range(NARROW):
        n_copy(item).wait_recv()
        start = (item % 2) * half + (chunks - 1 - item // 2) * LANES
        out_ref[0, :, start : start + LANES] += narrow_in[item]

    @pl.loop(NARROW, items)
    def _(item):
        f_copy(item, 1 - x).wait_recv()

    def square_rows(index, total):
        layer = index // (rows // 8)
        at = pl.multiple_of(index % (rows // 8) * 8, 8)
        for piece in range(cols // LANES):
            value = out_ref[layer, pl.ds(at, 8), piece * LANES : (piece + 1) * LANES]
            total = total + value * value
        return total

    def spread(src, landing, send_sems, recv_sems, axis, index, size):
        copies = []
        for offset in range(1, size):
            copies.append(
                pltpu.make_async_remote_copy(
                    src_ref=src, dst_ref=landing.at[offset - 1],
                    send_sem=send_sems.at[offset - 1], recv_sem=recv_sems.at[offset - 1],
                    device_id={axis: lax.rem(index + offset, size)},
                    device_id_type=pl.DeviceIdType.MESH,
                )
            )
        for copy in copies:
            copy.start()
        for copy in copies:
            copy.wait()
        total = src[...]
        for offset in range(1, size):
            total = total + landing[offset - 1]
        return total

    own_sq[...] = lax.fori_loop(
        0, layers * rows // 8, square_rows, jnp.zeros((8, LANES), jnp.float32)
    )
    sum_sq[...] = spread(own_sq, col_sq, qs_sem, qr_sem, "col", mine, col_count)
    sq_ref[...] = spread(sum_sq, dp_sq, ds_sem, dr_sem, "dp", me, count)


def factor_gradient(activations, cotangent, mesh_shape):
    count = mesh_shape["dp"]
    col_count = mesh_shape["col"]
    layers, tokens, cols = activations.shape
    line = count // 2
    features = cotangent.shape[2]
    rows = features // count
    half = cols // 2
    slots = line + 1
    items = NARROW + layers * (half // LANES) - NARROW // 2
    piece = (tokens, LANES)
    f32, bf16 = jnp.float32, jnp.bfloat16
    dma = pltpu.SemaphoreType.DMA
    regular = pltpu.SemaphoreType.REGULAR
    vmem = pl.BlockSpec(memory_space=pltpu.VMEM)
    hbm = pl.BlockSpec(memory_space=pl.ANY)
    return pl.pallas_call(
        functools.partial(factor_kernel, count, col_count),
        out_shape=(
            jax.ShapeDtypeStruct((layers, rows, cols), f32),
            jax.ShapeDtypeStruct((8, LANES), f32),
        ),
        in_specs=[hbm, hbm],
        out_specs=(vmem, vmem),
        scratch_shapes=[
            pltpu.VMEM((layers, tokens, features), bf16),
            pltpu.VMEM((layers, tokens, half), bf16),
            pltpu.VMEM((NARROW,) + piece, bf16),
            pltpu.VMEM((layers, features, 2 * tokens), bf16),
            pltpu.VMEM((layers, 2 * tokens, half), bf16),
            pltpu.VMEM((SEND_SLOTS,) + piece, f32),
            pltpu.VMEM((ACT_SLOTS,) + piece, f32),
            pltpu.VMEM((line, col_count) + piece, f32),
            pltpu.VMEM((slots, line, 2 * rows, LANES), f32),
            pltpu.VMEM((slots, line + 1, 2 * rows, LANES), f32),
            pltpu.VMEM((NARROW, rows, LANES), f32),
            pltpu.VMEM((8, LANES), f32),
            pltpu.VMEM((8, LANES), f32),
            pltpu.VMEM((col_count - 1, 8, LANES), f32),
            pltpu.VMEM((count - 1, 8, LANES), f32),
            dma((NARROW + 3 * layers,)),
            dma((SEND_SLOTS,)), dma((ACT_SLOTS,)), dma((line,)),
            dma((line, col_count - 1)), dma((line, col_count - 1)),
            dma((slots, line)), dma((slots, line)), dma((slots, line)), dma((slots, line)),
            dma((slots,)), dma((items,)),
            dma((col_count - 1,)), dma((col_count - 1,)), dma((count - 1,)), dma((count - 1,)),
            regular((ACT_SLOTS,)), regular((line,)), regular, regular,
        ],
        compiler_params=pltpu.CompilerParams(
            collective_id=0, has_side_effects=True, vmem_limit_bytes=62 * 2**20
        ),
    )(cotangent, activations)


def fits_factors(activations, cotangent, mesh_shape):
    count = mesh_shape["dp"]
    line = count // 2
    rows = cotangent.shape[2] // count
    chunks = activations.shape[2] // (2 * LANES)
    aligned = activations.shape[1] % LANES == 0 and activations.shape[2] % (2 * LANES) == 0
    return aligned and line >= 3 and 2 * rows == LANES * mesh_shape["col"] and chunks - NARROW // 2 > line


def local(
    mesh_shape, activations, cotangent, master_weights, moment_codes, square_codes, moment_scales, square_scales
):
    layer_count = activations.shape[0]
    shard_rows = master_weights.shape[1]
    shard_cols = master_weights.shape[2]
    block_count = moment_scales.shape[2]
    reduce = factor_gradient if fits_factors(activations, cotangent, mesh_shape) else reduced_gradient
    gradient, squares = reduce(activations, cotangent, mesh_shape)
    total_sq = jnp.sum(squares)
    rms = jnp.sqrt(total_sq / float(LAYERS * KV * D) + norm_eps)
    clip_factor = jnp.minimum(1.0, 1.0 / rms)
    correct_one = 1.0 - beta_one**STEP
    correct_two = 1.0 - beta_two**STEP
    own_block = lax.axis_index("col") * shard_cols // BLOCK
    selector = (jnp.arange(block_count, dtype=jnp.int32) == own_block).astype(jnp.float32)
    outs_weights, outs_mcode, outs_scode, outs_mscale, outs_sscale = ([], [], [], [], [])
    for layer_index in range(layer_count):
        moment_scale = jnp.sum(moment_scales[layer_index] * selector, axis=1)
        square_scale = jnp.sum(square_scales[layer_index] * selector, axis=1)
        old_moment = moment_codes[layer_index].astype(jnp.float32) * moment_scale[:, None]
        old_square = square_codes[layer_index].astype(jnp.float32) * square_scale[:, None]
        grad_now = clip_factor * gradient[layer_index]
        new_moment = beta_one * old_moment + (1.0 - beta_one) * grad_now
        new_square = beta_two * old_square + (1.0 - beta_two) * grad_now * grad_now
        moment_part = jnp.max(jnp.abs(new_moment), axis=1)[:, None] * selector
        square_part = jnp.max(new_square, axis=1)[:, None] * selector
        moment, square, moment_part, square_part = (
            new_moment,
            new_square,
            moment_part,
            square_part,
        )
        moment_max, square_max = lax.pmax((moment_part, square_part), "col")
        moment_div = jnp.sum(moment_max * selector, axis=1)[:, None]
        square_div = jnp.sum(square_max * selector, axis=1)[:, None]
        moment_out = (moment / (moment_div + scale_eps)).astype(jnp.bfloat16)
        square_out = (square / (square_div + scale_eps)).astype(jnp.bfloat16)
        ratio = moment / correct_one / (jnp.sqrt(square / correct_two) + adam_eps)
        weights = master_weights[layer_index]
        results = (weights - learn_rate * (decay_rate * weights + ratio), moment_out, square_out)
        outs_weights.append(results[0])
        outs_mcode.append(results[1])
        outs_scode.append(results[2])
        outs_mscale.append(moment_max)
        outs_sscale.append(square_max)
    return (
        jnp.stack(outs_weights),
        jnp.stack(outs_mcode),
        jnp.stack(outs_scode),
        jnp.stack(outs_mscale),
        jnp.stack(outs_sscale),
    )


def solution(mesh):
    in_specs = (
        P(None, "dp", "col"),
        P(None, "dp", None),
        P(None, "dp", "col"),
        P(None, "dp", "col"),
        P(None, "dp", "col"),
        P(None, "dp", None),
        P(None, "dp", None),
    )
    out_specs = (
        P(None, "dp", "col"),
        P(None, "dp", "col"),
        P(None, "dp", "col"),
        P(None, "dp", None),
        P(None, "dp", None),
    )
    return jax.shard_map(functools.partial(local, dict(mesh.shape)), mesh=mesh, in_specs=in_specs, out_specs=out_specs, check_vma=False)
```

```python
import functools

import jax
import jax.numpy as jnp
from jax import lax
from jax.experimental import pallas as pl
from jax.experimental.pallas import tpu as pltpu
from jax.sharding import PartitionSpec as P

D = 8192
KV = 2048
BLOCK = 2048
LAYERS = 2
STEP = 10


beta_one = 0.9
beta_two = 0.999
learn_rate = 0.001
decay_rate = 0.1
adam_eps = 1e-08
scale_eps = 1e-06
norm_eps = 1e-06

LANES = 128
AHEAD = 3
XSLOTS = 4


def reduce_kernel(
    count, col_count, cot_ref, act_ref, out_ref, sq_ref,
    xs, xr, part, arr, bs, br, own_sq, sum_sq, col_sq, dp_sq,
    xs_sem, xr_sem, rs_sem, rr_sem, ls_sem, ll_sem, bs_sem, br_sem,
    cs_sem, cr_sem, ds_sem, dr_sem, x_free, from_right, from_left,
):
    layers, pairs, line, rows, tokens = cot_ref.shape
    cols = act_ref.shape[2]
    slots = part.shape[0]
    wide_per = cols // (2 * LANES) - 1
    per_layer = wide_per + 2
    period = (per_layer + 1) // 2
    items = layers * per_layer
    wides = layers * wide_per
    me = lax.axis_index("dp")
    z = me // 2
    x = me % 2
    peer = 2 * z + 1 - x
    right = jnp.minimum(z + 1, line - 1) * 2 + x
    left = jnp.maximum(z - 1, 0) * 2 + x
    has_right = z < line - 1
    has_left = z > 0
    mirror = line - 1 - z

    def signal(sem, where):
        pl.semaphore_signal(
            sem, inc=1, device_id={"dp": where}, device_id_type=pl.DeviceIdType.MESH
        )

    barrier = pltpu.get_barrier_semaphore()
    mine = lax.axis_index("col")
    for offset in range(1, count):
        signal(barrier, lax.rem(me + offset, count))
    for offset in range(1, col_count):
        pl.semaphore_signal(
            barrier, inc=1, device_id={"col": lax.rem(mine + offset, col_count)},
            device_id_type=pl.DeviceIdType.MESH,
        )
    pl.semaphore_wait(barrier, count + col_count - 2)

    def remote(src, dst, send, recv, where):
        return pltpu.make_async_remote_copy(
            src_ref=src, dst_ref=dst, send_sem=send, recv_sem=recv,
            device_id={"dp": where}, device_id_type=pl.DeviceIdType.MESH,
        )

    def describe(item):
        layer = item // per_layer
        place = item % per_layer
        narrow = place % period == 0
        wide_at = place - (place + period - 1) // period
        narrow_at = place // period
        return layer, narrow, wide_at, narrow_at

    def x_copy(number):
        slot = number % XSLOTS
        return remote(xs.at[slot], xr.at[slot], xs_sem.at[slot], xr_sem.at[slot], peer)

    def r_copy(slot, target):
        return remote(
            part.at[slot, target], arr.at[slot, target + 1],
            rs_sem.at[slot, target], rr_sem.at[slot, target], right,
        )

    def l_copy(slot, target):
        return remote(
            part.at[slot, target], arr.at[slot, target],
            ls_sem.at[slot, target], ll_sem.at[slot, target], left,
        )

    def b_copy(number):
        return remote(
            bs.at[number], br.at[number], bs_sem.at[number], br_sem.at[number], peer
        )

    def product(layer, pair, target, start, width):
        return jnp.dot(
            cot_ref[layer, pair, target],
            act_ref[layer, :, pl.ds(pl.multiple_of(start, LANES), width)],
            preferred_element_type=jnp.float32,
        )

    def send_wide(item):
        layer, narrow, wide_at, _ = describe(item)

        @pl.when(jnp.logical_not(narrow))
        def _():
            number = layer * wide_per + wide_at
            slot = number % XSLOTS

            @pl.loop(0, line)
            def _(target):
                value = product(layer, 1 - x, target, wide_at * 2 * LANES, 2 * LANES)
                xs[slot, target, 0] = value[:, :LANES]
                xs[slot, target, 1] = value[:, LANES:]

            @pl.when(number >= XSLOTS)
            def _():
                pl.semaphore_wait(x_free, 1)

            x_copy(number).start()

    def form(item):
        layer, narrow, wide_at, narrow_at = describe(item)
        here = item % slots

        @pl.when(item >= slots)
        def _():
            @pl.when(has_right)
            def _():
                pl.semaphore_wait(from_right, 1)

            @pl.when(has_left)
            def _():
                pl.semaphore_wait(from_left, 1)

        @pl.when(narrow)
        def _():
            start = wide_per * 2 * LANES + narrow_at * LANES

            @pl.loop(0, line)
            def _(target):
                part[here, target, 0] = product(layer, 0, target, start, LANES)
                part[here, target, 1] = product(layer, 1, target, start, LANES)

        @pl.when(jnp.logical_not(narrow))
        def _():
            number = layer * wide_per + wide_at
            slot = number % XSLOTS
            x_copy(number).wait()

            @pl.loop(0, line)
            def _(target):
                value = product(layer, x, target, wide_at * 2 * LANES, 2 * LANES)
                part[here, target, 0] = value[:, :LANES] + xr[slot, target, 0]
                part[here, target, 1] = value[:, LANES:] + xr[slot, target, 1]

            @pl.when(number + XSLOTS < wides)
            def _():
                signal(x_free, peer)

    def hop(item, stage):
        here = item % slots

        @pl.when(z <= stage)
        def _():
            target = line - 1 - stage + z
            if stage > 0:
                @pl.when(has_left)
                def _():
                    r_copy(here, target).wait_recv()
                    part[here, target] += arr[here, target + 1]

            r_copy(here, target).start()

        @pl.when(mirror <= stage)
        def _():
            target = stage - mirror
            if stage > 0:
                @pl.when(has_right)
                def _():
                    l_copy(here, target).wait_recv()
                    part[here, target] += arr[here, target]

            l_copy(here, target).start()

    def finish(item):
        layer, narrow, wide_at, narrow_at = describe(item)
        here = item % slots

        @pl.when(has_left)
        def _():
            r_copy(here, z).wait_recv()
            part[here, z] += arr[here, z + 1]

        @pl.when(has_right)
        def _():
            l_copy(here, z).wait_recv()
            part[here, z] += arr[here, z]

        for target in range(line):
            @pl.when(target > z)
            def _(target=target):
                r_copy(here, target).wait_send()

            @pl.when(target < z)
            def _(target=target):
                l_copy(here, target).wait_send()

        @pl.when(narrow)
        def _():
            number = layer * 2 + narrow_at
            start = wide_per * 2 * LANES + narrow_at * LANES
            bs[number] = part[here, z, 1 - x]
            b_copy(number).start()
            out_ref[layer, :, pl.ds(pl.multiple_of(start, LANES), LANES)] = part[here, z, x]

        @pl.when(jnp.logical_not(narrow))
        def _():
            for half in range(2):
                start = wide_at * 2 * LANES + half * LANES
                out_ref[layer, :, pl.ds(pl.multiple_of(start, LANES), LANES)] = part[here, z, half]

        @pl.when(item + slots < items)
        def _():
            @pl.when(has_left)
            def _():
                signal(from_right, left)

            @pl.when(has_right)
            def _():
                signal(from_left, right)

    for item in range(1, AHEAD):
        send_wide(jnp.int32(item))

    @pl.loop(0, items + line - 1)
    def _(step):
        def guard(item, action):
            pl.when(jnp.logical_and(item >= 0, item < items))(lambda: action(item))

        guard(step + AHEAD, send_wide)
        guard(step - (line - 1), finish)
        for stage in reversed(range(1, line - 1)):
            guard(step - stage, functools.partial(hop, stage=stage))

        def begin(item):
            form(item)
            hop(item, 0)

        guard(step, begin)

    for number in range(2 * layers):
        b_copy(number).wait()
        start = wide_per * 2 * LANES + (number % 2) * LANES
        out_ref[number // 2, :, start : start + LANES] += br[number]

    def square_rows(index, total):
        layer = index // (rows // 8)
        at = pl.multiple_of(index % (rows // 8) * 8, 8)
        for piece in range(cols // LANES):
            value = out_ref[layer, pl.ds(at, 8), piece * LANES : (piece + 1) * LANES]
            total = total + value * value
        return total

    def spread(src, landing, send, recv, axis, index, size):
        copies = []
        for offset in range(1, size):
            copies.append(
                pltpu.make_async_remote_copy(
                    src_ref=src, dst_ref=landing.at[offset - 1],
                    send_sem=send.at[offset - 1], recv_sem=recv.at[offset - 1],
                    device_id={axis: lax.rem(index + offset, size)},
                    device_id_type=pl.DeviceIdType.MESH,
                )
            )
        for copy in copies:
            copy.start()
        for copy in copies:
            copy.wait()
        total = src[...]
        for offset in range(1, size):
            total = total + landing[offset - 1]
        return total

    own_sq[...] = lax.fori_loop(
        0, layers * rows // 8, square_rows, jnp.zeros((8, LANES), jnp.float32)
    )
    sum_sq[...] = spread(own_sq, col_sq, cs_sem, cr_sem, "col", mine, col_count)
    sq_ref[...] = spread(sum_sq, dp_sq, ds_sem, dr_sem, "dp", me, count)


def reduced_gradient(activations, cotangent, mesh_shape):
    count = mesh_shape["dp"]
    col_count = mesh_shape["col"]
    layers, tokens, cols = activations.shape
    line = count // 2
    rows = cotangent.shape[2] // count
    slots = line + 2
    cot = cotangent.reshape(layers, tokens, line, 2, rows).transpose(0, 3, 2, 4, 1)
    block = (line, 2, rows, LANES)
    dma = pltpu.SemaphoreType.DMA
    vmem = pl.BlockSpec(memory_space=pltpu.VMEM)
    return pl.pallas_call(
        functools.partial(reduce_kernel, count, col_count),
        out_shape=(
            jax.ShapeDtypeStruct((layers, rows, cols), jnp.float32),
            jax.ShapeDtypeStruct((8, LANES), jnp.float32),
        ),
        in_specs=[vmem, vmem],
        out_specs=(vmem, vmem),
        scratch_shapes=[
            pltpu.VMEM((XSLOTS,) + block, jnp.float32),
            pltpu.VMEM((XSLOTS,) + block, jnp.float32),
            pltpu.VMEM((slots,) + block, jnp.float32),
            pltpu.VMEM((slots, line + 1) + block[1:], jnp.float32),
            pltpu.VMEM((2 * layers, rows, LANES), jnp.float32),
            pltpu.VMEM((2 * layers, rows, LANES), jnp.float32),
            pltpu.VMEM((8, LANES), jnp.float32),
            pltpu.VMEM((8, LANES), jnp.float32),
            pltpu.VMEM((col_count - 1, 8, LANES), jnp.float32),
            pltpu.VMEM((count - 1, 8, LANES), jnp.float32),
            dma((XSLOTS,)), dma((XSLOTS,)),
            dma((slots, line)), dma((slots, line)), dma((slots, line)), dma((slots, line)),
            dma((2 * layers,)), dma((2 * layers,)),
            dma((col_count - 1,)), dma((col_count - 1,)), dma((count - 1,)), dma((count - 1,)),
            pltpu.SemaphoreType.REGULAR, pltpu.SemaphoreType.REGULAR, pltpu.SemaphoreType.REGULAR,
        ],
        compiler_params=pltpu.CompilerParams(
            collective_id=0, has_side_effects=True, vmem_limit_bytes=62 * 2**20
        ),
    )(cot, activations)


AHEAD_UNITS = 5
SEND_SLOTS = 6
ACT_SLOTS = 5
NARROW = 2
RELEASE = 3


def factor_kernel(
    count, col_count, cot_hbm, act_hbm, out_ref, sq_ref,
    cot_raw, act_raw, narrow_act, cot_t, act_cat, xs, xr, crx, part, arr, narrow_in, held,
    own_sq, sum_sq, col_sq, dp_sq,
    ld_sem, xs_sem, xr_sem, pr_sem, cs_sem, cr_sem, rs_sem, rr_sem, ls_sem, ll_sem, fs_sem, fr_sem,
    qs_sem, qr_sem, ds_sem, dr_sem, act_free, cot_free, from_right, from_left,
):
    layers, tokens, cols = act_hbm.shape
    half = cols // 2
    line = count // 2
    pair_rows = part.shape[2]
    rows = pair_rows // 2
    slots = part.shape[0]
    chunks = half // LANES
    first_chunks = chunks - NARROW // 2
    wides = first_chunks + (layers - 1) * chunks
    items = NARROW + wides
    first_units = first_chunks + line
    layer_units = chunks + line
    units = first_units + (layers - 1) * layer_units
    all_sent = items - chunks + line - 2
    groups = col_count // 2
    me = lax.axis_index("dp")
    mine = lax.axis_index("col")
    z = me // 2
    x = me % 2
    peer = 2 * z + 1 - x
    partner = mine + 1 - 2 * (mine % 2)
    right = jnp.minimum(z + 1, line - 1) * 2 + x
    left = jnp.maximum(z - 1, 0) * 2 + x
    has_right = z < line - 1
    has_left = z > 0
    mirror = line - 1 - z
    own_half = pl.multiple_of(x * half, LANES)
    peer_half = pl.multiple_of((1 - x) * half, LANES)

    def lanes(start, width=LANES):
        return pl.ds(pl.multiple_of(start, LANES), width)

    def signal(sem, where):
        pl.semaphore_signal(
            sem, inc=1, device_id={"dp": where}, device_id_type=pl.DeviceIdType.MESH
        )

    loads = []

    def load(src, dst):
        copy = pltpu.make_async_copy(src, dst, ld_sem.at[len(loads)])
        copy.start()
        loads.append(copy)

    def block_target(place):
        after = line - 1 - z
        rising = jnp.where(place < after, line - 1 - place, place - after)
        falling = jnp.where(place < z, place, line - 1 - (place - z))
        other = jnp.where(z < line // 2, rising, falling)
        return jnp.where(place < line - 1, other, z)

    for place in range(line):
        block = lanes(block_target(place) * pair_rows, pair_rows)
        load(cot_hbm.at[0, :, block], cot_raw.at[0, :, block])
    load(act_hbm.at[0, :, pl.ds(peer_half, half)], act_raw.at[0])
    for index in range(NARROW):
        start = (index % 2) * half + (chunks - 1 - index // 2) * LANES
        load(act_hbm.at[0, :, lanes(start)], narrow_act.at[index])
    for layer in range(layers):
        if layer > 0:
            load(cot_hbm.at[layer], cot_raw.at[layer])
            load(act_hbm.at[layer, :, pl.ds(peer_half, half)], act_raw.at[layer])
        load(act_hbm.at[layer, :, pl.ds(own_half, half)], act_cat.at[layer, pl.ds(0, tokens)])

    early_loads = line + 1 + NARROW

    barrier = pltpu.get_barrier_semaphore()
    for offset in range(1, count):
        signal(barrier, lax.rem(me + offset, count))
    for offset in range(1, col_count):
        pl.semaphore_signal(
            barrier, inc=1, device_id={"col": lax.rem(mine + offset, col_count)},
            device_id_type=pl.DeviceIdType.MESH,
        )
    pl.semaphore_wait(barrier, count + col_count - 2)

    def remote(src, dst, send, recv, where):
        return pltpu.make_async_remote_copy(
            src_ref=src, dst_ref=dst, send_sem=send, recv_sem=recv,
            device_id={"dp": where}, device_id_type=pl.DeviceIdType.MESH,
        )

    def describe(item):
        number = item - NARROW
        narrow = item < NARROW
        later = jnp.maximum(number - first_chunks, 0)
        layer = jnp.where(number < first_chunks, 0, 1 + later // chunks)
        chunk = jnp.where(number < first_chunks, number, later % chunks)
        return layer, narrow, chunk

    def unit_base(layer):
        return jnp.where(layer == 0, 0, first_units + (layer - 1) * layer_units)

    def act_number(layer, chunk):
        return jnp.where(layer == 0, chunk, first_chunks + (layer - 1) * chunks + chunk)

    def act_copy(unit, number):
        here = unit % SEND_SLOTS
        slot = number % ACT_SLOTS
        return remote(xs.at[here], xr.at[slot], xs_sem.at[here], xr_sem.at[slot], peer)

    def cot_copy(unit, place):
        here = unit % SEND_SLOTS
        return remote(xs.at[here], crx.at[place, mine], xs_sem.at[here], pr_sem.at[place], peer)

    def col_copy(place, owner, number, where):
        return pltpu.make_async_remote_copy(
            src_ref=crx.at[place, owner], dst_ref=crx.at[place, owner],
            send_sem=cs_sem.at[place, number], recv_sem=cr_sem.at[place, owner],
            device_id={"col": where}, device_id_type=pl.DeviceIdType.MESH,
        )

    def far(index):
        return lax.rem(mine + 2 * index, col_count)

    def r_copy(slot, target):
        return remote(
            part.at[slot, target], arr.at[slot, target + 1],
            rs_sem.at[slot, target], rr_sem.at[slot, target], right,
        )

    def l_copy(slot, target):
        return remote(
            part.at[slot, target], arr.at[slot, target],
            ls_sem.at[slot, target], ll_sem.at[slot, target], left,
        )

    def n_copy(item):
        where = narrow_in.at[jnp.minimum(item, NARROW - 1)]
        return remote(held.at[item], where, fs_sem.at[item], fr_sem.at[item], peer)

    def f_copy(item, side):
        layer, narrow, chunk = describe(item)
        where = out_ref.at[layer, :, lanes(side * half + chunk * LANES)]
        return remote(held.at[item], where, fs_sem.at[item], fr_sem.at[item], peer)

    def exchange(item):
        @pl.when(item < NARROW)
        def _():
            n_copy(item).start()

        @pl.when(item >= NARROW)
        def _():
            f_copy(item, x).start()

    def exchanged(step):
        done = jnp.minimum(step - (line - 1), RELEASE * (step - 1 - all_sent))
        return jnp.clip(done, 0, items)

    def send(unit):
        @pl.when(unit < units)
        def _():
            layer = jnp.where(unit < first_units, 0, 1 + (unit - first_units) // layer_units)
            index = unit - unit_base(layer)
            is_cot = jnp.logical_or(index < line - 1, index == 2 * line - 2)
            here = unit % SEND_SLOTS

            @pl.when(unit >= SEND_SLOTS)
            def _():
                act_copy(unit, 0).wait_send()

            @pl.when(is_cot)
            def _():
                place = jnp.minimum(index, line - 1)
                start = block_target(place) * pair_rows + mine * LANES
                xs[here] = cot_raw[layer, :, lanes(start)].astype(jnp.float32)

                @pl.when(layer > 0)
                def _():
                    pl.semaphore_wait(cot_free.at[place], 1)

                cot_copy(unit, place).start()

            @pl.when(jnp.logical_not(is_cot))
            def _():
                chunk = jnp.where(index < 2 * line - 2, index - (line - 1), index - line)
                number = act_number(layer, chunk)
                xs[here] = act_raw[layer, :, lanes(chunk * LANES)].astype(jnp.float32)

                @pl.when(number >= ACT_SLOTS)
                def _():
                    pl.semaphore_wait(act_free.at[number % ACT_SLOTS], 1)

                act_copy(unit, number).start()

    def forward(layer, place):
        cot_copy(0, place).wait_recv()
        for index in range(1, groups):
            col_copy(place, mine, index, far(index)).start()
        col_copy(place, mine, 0, partner).start()
        send(unit_base(layer) + jnp.where(place < line - 1, place, 2 * line - 2) + AHEAD_UNITS)

    def relay(place):
        for index in range(1, groups):
            col_copy(place, far(index), groups - 1 + index, partner).wait_recv()
            col_copy(place, far(index), groups - 1 + index, partner).start()

    def prepare(layer, place):
        base = block_target(place) * pair_rows

        @pl.loop(0, col_count)
        def _(member):
            start = base + member * LANES
            value = cot_raw[layer, :, lanes(start)].astype(jnp.float32)
            cot_t[layer, lanes(start), pl.ds(0, tokens)] = value.T.astype(jnp.bfloat16)

    def absorb(layer, place):
        @pl.when(layer > 0)
        def _():
            prepare(layer, place)

        base = block_target(place) * pair_rows
        col_copy(place, partner, 0, partner).wait_recv()
        for index in range(1, groups):
            col_copy(place, lax.rem(partner + 2 * index, col_count), 0, partner).wait_recv()

        @pl.loop(0, col_count)
        def _(owner):
            source = crx[place, owner]
            cot_t[layer, lanes(base + owner * LANES), pl.ds(tokens, tokens)] = source.T.astype(jnp.bfloat16)

        for number in range(col_count - 1):
            col_copy(place, mine, number, partner).wait_send()

        @pl.when(layer < layers - 1)
        def _():
            signal(cot_free.at[place], peer)

    def take(layer, chunk):
        number = act_number(layer, chunk)
        slot = number % ACT_SLOTS
        act_copy(0, number).wait_recv()
        act_cat[layer, pl.ds(tokens, tokens), lanes(chunk * LANES)] = xr[slot].astype(jnp.bfloat16)

        @pl.when(number + ACT_SLOTS < wides)
        def _():
            signal(act_free.at[slot], peer)

        index = jnp.where(chunk < line - 1, chunk + line - 1, chunk + line)
        send(unit_base(layer) + index + AHEAD_UNITS)

    def form(item, target):
        layer, narrow, chunk = describe(item)
        here = item % slots
        at = pl.ds(pl.multiple_of(target * pair_rows, LANES), pair_rows)

        @pl.when(narrow)
        def _():
            part[here, target] = jnp.dot(
                cot_t[0, at, pl.ds(0, tokens)], narrow_act[jnp.minimum(item, NARROW - 1)],
                preferred_element_type=jnp.float32,
            )

        @pl.when(jnp.logical_not(narrow))
        def _():
            part[here, target] = jnp.dot(
                cot_t[layer, at, :], act_cat[layer, :, lanes(chunk * LANES)],
                preferred_element_type=jnp.float32,
            )

    def opens(item):
        layer, narrow, chunk = describe(item)
        return layer, jnp.logical_and(jnp.logical_not(narrow), chunk == 0)

    def ready(item, place):
        @pl.when(item == 0)
        def _():
            prepare(0, place)

        layer, first = opens(item)

        @pl.when(first)
        def _():
            if place == 0:
                @pl.when(layer == 0)
                def _():
                    for early in range(2):
                        forward(layer, early)

                for early in range(2, line - 1):
                    forward(layer, early)
                for early in range(2):
                    relay(early)
            if place == line - 1:
                relay(place)
            absorb(layer, place)

    def hop(item, stage):
        here = item % slots

        @pl.when(z <= stage)
        def _():
            target = line - 1 - stage + z
            form(item, target)
            if stage > 0:
                @pl.when(has_left)
                def _():
                    r_copy(here, target).wait_recv()
                    part[here, target] += arr[here, target + 1]

            r_copy(here, target).start()

        @pl.when(mirror <= stage)
        def _():
            target = stage - mirror
            form(item, target)
            if stage > 0:
                @pl.when(has_right)
                def _():
                    l_copy(here, target).wait_recv()
                    part[here, target] += arr[here, target]

            l_copy(here, target).start()

    def begin(item):
        layer, narrow, chunk = describe(item)
        ready(item, 0)

        @pl.when(jnp.logical_not(narrow))
        def _():
            take(layer, chunk)

        @pl.when(item >= slots)
        def _():
            @pl.when(has_right)
            def _():
                pl.semaphore_wait(from_right, 1)

            @pl.when(has_left)
            def _():
                pl.semaphore_wait(from_left, 1)

        hop(item, 0)

        @pl.when(item == 1)
        def _():
            for copy in loads[early_loads:]:
                copy.wait()

        @pl.when(jnp.logical_and(jnp.logical_not(narrow), chunk == 0))
        def _():
            for early in range(2, line - 1):
                relay(early)

        next_layer, next_first = opens(item + 1)

        @pl.when(jnp.logical_and(next_first, jnp.logical_and(next_layer > 0, item + 1 < items)))
        def _():
            for place in range(2):
                forward(next_layer, place)

        @pl.when(jnp.logical_and(jnp.logical_not(narrow), chunk == line - 2))
        def _():
            forward(layer, line - 1)

    def middle(item, stage):
        ready(item, stage)
        hop(item, stage)

    def finish(item):
        layer, narrow, chunk = describe(item)
        here = item % slots
        ready(item, line - 1)

        form(item, z)

        @pl.when(has_left)
        def _():
            r_copy(here, z).wait_recv()
            part[here, z] += arr[here, z + 1]

        @pl.when(has_right)
        def _():
            l_copy(here, z).wait_recv()
            part[here, z] += arr[here, z]

        for target in range(line):
            @pl.when(target > z)
            def _(target=target):
                r_copy(here, target).wait_send()

            @pl.when(target < z)
            def _(target=target):
                l_copy(here, target).wait_send()

        kept = pl.ds(pl.multiple_of(x * rows, 8), rows)
        held[item] = part[here, z, pl.ds(pl.multiple_of((1 - x) * rows, 8), rows)]

        @pl.when(narrow)
        def _():
            start = (item % 2) * half + (chunks - 1 - item // 2) * LANES
            out_ref[0, :, lanes(start)] = part[here, z, kept]

        @pl.when(jnp.logical_not(narrow))
        def _():
            out_ref[layer, :, lanes(own_half + chunk * LANES)] = part[here, z, kept]

        @pl.when(item + slots < items)
        def _():
            @pl.when(has_left)
            def _():
                signal(from_right, left)

            @pl.when(has_right)
            def _():
                signal(from_left, right)

    for unit in range(line - 1):
        loads[unit].wait()
        send(jnp.int32(unit))
    for copy in loads[line - 1 : early_loads]:
        copy.wait()
    for unit in range(line - 1, AHEAD_UNITS):
        send(jnp.int32(unit))

    @pl.loop(0, items + line)
    def _(step):
        def guard(turn, action):
            item = turn - (turn > NARROW).astype(jnp.int32)
            real = jnp.logical_and(turn >= 0, turn != NARROW)
            pl.when(jnp.logical_and(real, item < items))(lambda: action(item))

        for stage in reversed(range(1, line - 1)):
            guard(step - stage, functools.partial(middle, stage=stage))
        guard(step, begin)
        guard(step - (line - 1), finish)

        @pl.loop(exchanged(step - 1), exchanged(step))
        def _(item):
            exchange(item)

    @pl.loop(units - SEND_SLOTS, units)
    def _(unit):
        act_copy(unit, 0).wait_send()

    @pl.loop(0, items)
    def _(item):
        n_copy(item).wait_send()

    for item in range(NARROW):
        n_copy(item).wait_recv()
        start = (item % 2) * half + (chunks - 1 - item // 2) * LANES
        out_ref[0, :, start : start + LANES] += narrow_in[item]

    @pl.loop(NARROW, items)
    def _(item):
        f_copy(item, 1 - x).wait_recv()

    def square_rows(index, total):
        layer = index // (rows // 8)
        at = pl.multiple_of(index % (rows // 8) * 8, 8)
        for piece in range(cols // LANES):
            value = out_ref[layer, pl.ds(at, 8), piece * LANES : (piece + 1) * LANES]
            total = total + value * value
        return total

    def spread(src, landing, send_sems, recv_sems, axis, index, size):
        copies = []
        for offset in range(1, size):
            copies.append(
                pltpu.make_async_remote_copy(
                    src_ref=src, dst_ref=landing.at[offset - 1],
                    send_sem=send_sems.at[offset - 1], recv_sem=recv_sems.at[offset - 1],
                    device_id={axis: lax.rem(index + offset, size)},
                    device_id_type=pl.DeviceIdType.MESH,
                )
            )
        for copy in copies:
            copy.start()
        for copy in copies:
            copy.wait()
        total = src[...]
        for offset in range(1, size):
            total = total + landing[offset - 1]
        return total

    own_sq[...] = lax.fori_loop(
        0, layers * rows // 8, square_rows, jnp.zeros((8, LANES), jnp.float32)
    )
    sum_sq[...] = spread(own_sq, col_sq, qs_sem, qr_sem, "col", mine, col_count)
    sq_ref[...] = spread(sum_sq, dp_sq, ds_sem, dr_sem, "dp", me, count)


def factor_gradient(activations, cotangent, mesh_shape):
    count = mesh_shape["dp"]
    col_count = mesh_shape["col"]
    layers, tokens, cols = activations.shape
    line = count // 2
    features = cotangent.shape[2]
    rows = features // count
    half = cols // 2
    slots = line + 1
    items = NARROW + layers * (half // LANES) - NARROW // 2
    piece = (tokens, LANES)
    f32, bf16 = jnp.float32, jnp.bfloat16
    dma = pltpu.SemaphoreType.DMA
    regular = pltpu.SemaphoreType.REGULAR
    vmem = pl.BlockSpec(memory_space=pltpu.VMEM)
    hbm = pl.BlockSpec(memory_space=pl.ANY)
    return pl.pallas_call(
        functools.partial(factor_kernel, count, col_count),
        out_shape=(
            jax.ShapeDtypeStruct((layers, rows, cols), f32),
            jax.ShapeDtypeStruct((8, LANES), f32),
        ),
        in_specs=[hbm, hbm],
        out_specs=(vmem, vmem),
        scratch_shapes=[
            pltpu.VMEM((layers, tokens, features), bf16),
            pltpu.VMEM((layers, tokens, half), bf16),
            pltpu.VMEM((NARROW,) + piece, bf16),
            pltpu.VMEM((layers, features, 2 * tokens), bf16),
            pltpu.VMEM((layers, 2 * tokens, half), bf16),
            pltpu.VMEM((SEND_SLOTS,) + piece, f32),
            pltpu.VMEM((ACT_SLOTS,) + piece, f32),
            pltpu.VMEM((line, col_count) + piece, f32),
            pltpu.VMEM((slots, line, 2 * rows, LANES), f32),
            pltpu.VMEM((slots, line + 1, 2 * rows, LANES), f32),
            pltpu.VMEM((NARROW, rows, LANES), f32),
            pltpu.VMEM((items, rows, LANES), f32),
            pltpu.VMEM((8, LANES), f32),
            pltpu.VMEM((8, LANES), f32),
            pltpu.VMEM((col_count - 1, 8, LANES), f32),
            pltpu.VMEM((count - 1, 8, LANES), f32),
            dma((NARROW + line + 3 * layers - 1,)),
            dma((SEND_SLOTS,)), dma((ACT_SLOTS,)), dma((line,)),
            dma((line, col_count - 1)), dma((line, col_count)),
            dma((slots, line)), dma((slots, line)), dma((slots, line)), dma((slots, line)),
            dma((items,)), dma((items,)),
            dma((col_count - 1,)), dma((col_count - 1,)), dma((count - 1,)), dma((count - 1,)),
            regular((ACT_SLOTS,)), regular((line,)), regular, regular,
        ],
        compiler_params=pltpu.CompilerParams(
            collective_id=0, has_side_effects=True, vmem_limit_bytes=67043328
        ),
    )(cotangent, activations)


def fits_factors(activations, cotangent, mesh_shape):
    count = mesh_shape["dp"]
    line = count // 2
    rows = cotangent.shape[2] // count
    chunks = activations.shape[2] // (2 * LANES)
    aligned = activations.shape[1] % LANES == 0 and activations.shape[2] % (2 * LANES) == 0
    return aligned and line >= 3 and 2 * rows == LANES * mesh_shape["col"] and mesh_shape["col"] % 2 == 0 and chunks - NARROW // 2 > line


def local(
    mesh_shape, activations, cotangent, master_weights, moment_codes, square_codes, moment_scales, square_scales
):
    layer_count = activations.shape[0]
    shard_rows = master_weights.shape[1]
    shard_cols = master_weights.shape[2]
    block_count = moment_scales.shape[2]
    reduce = factor_gradient if fits_factors(activations, cotangent, mesh_shape) else reduced_gradient
    gradient, squares = reduce(activations, cotangent, mesh_shape)
    total_sq = jnp.sum(squares)
    rms = jnp.sqrt(total_sq / float(LAYERS * KV * D) + norm_eps)
    clip_factor = jnp.minimum(1.0, 1.0 / rms)
    correct_one = 1.0 - beta_one**STEP
    correct_two = 1.0 - beta_two**STEP
    own_block = lax.axis_index("col") * shard_cols // BLOCK
    selector = (jnp.arange(block_count, dtype=jnp.int32) == own_block).astype(jnp.float32)
    outs_weights, outs_mcode, outs_scode, outs_mscale, outs_sscale = ([], [], [], [], [])
    for layer_index in range(layer_count):
        moment_scale = jnp.sum(moment_scales[layer_index] * selector, axis=1)
        square_scale = jnp.sum(square_scales[layer_index] * selector, axis=1)
        old_moment = moment_codes[layer_index].astype(jnp.float32) * moment_scale[:, None]
        old_square = square_codes[layer_index].astype(jnp.float32) * square_scale[:, None]
        grad_now = clip_factor * gradient[layer_index]
        new_moment = beta_one * old_moment + (1.0 - beta_one) * grad_now
        new_square = beta_two * old_square + (1.0 - beta_two) * grad_now * grad_now
        moment_part = jnp.max(jnp.abs(new_moment), axis=1)[:, None] * selector
        square_part = jnp.max(new_square, axis=1)[:, None] * selector
        moment, square, moment_part, square_part = (
            new_moment,
            new_square,
            moment_part,
            square_part,
        )
        moment_max, square_max = lax.pmax((moment_part, square_part), "col")
        moment_div = jnp.sum(moment_max * selector, axis=1)[:, None]
        square_div = jnp.sum(square_max * selector, axis=1)[:, None]
        moment_out = (moment / (moment_div + scale_eps)).astype(jnp.bfloat16)
        square_out = (square / (square_div + scale_eps)).astype(jnp.bfloat16)
        ratio = moment / correct_one / (jnp.sqrt(square / correct_two) + adam_eps)
        weights = master_weights[layer_index]
        results = (weights - learn_rate * (decay_rate * weights + ratio), moment_out, square_out)
        outs_weights.append(results[0])
        outs_mcode.append(results[1])
        outs_scode.append(results[2])
        outs_mscale.append(moment_max)
        outs_sscale.append(square_max)
    return (
        jnp.stack(outs_weights),
        jnp.stack(outs_mcode),
        jnp.stack(outs_scode),
        jnp.stack(outs_mscale),
        jnp.stack(outs_sscale),
    )


def solution(mesh):
    in_specs = (
        P(None, "dp", "col"),
        P(None, "dp", None),
        P(None, "dp", "col"),
        P(None, "dp", "col"),
        P(None, "dp", "col"),
        P(None, "dp", None),
        P(None, "dp", None),
    )
    out_specs = (
        P(None, "dp", "col"),
        P(None, "dp", "col"),
        P(None, "dp", "col"),
        P(None, "dp", None),
        P(None, "dp", None),
    )
    return jax.shard_map(functools.partial(local, dict(mesh.shape)), mesh=mesh, in_specs=in_specs, out_specs=out_specs, check_vma=False)
```

```python
import functools

import jax
import jax.numpy as jnp
from jax import lax
from jax.experimental import pallas as pl
from jax.experimental.pallas import tpu as pltpu
from jax.sharding import PartitionSpec as P

D = 8192
KV = 2048
BLOCK = 2048
LAYERS = 2
STEP = 10


beta_one = 0.9
beta_two = 0.999
learn_rate = 0.001
decay_rate = 0.1
adam_eps = 1e-08
scale_eps = 1e-06
norm_eps = 1e-06

LANES = 128
AHEAD = 3
XSLOTS = 4


def reduce_kernel(
    count, col_count, cot_ref, act_ref, out_ref, sq_ref,
    xs, xr, part, arr, bs, br, own_sq, sum_sq, col_sq, dp_sq,
    xs_sem, xr_sem, rs_sem, rr_sem, ls_sem, ll_sem, bs_sem, br_sem,
    cs_sem, cr_sem, ds_sem, dr_sem, x_free, from_right, from_left,
):
    layers, pairs, line, rows, tokens = cot_ref.shape
    cols = act_ref.shape[2]
    slots = part.shape[0]
    wide_per = cols // (2 * LANES) - 1
    per_layer = wide_per + 2
    period = (per_layer + 1) // 2
    items = layers * per_layer
    wides = layers * wide_per
    me = lax.axis_index("dp")
    z = me // 2
    x = me % 2
    peer = 2 * z + 1 - x
    right = jnp.minimum(z + 1, line - 1) * 2 + x
    left = jnp.maximum(z - 1, 0) * 2 + x
    has_right = z < line - 1
    has_left = z > 0
    mirror = line - 1 - z

    def signal(sem, where):
        pl.semaphore_signal(
            sem, inc=1, device_id={"dp": where}, device_id_type=pl.DeviceIdType.MESH
        )

    barrier = pltpu.get_barrier_semaphore()
    mine = lax.axis_index("col")
    for offset in range(1, count):
        signal(barrier, lax.rem(me + offset, count))
    for offset in range(1, col_count):
        pl.semaphore_signal(
            barrier, inc=1, device_id={"col": lax.rem(mine + offset, col_count)},
            device_id_type=pl.DeviceIdType.MESH,
        )
    pl.semaphore_wait(barrier, count + col_count - 2)

    def remote(src, dst, send, recv, where):
        return pltpu.make_async_remote_copy(
            src_ref=src, dst_ref=dst, send_sem=send, recv_sem=recv,
            device_id={"dp": where}, device_id_type=pl.DeviceIdType.MESH,
        )

    def describe(item):
        layer = item // per_layer
        place = item % per_layer
        narrow = place % period == 0
        wide_at = place - (place + period - 1) // period
        narrow_at = place // period
        return layer, narrow, wide_at, narrow_at

    def x_copy(number):
        slot = number % XSLOTS
        return remote(xs.at[slot], xr.at[slot], xs_sem.at[slot], xr_sem.at[slot], peer)

    def r_copy(slot, target):
        return remote(
            part.at[slot, target], arr.at[slot, target + 1],
            rs_sem.at[slot, target], rr_sem.at[slot, target], right,
        )

    def l_copy(slot, target):
        return remote(
            part.at[slot, target], arr.at[slot, target],
            ls_sem.at[slot, target], ll_sem.at[slot, target], left,
        )

    def b_copy(number):
        return remote(
            bs.at[number], br.at[number], bs_sem.at[number], br_sem.at[number], peer
        )

    def product(layer, pair, target, start, width):
        return jnp.dot(
            cot_ref[layer, pair, target],
            act_ref[layer, :, pl.ds(pl.multiple_of(start, LANES), width)],
            preferred_element_type=jnp.float32,
        )

    def send_wide(item):
        layer, narrow, wide_at, _ = describe(item)

        @pl.when(jnp.logical_not(narrow))
        def _():
            number = layer * wide_per + wide_at
            slot = number % XSLOTS

            @pl.loop(0, line)
            def _(target):
                value = product(layer, 1 - x, target, wide_at * 2 * LANES, 2 * LANES)
                xs[slot, target, 0] = value[:, :LANES]
                xs[slot, target, 1] = value[:, LANES:]

            @pl.when(number >= XSLOTS)
            def _():
                pl.semaphore_wait(x_free, 1)

            x_copy(number).start()

    def form(item):
        layer, narrow, wide_at, narrow_at = describe(item)
        here = item % slots

        @pl.when(item >= slots)
        def _():
            @pl.when(has_right)
            def _():
                pl.semaphore_wait(from_right, 1)

            @pl.when(has_left)
            def _():
                pl.semaphore_wait(from_left, 1)

        @pl.when(narrow)
        def _():
            start = wide_per * 2 * LANES + narrow_at * LANES

            @pl.loop(0, line)
            def _(target):
                part[here, target, 0] = product(layer, 0, target, start, LANES)
                part[here, target, 1] = product(layer, 1, target, start, LANES)

        @pl.when(jnp.logical_not(narrow))
        def _():
            number = layer * wide_per + wide_at
            slot = number % XSLOTS
            x_copy(number).wait()

            @pl.loop(0, line)
            def _(target):
                value = product(layer, x, target, wide_at * 2 * LANES, 2 * LANES)
                part[here, target, 0] = value[:, :LANES] + xr[slot, target, 0]
                part[here, target, 1] = value[:, LANES:] + xr[slot, target, 1]

            @pl.when(number + XSLOTS < wides)
            def _():
                signal(x_free, peer)

    def hop(item, stage):
        here = item % slots

        @pl.when(z <= stage)
        def _():
            target = line - 1 - stage + z
            if stage > 0:
                @pl.when(has_left)
                def _():
                    r_copy(here, target).wait_recv()
                    part[here, target] += arr[here, target + 1]

            r_copy(here, target).start()

        @pl.when(mirror <= stage)
        def _():
            target = stage - mirror
            if stage > 0:
                @pl.when(has_right)
                def _():
                    l_copy(here, target).wait_recv()
                    part[here, target] += arr[here, target]

            l_copy(here, target).start()

    def finish(item):
        layer, narrow, wide_at, narrow_at = describe(item)
        here = item % slots

        @pl.when(has_left)
        def _():
            r_copy(here, z).wait_recv()
            part[here, z] += arr[here, z + 1]

        @pl.when(has_right)
        def _():
            l_copy(here, z).wait_recv()
            part[here, z] += arr[here, z]

        for target in range(line):
            @pl.when(target > z)
            def _(target=target):
                r_copy(here, target).wait_send()

            @pl.when(target < z)
            def _(target=target):
                l_copy(here, target).wait_send()

        @pl.when(narrow)
        def _():
            number = layer * 2 + narrow_at
            start = wide_per * 2 * LANES + narrow_at * LANES
            bs[number] = part[here, z, 1 - x]
            b_copy(number).start()
            out_ref[layer, :, pl.ds(pl.multiple_of(start, LANES), LANES)] = part[here, z, x]

        @pl.when(jnp.logical_not(narrow))
        def _():
            for half in range(2):
                start = wide_at * 2 * LANES + half * LANES
                out_ref[layer, :, pl.ds(pl.multiple_of(start, LANES), LANES)] = part[here, z, half]

        @pl.when(item + slots < items)
        def _():
            @pl.when(has_left)
            def _():
                signal(from_right, left)

            @pl.when(has_right)
            def _():
                signal(from_left, right)

    for item in range(1, AHEAD):
        send_wide(jnp.int32(item))

    @pl.loop(0, items + line - 1)
    def _(step):
        def guard(item, action):
            pl.when(jnp.logical_and(item >= 0, item < items))(lambda: action(item))

        guard(step + AHEAD, send_wide)
        guard(step - (line - 1), finish)
        for stage in reversed(range(1, line - 1)):
            guard(step - stage, functools.partial(hop, stage=stage))

        def begin(item):
            form(item)
            hop(item, 0)

        guard(step, begin)

    for number in range(2 * layers):
        b_copy(number).wait()
        start = wide_per * 2 * LANES + (number % 2) * LANES
        out_ref[number // 2, :, start : start + LANES] += br[number]

    def square_rows(index, total):
        layer = index // (rows // 8)
        at = pl.multiple_of(index % (rows // 8) * 8, 8)
        for piece in range(cols // LANES):
            value = out_ref[layer, pl.ds(at, 8), piece * LANES : (piece + 1) * LANES]
            total = total + value * value
        return total

    def spread(src, landing, send, recv, axis, index, size):
        copies = []
        for offset in range(1, size):
            copies.append(
                pltpu.make_async_remote_copy(
                    src_ref=src, dst_ref=landing.at[offset - 1],
                    send_sem=send.at[offset - 1], recv_sem=recv.at[offset - 1],
                    device_id={axis: lax.rem(index + offset, size)},
                    device_id_type=pl.DeviceIdType.MESH,
                )
            )
        for copy in copies:
            copy.start()
        for copy in copies:
            copy.wait()
        total = src[...]
        for offset in range(1, size):
            total = total + landing[offset - 1]
        return total

    own_sq[...] = lax.fori_loop(
        0, layers * rows // 8, square_rows, jnp.zeros((8, LANES), jnp.float32)
    )
    sum_sq[...] = spread(own_sq, col_sq, cs_sem, cr_sem, "col", mine, col_count)
    sq_ref[...] = spread(sum_sq, dp_sq, ds_sem, dr_sem, "dp", me, count)


def reduced_gradient(activations, cotangent, mesh_shape):
    count = mesh_shape["dp"]
    col_count = mesh_shape["col"]
    layers, tokens, cols = activations.shape
    line = count // 2
    rows = cotangent.shape[2] // count
    slots = line + 2
    cot = cotangent.reshape(layers, tokens, line, 2, rows).transpose(0, 3, 2, 4, 1)
    block = (line, 2, rows, LANES)
    dma = pltpu.SemaphoreType.DMA
    vmem = pl.BlockSpec(memory_space=pltpu.VMEM)
    return pl.pallas_call(
        functools.partial(reduce_kernel, count, col_count),
        out_shape=(
            jax.ShapeDtypeStruct((layers, rows, cols), jnp.float32),
            jax.ShapeDtypeStruct((8, LANES), jnp.float32),
        ),
        in_specs=[vmem, vmem],
        out_specs=(vmem, vmem),
        scratch_shapes=[
            pltpu.VMEM((XSLOTS,) + block, jnp.float32),
            pltpu.VMEM((XSLOTS,) + block, jnp.float32),
            pltpu.VMEM((slots,) + block, jnp.float32),
            pltpu.VMEM((slots, line + 1) + block[1:], jnp.float32),
            pltpu.VMEM((2 * layers, rows, LANES), jnp.float32),
            pltpu.VMEM((2 * layers, rows, LANES), jnp.float32),
            pltpu.VMEM((8, LANES), jnp.float32),
            pltpu.VMEM((8, LANES), jnp.float32),
            pltpu.VMEM((col_count - 1, 8, LANES), jnp.float32),
            pltpu.VMEM((count - 1, 8, LANES), jnp.float32),
            dma((XSLOTS,)), dma((XSLOTS,)),
            dma((slots, line)), dma((slots, line)), dma((slots, line)), dma((slots, line)),
            dma((2 * layers,)), dma((2 * layers,)),
            dma((col_count - 1,)), dma((col_count - 1,)), dma((count - 1,)), dma((count - 1,)),
            pltpu.SemaphoreType.REGULAR, pltpu.SemaphoreType.REGULAR, pltpu.SemaphoreType.REGULAR,
        ],
        compiler_params=pltpu.CompilerParams(
            collective_id=0, has_side_effects=True, vmem_limit_bytes=62 * 2**20
        ),
    )(cot, activations)


AHEAD_UNITS = 5
SEND_SLOTS = 6
ACT_SLOTS = 5
NARROW = 2
RELEASE = 3
PEAK_ROWS = 32
APPLY_ROWS = 64


def factor_kernel(
    count, col_count, cot_hbm, act_hbm, weights_hbm, moments_hbm, squares_hbm, moment_scale, square_scale,
    new_weights, new_moments, new_squares, new_moment_scale, new_square_scale, grad,
    scale_rows, peak, peak_rows,
    cot_raw, act_raw, narrow_act, cot_t, act_cat, xs, xr, crx, part, arr, narrow_in, held,
    own_sq, sum_sq, col_sq, dp_sq,
    ld_sem, w_in, w_out, c_in, c_out, ms_sem, mr_sem, xs_sem, xr_sem, pr_sem, cs_sem, cr_sem, rs_sem, rr_sem, ls_sem, ll_sem, fs_sem, fr_sem,
    qs_sem, qr_sem, ds_sem, dr_sem, act_free, cot_free, from_right, from_left,
):
    layers, tokens, cols = act_hbm.shape
    half = cols // 2
    line = count // 2
    pair_rows = part.shape[2]
    rows = pair_rows // 2
    slots = part.shape[0]
    chunks = half // LANES
    first_chunks = chunks - NARROW // 2
    wides = first_chunks + (layers - 1) * chunks
    items = NARROW + wides
    first_units = first_chunks + line
    layer_units = chunks + line
    units = first_units + (layers - 1) * layer_units
    all_sent = items - chunks + line - 2
    groups = col_count // 2
    pieces = cols // LANES
    features = cot_hbm.shape[2]
    me = lax.axis_index("dp")
    mine = lax.axis_index("col")
    z = me // 2
    x = me % 2
    peer = 2 * z + 1 - x
    partner = mine + 1 - 2 * (mine % 2)
    right = jnp.minimum(z + 1, line - 1) * 2 + x
    left = jnp.maximum(z - 1, 0) * 2 + x
    has_right = z < line - 1
    has_left = z > 0
    mirror = line - 1 - z
    own_half = pl.multiple_of(x * half, LANES)
    peer_half = pl.multiple_of((1 - x) * half, LANES)

    def lanes(start, width=LANES):
        return pl.ds(pl.multiple_of(start, LANES), width)

    def signal(sem, where):
        pl.semaphore_signal(
            sem, inc=1, device_id={"dp": where}, device_id_type=pl.DeviceIdType.MESH
        )

    loads = []

    def load(src, dst):
        copy = pltpu.make_async_copy(src, dst, ld_sem.at[len(loads)])
        copy.start()
        loads.append(copy)

    def block_target(place):
        after = line - 1 - z
        rising = jnp.where(place < after, line - 1 - place, place - after)
        falling = jnp.where(place < z, place, line - 1 - (place - z))
        other = jnp.where(z < line // 2, rising, falling)
        return jnp.where(place < line - 1, other, z)

    for place in range(line):
        block = lanes(block_target(place) * pair_rows, pair_rows)
        load(cot_hbm.at[0, :, block], cot_raw.at[0, :, block])
    load(act_hbm.at[0, :, pl.ds(peer_half, half)], act_raw.at[0])
    for index in range(NARROW):
        start = (index % 2) * half + (chunks - 1 - index // 2) * LANES
        load(act_hbm.at[0, :, lanes(start)], narrow_act.at[index])
    for layer in range(layers):
        if layer > 0:
            load(cot_hbm.at[layer], cot_raw.at[layer])
            load(act_hbm.at[layer, :, pl.ds(peer_half, half)], act_raw.at[layer])
        load(act_hbm.at[layer, :, pl.ds(own_half, half)], act_cat.at[layer, pl.ds(0, tokens)])

    early_loads = line + 1 + NARROW

    barrier = pltpu.get_barrier_semaphore()
    for offset in range(1, count):
        signal(barrier, lax.rem(me + offset, count))
    for offset in range(1, col_count):
        pl.semaphore_signal(
            barrier, inc=1, device_id={"col": lax.rem(mine + offset, col_count)},
            device_id_type=pl.DeviceIdType.MESH,
        )
    pl.semaphore_wait(barrier, count + col_count - 2)

    def remote(src, dst, send, recv, where):
        return pltpu.make_async_remote_copy(
            src_ref=src, dst_ref=dst, send_sem=send, recv_sem=recv,
            device_id={"dp": where}, device_id_type=pl.DeviceIdType.MESH,
        )

    def describe(item):
        number = item - NARROW
        narrow = item < NARROW
        later = jnp.maximum(number - first_chunks, 0)
        layer = jnp.where(number < first_chunks, 0, 1 + later // chunks)
        chunk = jnp.where(number < first_chunks, number, later % chunks)
        return layer, narrow, chunk

    def unit_base(layer):
        return jnp.where(layer == 0, 0, first_units + (layer - 1) * layer_units)

    def act_number(layer, chunk):
        return jnp.where(layer == 0, chunk, first_chunks + (layer - 1) * chunks + chunk)

    def act_copy(unit, number):
        here = unit % SEND_SLOTS
        slot = number % ACT_SLOTS
        return remote(xs.at[here], xr.at[slot], xs_sem.at[here], xr_sem.at[slot], peer)

    def cot_copy(unit, place):
        here = unit % SEND_SLOTS
        return remote(xs.at[here], crx.at[place, mine], xs_sem.at[here], pr_sem.at[place], peer)

    def col_copy(place, owner, number, where):
        return pltpu.make_async_remote_copy(
            src_ref=crx.at[place, owner], dst_ref=crx.at[place, owner],
            send_sem=cs_sem.at[place, number], recv_sem=cr_sem.at[place, owner],
            device_id={"col": where}, device_id_type=pl.DeviceIdType.MESH,
        )

    def far(index):
        return lax.rem(mine + 2 * index, col_count)

    def r_copy(slot, target):
        return remote(
            part.at[slot, target], arr.at[slot, target + 1],
            rs_sem.at[slot, target], rr_sem.at[slot, target], right,
        )

    def l_copy(slot, target):
        return remote(
            part.at[slot, target], arr.at[slot, target],
            ls_sem.at[slot, target], ll_sem.at[slot, target], left,
        )

    def n_copy(item):
        where = narrow_in.at[jnp.minimum(item, NARROW - 1)]
        return remote(held.at[item], where, fs_sem.at[item], fr_sem.at[item], peer)

    def f_copy(item, side):
        layer, narrow, chunk = describe(item)
        where = grad.at[layer, :, lanes(side * half + chunk * LANES)]
        return remote(held.at[item], where, fs_sem.at[item], fr_sem.at[item], peer)

    def exchange(item):
        @pl.when(item < NARROW)
        def _():
            n_copy(item).start()

        @pl.when(item >= NARROW)
        def _():
            f_copy(item, x).start()

    def exchanged(step):
        done = jnp.minimum(step - (line - 1), RELEASE * (step - 1 - all_sent))
        return jnp.clip(done, 0, items)

    def send(unit):
        @pl.when(unit < units)
        def _():
            layer = jnp.where(unit < first_units, 0, 1 + (unit - first_units) // layer_units)
            index = unit - unit_base(layer)
            is_cot = jnp.logical_or(index < line - 1, index == 2 * line - 2)
            here = unit % SEND_SLOTS

            @pl.when(unit >= SEND_SLOTS)
            def _():
                act_copy(unit, 0).wait_send()

            @pl.when(is_cot)
            def _():
                place = jnp.minimum(index, line - 1)
                start = block_target(place) * pair_rows + mine * LANES
                xs[here] = cot_raw[layer, :, lanes(start)].astype(jnp.float32)

                @pl.when(layer > 0)
                def _():
                    pl.semaphore_wait(cot_free.at[place], 1)

                cot_copy(unit, place).start()

            @pl.when(jnp.logical_not(is_cot))
            def _():
                chunk = jnp.where(index < 2 * line - 2, index - (line - 1), index - line)
                number = act_number(layer, chunk)
                xs[here] = act_raw[layer, :, lanes(chunk * LANES)].astype(jnp.float32)

                @pl.when(number >= ACT_SLOTS)
                def _():
                    pl.semaphore_wait(act_free.at[number % ACT_SLOTS], 1)

                act_copy(unit, number).start()

    def forward(layer, place):
        cot_copy(0, place).wait_recv()
        for index in range(1, groups):
            col_copy(place, mine, index, far(index)).start()
        col_copy(place, mine, 0, partner).start()
        send(unit_base(layer) + jnp.where(place < line - 1, place, 2 * line - 2) + AHEAD_UNITS)

    def relay(place):
        for index in range(1, groups):
            col_copy(place, far(index), groups - 1 + index, partner).wait_recv()
            col_copy(place, far(index), groups - 1 + index, partner).start()

    def prepare(layer, place):
        base = block_target(place) * pair_rows

        @pl.loop(0, col_count)
        def _(member):
            start = base + member * LANES
            value = cot_raw[layer, :, lanes(start)].astype(jnp.float32)
            cot_t[layer, lanes(start), pl.ds(0, tokens)] = value.T.astype(jnp.bfloat16)

    def absorb(layer, place):
        @pl.when(layer > 0)
        def _():
            prepare(layer, place)

        base = block_target(place) * pair_rows
        col_copy(place, partner, 0, partner).wait_recv()
        for index in range(1, groups):
            col_copy(place, lax.rem(partner + 2 * index, col_count), 0, partner).wait_recv()

        @pl.loop(0, col_count)
        def _(owner):
            source = crx[place, owner]
            cot_t[layer, lanes(base + owner * LANES), pl.ds(tokens, tokens)] = source.T.astype(jnp.bfloat16)

        for number in range(col_count - 1):
            col_copy(place, mine, number, partner).wait_send()

        @pl.when(layer < layers - 1)
        def _():
            signal(cot_free.at[place], peer)

    def take(layer, chunk):
        number = act_number(layer, chunk)
        slot = number % ACT_SLOTS
        act_copy(0, number).wait_recv()
        act_cat[layer, pl.ds(tokens, tokens), lanes(chunk * LANES)] = xr[slot].astype(jnp.bfloat16)

        @pl.when(number + ACT_SLOTS < wides)
        def _():
            signal(act_free.at[slot], peer)

        index = jnp.where(chunk < line - 1, chunk + line - 1, chunk + line)
        send(unit_base(layer) + index + AHEAD_UNITS)

    def form(item, target):
        layer, narrow, chunk = describe(item)
        here = item % slots
        at = pl.ds(pl.multiple_of(target * pair_rows, LANES), pair_rows)

        @pl.when(narrow)
        def _():
            part[here, target] = jnp.dot(
                cot_t[0, at, pl.ds(0, tokens)], narrow_act[jnp.minimum(item, NARROW - 1)],
                preferred_element_type=jnp.float32,
            )

        @pl.when(jnp.logical_not(narrow))
        def _():
            part[here, target] = jnp.dot(
                cot_t[layer, at, :], act_cat[layer, :, lanes(chunk * LANES)],
                preferred_element_type=jnp.float32,
            )

    def opens(item):
        layer, narrow, chunk = describe(item)
        return layer, jnp.logical_and(jnp.logical_not(narrow), chunk == 0)

    def ready(item, place):
        @pl.when(item == 0)
        def _():
            prepare(0, place)

        layer, first = opens(item)

        @pl.when(first)
        def _():
            if place == 0:
                @pl.when(layer == 0)
                def _():
                    for early in range(2):
                        forward(layer, early)

                for early in range(2, line - 1):
                    forward(layer, early)
                for early in range(2):
                    relay(early)
            if place == line - 1:
                relay(place)
            absorb(layer, place)

    def hop(item, stage):
        here = item % slots

        @pl.when(z <= stage)
        def _():
            target = line - 1 - stage + z
            form(item, target)
            if stage > 0:
                @pl.when(has_left)
                def _():
                    r_copy(here, target).wait_recv()
                    part[here, target] += arr[here, target + 1]

            r_copy(here, target).start()

        @pl.when(mirror <= stage)
        def _():
            target = stage - mirror
            form(item, target)
            if stage > 0:
                @pl.when(has_right)
                def _():
                    l_copy(here, target).wait_recv()
                    part[here, target] += arr[here, target]

            l_copy(here, target).start()

    def weight_place(layer, piece):
        row = pl.ds(pl.multiple_of(layer * rows, 8), rows)
        return crx.at[piece // col_count, piece % col_count, row]

    def weight_in(layer, piece):
        return pltpu.make_async_copy(
            weights_hbm.at[layer, :, lanes(piece * LANES)], weight_place(layer, piece), w_in.at[layer, piece]
        )

    def weight_out(layer, piece):
        return pltpu.make_async_copy(
            weight_place(layer, piece), new_weights.at[layer, :, lanes(piece * LANES)], w_out.at[layer, piece]
        )

    def code_in(layer, kind):
        source = (moments_hbm, squares_hbm)[kind].at[layer]
        return pltpu.make_async_copy(
            source, cot_raw.at[layer, pl.ds(kind * rows, rows), pl.ds(0, cols)], c_in.at[layer, kind]
        )

    def code_out(layer, piece, kind):
        place = cot_raw.at[layer, pl.ds(kind * rows, rows), lanes(piece * LANES)]
        target = (new_moments, new_squares)[kind].at[layer, :, lanes(piece * LANES)]
        return pltpu.make_async_copy(place, target, c_out.at[layer, piece, kind])

    def spread_scales():
        for layer in range(layers):
            for kind in range(2):
                source = (moment_scale, square_scale)[kind]
                factor = (beta_one, beta_two)[kind]
                row = source[layer, pl.ds(mine, 1), :] * factor
                for part_at in range(0, rows, LANES):
                    tile = jnp.broadcast_to(row[:, part_at : part_at + LANES], (LANES, LANES))
                    scale_rows[kind, layer, part_at : part_at + LANES] = tile.T

    def begin(item):
        layer, narrow, chunk = describe(item)
        ready(item, 0)

        @pl.when(jnp.logical_not(narrow))
        def _():
            take(layer, chunk)

        @pl.when(item >= slots)
        def _():
            @pl.when(has_right)
            def _():
                pl.semaphore_wait(from_right, 1)

            @pl.when(has_left)
            def _():
                pl.semaphore_wait(from_left, 1)

        hop(item, 0)

        @pl.when(item == 1)
        def _():
            for copy in loads[early_loads:]:
                copy.wait()

        @pl.when(item == items - 2)
        def _():
            spread_scales()
            for index in range(layers):
                for kind in range(2):
                    code_in(index, kind).start()

            @pl.loop(0, layers * pieces)
            def _(index):
                weight_in(index // pieces, index % pieces).start()

        @pl.when(jnp.logical_and(jnp.logical_not(narrow), chunk == 0))
        def _():
            for early in range(2, line - 1):
                relay(early)

        next_layer, next_first = opens(item + 1)

        @pl.when(jnp.logical_and(next_first, jnp.logical_and(next_layer > 0, item + 1 < items)))
        def _():
            for place in range(2):
                forward(next_layer, place)

        @pl.when(jnp.logical_and(jnp.logical_not(narrow), chunk == line - 2))
        def _():
            forward(layer, line - 1)

    def middle(item, stage):
        ready(item, stage)
        hop(item, stage)

    def add_squares(value):
        rows8 = value.reshape(value.shape[0] // 8, 8, LANES)
        own_sq[...] += jnp.sum(rows8 * rows8, axis=0)

    def join_narrow():
        for item in range(NARROW):
            n_copy(item).wait_recv()
            where = lanes((item % 2) * half + (chunks - 1 - item // 2) * LANES)
            value = grad[0, :, where] + narrow_in[item]
            grad[0, :, where] = value
            add_squares(value)

    def finish(item):
        layer, narrow, chunk = describe(item)
        here = item % slots
        ready(item, line - 1)

        @pl.when(item == items - 2)
        def _():
            join_narrow()

        form(item, z)

        @pl.when(has_left)
        def _():
            r_copy(here, z).wait_recv()
            part[here, z] += arr[here, z + 1]

        @pl.when(has_right)
        def _():
            l_copy(here, z).wait_recv()
            part[here, z] += arr[here, z]

        for target in range(line):
            @pl.when(target > z)
            def _(target=target):
                r_copy(here, target).wait_send()

            @pl.when(target < z)
            def _(target=target):
                l_copy(here, target).wait_send()

        kept = pl.ds(pl.multiple_of(x * rows, 8), rows)
        held[item] = part[here, z, pl.ds(pl.multiple_of((1 - x) * rows, 8), rows)]

        @pl.when(narrow)
        def _():
            start = (item % 2) * half + (chunks - 1 - item // 2) * LANES
            grad[0, :, lanes(start)] = part[here, z, kept]

        @pl.when(jnp.logical_not(narrow))
        def _():
            grad[layer, :, lanes(own_half + chunk * LANES)] = part[here, z, kept]
            add_squares(part[here, z])

        @pl.when(item + slots < items)
        def _():
            @pl.when(has_left)
            def _():
                signal(from_right, left)

            @pl.when(has_right)
            def _():
                signal(from_left, right)

    own_sq[...] = jnp.zeros_like(own_sq)
    for unit in range(line - 1):
        loads[unit].wait()
        send(jnp.int32(unit))
    for copy in loads[line - 1 : early_loads]:
        copy.wait()
    for unit in range(line - 1, AHEAD_UNITS):
        send(jnp.int32(unit))

    @pl.loop(0, items + line)
    def _(step):
        def guard(turn, action):
            item = turn - (turn > NARROW).astype(jnp.int32)
            real = jnp.logical_and(turn >= 0, turn != NARROW)
            pl.when(jnp.logical_and(real, item < items))(lambda: action(item))

        for stage in reversed(range(1, line - 1)):
            guard(step - stage, functools.partial(middle, stage=stage))
        guard(step, begin)
        guard(step - (line - 1), finish)

        @pl.loop(exchanged(step - 1), exchanged(step))
        def _(item):
            exchange(item)

    def spread(src, landing, send_sems, recv_sems, axis, index, size):
        copies = []
        for offset in range(1, size):
            copies.append(
                pltpu.make_async_remote_copy(
                    src_ref=src, dst_ref=landing.at[offset - 1],
                    send_sem=send_sems.at[offset - 1], recv_sem=recv_sems.at[offset - 1],
                    device_id={axis: lax.rem(index + offset, size)},
                    device_id_type=pl.DeviceIdType.MESH,
                )
            )
        for copy in copies:
            copy.start()
        for copy in copies:
            copy.wait()
        total = src[...]
        for offset in range(1, size):
            total = total + landing[offset - 1]
        return total

    sum_sq[...] = spread(own_sq, col_sq, qs_sem, qr_sem, "col", mine, col_count)
    total = spread(sum_sq, dp_sq, ds_sem, dr_sem, "dp", me, count)
    total = jnp.sum(jnp.sum(total, axis=0, keepdims=True), axis=1, keepdims=True)
    rms = jnp.sqrt(total / float(layers * features * cols * col_count) + norm_eps)
    clip = jnp.minimum(1.0, 1.0 / rms)
    moment_gain = clip * (1.0 - beta_one)
    square_gain = clip * clip * (1.0 - beta_two)
    correct_one = 1.0 - beta_one**STEP
    correct_two = 1.0 - beta_two**STEP

    for index in range(layers):
        for kind in range(2):
            code_in(index, kind).wait()

    @pl.loop(NARROW, items)
    def _(item):
        f_copy(item, 1 - x).wait_recv()

    def moments_of(layer, at, height, piece):
        where = lanes(piece * LANES)
        value = grad[layer, pl.ds(at, height), where]
        moment = cot_raw[layer, pl.ds(at, height), where].astype(jnp.float32)
        square = cot_raw[layer, pl.ds(pl.multiple_of(rows + at, 16), height), where].astype(jnp.float32)
        moment = moment * scale_rows[0, layer, pl.ds(at, height)] + moment_gain * value
        square = square * scale_rows[1, layer, pl.ds(at, height)] + square_gain * (value * value)
        return moment, square

    @pl.loop(0, layers * (rows // PEAK_ROWS))
    def _(index):
        layer = index // (rows // PEAK_ROWS)
        at = pl.multiple_of(index % (rows // PEAK_ROWS) * PEAK_ROWS, PEAK_ROWS)
        high_moment = jnp.zeros((PEAK_ROWS, LANES), jnp.float32)
        high_square = jnp.zeros((PEAK_ROWS, LANES), jnp.float32)
        for piece in range(pieces):
            moment, square = moments_of(layer, at, PEAK_ROWS, piece)
            high_moment = jnp.maximum(high_moment, jnp.abs(moment))
            high_square = jnp.maximum(high_square, square)
        peak[0, layer, pl.ds(at, PEAK_ROWS)] = high_moment
        peak[1, layer, pl.ds(at, PEAK_ROWS)] = high_square

    for layer in range(layers):
        for kind in range(2):
            for at in range(0, rows, LANES):
                tile = peak[kind, layer, at : at + LANES].T
                row = jnp.max(tile, axis=0, keepdims=True)
                peak_rows[mine, kind, layer : layer + 1, at : at + LANES] = row
                inverse = 1.0 / (row + scale_eps)
                peak[kind, layer, at : at + LANES] = jnp.broadcast_to(inverse, (LANES, LANES)).T

    def peak_copy(offset):
        return pltpu.make_async_remote_copy(
            src_ref=peak_rows.at[mine], dst_ref=peak_rows.at[mine],
            send_sem=ms_sem.at[offset - 1], recv_sem=mr_sem.at[mine],
            device_id={"col": lax.rem(mine + offset, col_count)},
            device_id_type=pl.DeviceIdType.MESH,
        )

    def peak_arrival(owner):
        return pltpu.make_async_remote_copy(
            src_ref=peak_rows.at[owner], dst_ref=peak_rows.at[owner],
            send_sem=ms_sem.at[0], recv_sem=mr_sem.at[owner],
            device_id={"col": partner}, device_id_type=pl.DeviceIdType.MESH,
        )

    for offset in range(1, col_count):
        peak_copy(offset).start()

    @pl.loop(0, layers * pieces)
    def _(index):
        layer = index // pieces
        piece = index % pieces
        where = lanes(piece * LANES)
        weight_in(layer, piece).wait()

        for at in range(0, rows, APPLY_ROWS):
            moment, square = moments_of(layer, at, APPLY_ROWS, piece)
            span = pl.ds(at, APPLY_ROWS)
            cot_raw[layer, span, where] = (moment * peak[0, layer, span]).astype(jnp.bfloat16)
            cot_raw[layer, pl.ds(rows + at, APPLY_ROWS), where] = (square * peak[1, layer, span]).astype(jnp.bfloat16)
            ratio = moment * (1.0 / correct_one) / (jnp.sqrt(square * (1.0 / correct_two)) + adam_eps)
            place = (piece // col_count, piece % col_count, pl.ds(pl.multiple_of(layer * rows + at, 8), APPLY_ROWS))
            weights = crx[place]
            crx[place] = weights - learn_rate * (decay_rate * weights + ratio)

        weight_out(layer, piece).start()
        for kind in range(2):
            code_out(layer, piece, kind).start()

    for offset in range(1, col_count):
        peak_arrival(lax.rem(mine + offset, col_count)).wait_recv()
    for owner in range(col_count):
        for layer in range(layers):
            new_moment_scale[layer, owner : owner + 1, :] = peak_rows[owner, 0, layer : layer + 1, :]
            new_square_scale[layer, owner : owner + 1, :] = peak_rows[owner, 1, layer : layer + 1, :]

    for offset in range(1, col_count):
        peak_copy(offset).wait_send()

    @pl.loop(units - SEND_SLOTS, units)
    def _(unit):
        act_copy(unit, 0).wait_send()

    @pl.loop(0, items)
    def _(item):
        n_copy(item).wait_send()

    @pl.loop(0, layers * pieces)
    def _(index):
        layer = index // pieces
        piece = index % pieces
        weight_out(layer, piece).wait()
        for kind in range(2):
            code_out(layer, piece, kind).wait()


def factor_step(
    mesh_shape, activations, cotangent, master_weights, moment_codes, square_codes, moment_scales, square_scales
):
    count = mesh_shape["dp"]
    col_count = mesh_shape["col"]
    layers, tokens, cols = activations.shape
    line = count // 2
    features = cotangent.shape[2]
    rows = features // count
    half = cols // 2
    slots = line + 1
    pieces = cols // LANES
    items = NARROW + layers * (half // LANES) - NARROW // 2
    piece = (tokens, LANES)
    f32, bf16 = jnp.float32, jnp.bfloat16
    dma = pltpu.SemaphoreType.DMA
    regular = pltpu.SemaphoreType.REGULAR
    vmem = pl.BlockSpec(memory_space=pltpu.VMEM)
    hbm = pl.BlockSpec(memory_space=pl.ANY)
    outs = pl.pallas_call(
        functools.partial(factor_kernel, count, col_count),
        out_shape=(
            jax.ShapeDtypeStruct((layers, rows, cols), f32),
            jax.ShapeDtypeStruct((layers, rows, cols), bf16),
            jax.ShapeDtypeStruct((layers, rows, cols), bf16),
            jax.ShapeDtypeStruct((layers, col_count, rows), f32),
            jax.ShapeDtypeStruct((layers, col_count, rows), f32),
        ),
        in_specs=[hbm, hbm, hbm, hbm, hbm, vmem, vmem],
        out_specs=(hbm, hbm, hbm, vmem, vmem),
        scratch_shapes=[
            pltpu.VMEM((layers, rows, cols), f32),
            pltpu.VMEM((2, layers, rows, LANES), f32),
            pltpu.VMEM((2, layers, rows, LANES), f32),
            pltpu.VMEM((col_count, 2, layers, rows), f32),
            pltpu.VMEM((layers, tokens, features), bf16),
            pltpu.VMEM((layers, tokens, half), bf16),
            pltpu.VMEM((NARROW,) + piece, bf16),
            pltpu.VMEM((layers, features, 2 * tokens), bf16),
            pltpu.VMEM((layers, 2 * tokens, half), bf16),
            pltpu.VMEM((SEND_SLOTS,) + piece, f32),
            pltpu.VMEM((ACT_SLOTS,) + piece, f32),
            pltpu.VMEM((line, col_count) + piece, f32),
            pltpu.VMEM((slots, line, 2 * rows, LANES), f32),
            pltpu.VMEM((slots, line + 1, 2 * rows, LANES), f32),
            pltpu.VMEM((NARROW, rows, LANES), f32),
            pltpu.VMEM((items, rows, LANES), f32),
            pltpu.VMEM((8, LANES), f32),
            pltpu.VMEM((8, LANES), f32),
            pltpu.VMEM((col_count - 1, 8, LANES), f32),
            pltpu.VMEM((count - 1, 8, LANES), f32),
            dma((NARROW + line + 3 * layers - 1,)),
            dma((layers, pieces)), dma((layers, pieces)), dma((layers, 2)), dma((layers, pieces, 2)),
            dma((col_count - 1,)), dma((col_count,)),
            dma((SEND_SLOTS,)), dma((ACT_SLOTS,)), dma((line,)),
            dma((line, col_count - 1)), dma((line, col_count)),
            dma((slots, line)), dma((slots, line)), dma((slots, line)), dma((slots, line)),
            dma((items,)), dma((items,)),
            dma((col_count - 1,)), dma((col_count - 1,)), dma((count - 1,)), dma((count - 1,)),
            regular((ACT_SLOTS,)), regular((line,)), regular, regular,
        ],
        compiler_params=pltpu.CompilerParams(
            collective_id=0, has_side_effects=True, vmem_limit_bytes=67043328
        ),
    )(
        cotangent, activations, master_weights, moment_codes, square_codes,
        moment_scales.transpose(0, 2, 1), square_scales.transpose(0, 2, 1),
    )
    return outs[:3] + (outs[3].transpose(0, 2, 1), outs[4].transpose(0, 2, 1))


def fits_factors(activations, cotangent, block_count, mesh_shape):
    count = mesh_shape["dp"]
    line = count // 2
    rows = cotangent.shape[2] // count
    chunks = activations.shape[2] // (2 * LANES)
    aligned = activations.shape[1] % LANES == 0 and activations.shape[2] % (2 * LANES) == 0
    layers, tokens, cols = activations.shape
    aligned = aligned and rows % LANES == 0 and cols % LANES == 0 and block_count == mesh_shape["col"]
    roomy = layers * rows <= tokens and cols <= cotangent.shape[2] and cols <= LANES * line * mesh_shape["col"]
    return aligned and roomy and line >= 3 and 2 * rows == LANES * mesh_shape["col"] and mesh_shape["col"] % 2 == 0 and chunks - NARROW // 2 > line


def local(
    mesh_shape, activations, cotangent, master_weights, moment_codes, square_codes, moment_scales, square_scales
):
    layer_count = activations.shape[0]
    shard_rows = master_weights.shape[1]
    shard_cols = master_weights.shape[2]
    block_count = moment_scales.shape[2]
    if fits_factors(activations, cotangent, block_count, mesh_shape):
        return factor_step(
            mesh_shape, activations, cotangent, master_weights, moment_codes, square_codes,
            moment_scales, square_scales,
        )
    gradient, squares = reduced_gradient(activations, cotangent, mesh_shape)
    total_sq = jnp.sum(squares)
    rms = jnp.sqrt(total_sq / float(LAYERS * KV * D) + norm_eps)
    clip_factor = jnp.minimum(1.0, 1.0 / rms)
    correct_one = 1.0 - beta_one**STEP
    correct_two = 1.0 - beta_two**STEP
    own_block = lax.axis_index("col") * shard_cols // BLOCK
    selector = (jnp.arange(block_count, dtype=jnp.int32) == own_block).astype(jnp.float32)
    outs_weights, outs_mcode, outs_scode, outs_mscale, outs_sscale = ([], [], [], [], [])
    for layer_index in range(layer_count):
        moment_scale = jnp.sum(moment_scales[layer_index] * selector, axis=1)
        square_scale = jnp.sum(square_scales[layer_index] * selector, axis=1)
        old_moment = moment_codes[layer_index].astype(jnp.float32) * moment_scale[:, None]
        old_square = square_codes[layer_index].astype(jnp.float32) * square_scale[:, None]
        grad_now = clip_factor * gradient[layer_index]
        new_moment = beta_one * old_moment + (1.0 - beta_one) * grad_now
        new_square = beta_two * old_square + (1.0 - beta_two) * grad_now * grad_now
        moment_part = jnp.max(jnp.abs(new_moment), axis=1)[:, None] * selector
        square_part = jnp.max(new_square, axis=1)[:, None] * selector
        moment, square, moment_part, square_part = (
            new_moment,
            new_square,
            moment_part,
            square_part,
        )
        moment_max, square_max = lax.pmax((moment_part, square_part), "col")
        moment_div = jnp.sum(moment_max * selector, axis=1)[:, None]
        square_div = jnp.sum(square_max * selector, axis=1)[:, None]
        moment_out = (moment / (moment_div + scale_eps)).astype(jnp.bfloat16)
        square_out = (square / (square_div + scale_eps)).astype(jnp.bfloat16)
        ratio = moment / correct_one / (jnp.sqrt(square / correct_two) + adam_eps)
        weights = master_weights[layer_index]
        results = (weights - learn_rate * (decay_rate * weights + ratio), moment_out, square_out)
        outs_weights.append(results[0])
        outs_mcode.append(results[1])
        outs_scode.append(results[2])
        outs_mscale.append(moment_max)
        outs_sscale.append(square_max)
    return (
        jnp.stack(outs_weights),
        jnp.stack(outs_mcode),
        jnp.stack(outs_scode),
        jnp.stack(outs_mscale),
        jnp.stack(outs_sscale),
    )


def solution(mesh):
    in_specs = (
        P(None, "dp", "col"),
        P(None, "dp", None),
        P(None, "dp", "col"),
        P(None, "dp", "col"),
        P(None, "dp", "col"),
        P(None, "dp", None),
        P(None, "dp", None),
    )
    out_specs = (
        P(None, "dp", "col"),
        P(None, "dp", "col"),
        P(None, "dp", "col"),
        P(None, "dp", None),
        P(None, "dp", None),
    )
    return jax.shard_map(functools.partial(local, dict(mesh.shape)), mesh=mesh, in_specs=in_specs, out_specs=out_specs, check_vma=False)
```

```python
import functools

import jax
import jax.numpy as jnp
from jax import lax
from jax.experimental import pallas as pl
from jax.experimental.pallas import tpu as pltpu
from jax.sharding import PartitionSpec as P

D = 8192
KV = 2048
BLOCK = 2048
LAYERS = 2
STEP = 10


beta_one = 0.9
beta_two = 0.999
learn_rate = 0.001
decay_rate = 0.1
adam_eps = 1e-08
scale_eps = 1e-06
norm_eps = 1e-06

LANES = 128
AHEAD = 3
XSLOTS = 4


def reduce_kernel(
    count, col_count, cot_ref, act_ref, out_ref, sq_ref,
    xs, xr, part, arr, bs, br, own_sq, sum_sq, col_sq, dp_sq,
    xs_sem, xr_sem, rs_sem, rr_sem, ls_sem, ll_sem, bs_sem, br_sem,
    cs_sem, cr_sem, ds_sem, dr_sem, x_free, from_right, from_left,
):
    layers, pairs, line, rows, tokens = cot_ref.shape
    cols = act_ref.shape[2]
    slots = part.shape[0]
    wide_per = cols // (2 * LANES) - 1
    per_layer = wide_per + 2
    period = (per_layer + 1) // 2
    items = layers * per_layer
    wides = layers * wide_per
    me = lax.axis_index("dp")
    z = me // 2
    x = me % 2
    peer = 2 * z + 1 - x
    right = jnp.minimum(z + 1, line - 1) * 2 + x
    left = jnp.maximum(z - 1, 0) * 2 + x
    has_right = z < line - 1
    has_left = z > 0
    mirror = line - 1 - z

    def signal(sem, where):
        pl.semaphore_signal(
            sem, inc=1, device_id={"dp": where}, device_id_type=pl.DeviceIdType.MESH
        )

    barrier = pltpu.get_barrier_semaphore()
    mine = lax.axis_index("col")
    for offset in range(1, count):
        signal(barrier, lax.rem(me + offset, count))
    for offset in range(1, col_count):
        pl.semaphore_signal(
            barrier, inc=1, device_id={"col": lax.rem(mine + offset, col_count)},
            device_id_type=pl.DeviceIdType.MESH,
        )
    pl.semaphore_wait(barrier, count + col_count - 2)

    def remote(src, dst, send, recv, where):
        return pltpu.make_async_remote_copy(
            src_ref=src, dst_ref=dst, send_sem=send, recv_sem=recv,
            device_id={"dp": where}, device_id_type=pl.DeviceIdType.MESH,
        )

    def describe(item):
        layer = item // per_layer
        place = item % per_layer
        narrow = place % period == 0
        wide_at = place - (place + period - 1) // period
        narrow_at = place // period
        return layer, narrow, wide_at, narrow_at

    def x_copy(number):
        slot = number % XSLOTS
        return remote(xs.at[slot], xr.at[slot], xs_sem.at[slot], xr_sem.at[slot], peer)

    def r_copy(slot, target):
        return remote(
            part.at[slot, target], arr.at[slot, target + 1],
            rs_sem.at[slot, target], rr_sem.at[slot, target], right,
        )

    def l_copy(slot, target):
        return remote(
            part.at[slot, target], arr.at[slot, target],
            ls_sem.at[slot, target], ll_sem.at[slot, target], left,
        )

    def b_copy(number):
        return remote(
            bs.at[number], br.at[number], bs_sem.at[number], br_sem.at[number], peer
        )

    def product(layer, pair, target, start, width):
        return jnp.dot(
            cot_ref[layer, pair, target],
            act_ref[layer, :, pl.ds(pl.multiple_of(start, LANES), width)],
            preferred_element_type=jnp.float32,
        )

    def send_wide(item):
        layer, narrow, wide_at, _ = describe(item)

        @pl.when(jnp.logical_not(narrow))
        def _():
            number = layer * wide_per + wide_at
            slot = number % XSLOTS

            @pl.loop(0, line)
            def _(target):
                value = product(layer, 1 - x, target, wide_at * 2 * LANES, 2 * LANES)
                xs[slot, target, 0] = value[:, :LANES]
                xs[slot, target, 1] = value[:, LANES:]

            @pl.when(number >= XSLOTS)
            def _():
                pl.semaphore_wait(x_free, 1)

            x_copy(number).start()

    def form(item):
        layer, narrow, wide_at, narrow_at = describe(item)
        here = item % slots

        @pl.when(item >= slots)
        def _():
            @pl.when(has_right)
            def _():
                pl.semaphore_wait(from_right, 1)

            @pl.when(has_left)
            def _():
                pl.semaphore_wait(from_left, 1)

        @pl.when(narrow)
        def _():
            start = wide_per * 2 * LANES + narrow_at * LANES

            @pl.loop(0, line)
            def _(target):
                part[here, target, 0] = product(layer, 0, target, start, LANES)
                part[here, target, 1] = product(layer, 1, target, start, LANES)

        @pl.when(jnp.logical_not(narrow))
        def _():
            number = layer * wide_per + wide_at
            slot = number % XSLOTS
            x_copy(number).wait()

            @pl.loop(0, line)
            def _(target):
                value = product(layer, x, target, wide_at * 2 * LANES, 2 * LANES)
                part[here, target, 0] = value[:, :LANES] + xr[slot, target, 0]
                part[here, target, 1] = value[:, LANES:] + xr[slot, target, 1]

            @pl.when(number + XSLOTS < wides)
            def _():
                signal(x_free, peer)

    def hop(item, stage):
        here = item % slots

        @pl.when(z <= stage)
        def _():
            target = line - 1 - stage + z
            if stage > 0:
                @pl.when(has_left)
                def _():
                    r_copy(here, target).wait_recv()
                    part[here, target] += arr[here, target + 1]

            r_copy(here, target).start()

        @pl.when(mirror <= stage)
        def _():
            target = stage - mirror
            if stage > 0:
                @pl.when(has_right)
                def _():
                    l_copy(here, target).wait_recv()
                    part[here, target] += arr[here, target]

            l_copy(here, target).start()

    def finish(item):
        layer, narrow, wide_at, narrow_at = describe(item)
        here = item % slots

        @pl.when(has_left)
        def _():
            r_copy(here, z).wait_recv()
            part[here, z] += arr[here, z + 1]

        @pl.when(has_right)
        def _():
            l_copy(here, z).wait_recv()
            part[here, z] += arr[here, z]

        for target in range(line):
            @pl.when(target > z)
            def _(target=target):
                r_copy(here, target).wait_send()

            @pl.when(target < z)
            def _(target=target):
                l_copy(here, target).wait_send()

        @pl.when(narrow)
        def _():
            number = layer * 2 + narrow_at
            start = wide_per * 2 * LANES + narrow_at * LANES
            bs[number] = part[here, z, 1 - x]
            b_copy(number).start()
            out_ref[layer, :, pl.ds(pl.multiple_of(start, LANES), LANES)] = part[here, z, x]

        @pl.when(jnp.logical_not(narrow))
        def _():
            for half in range(2):
                start = wide_at * 2 * LANES + half * LANES
                out_ref[layer, :, pl.ds(pl.multiple_of(start, LANES), LANES)] = part[here, z, half]

        @pl.when(item + slots < items)
        def _():
            @pl.when(has_left)
            def _():
                signal(from_right, left)

            @pl.when(has_right)
            def _():
                signal(from_left, right)

    for item in range(1, AHEAD):
        send_wide(jnp.int32(item))

    @pl.loop(0, items + line - 1)
    def _(step):
        def guard(item, action):
            pl.when(jnp.logical_and(item >= 0, item < items))(lambda: action(item))

        guard(step + AHEAD, send_wide)
        guard(step - (line - 1), finish)
        for stage in reversed(range(1, line - 1)):
            guard(step - stage, functools.partial(hop, stage=stage))

        def begin(item):
            form(item)
            hop(item, 0)

        guard(step, begin)

    for number in range(2 * layers):
        b_copy(number).wait()
        start = wide_per * 2 * LANES + (number % 2) * LANES
        out_ref[number // 2, :, start : start + LANES] += br[number]

    def square_rows(index, total):
        layer = index // (rows // 8)
        at = pl.multiple_of(index % (rows // 8) * 8, 8)
        for piece in range(cols // LANES):
            value = out_ref[layer, pl.ds(at, 8), piece * LANES : (piece + 1) * LANES]
            total = total + value * value
        return total

    def spread(src, landing, send, recv, axis, index, size):
        copies = []
        for offset in range(1, size):
            copies.append(
                pltpu.make_async_remote_copy(
                    src_ref=src, dst_ref=landing.at[offset - 1],
                    send_sem=send.at[offset - 1], recv_sem=recv.at[offset - 1],
                    device_id={axis: lax.rem(index + offset, size)},
                    device_id_type=pl.DeviceIdType.MESH,
                )
            )
        for copy in copies:
            copy.start()
        for copy in copies:
            copy.wait()
        total = src[...]
        for offset in range(1, size):
            total = total + landing[offset - 1]
        return total

    own_sq[...] = lax.fori_loop(
        0, layers * rows // 8, square_rows, jnp.zeros((8, LANES), jnp.float32)
    )
    sum_sq[...] = spread(own_sq, col_sq, cs_sem, cr_sem, "col", mine, col_count)
    sq_ref[...] = spread(sum_sq, dp_sq, ds_sem, dr_sem, "dp", me, count)


def reduced_gradient(activations, cotangent, mesh_shape):
    count = mesh_shape["dp"]
    col_count = mesh_shape["col"]
    layers, tokens, cols = activations.shape
    line = count // 2
    rows = cotangent.shape[2] // count
    slots = line + 2
    cot = cotangent.reshape(layers, tokens, line, 2, rows).transpose(0, 3, 2, 4, 1)
    block = (line, 2, rows, LANES)
    dma = pltpu.SemaphoreType.DMA
    vmem = pl.BlockSpec(memory_space=pltpu.VMEM)
    return pl.pallas_call(
        functools.partial(reduce_kernel, count, col_count),
        out_shape=(
            jax.ShapeDtypeStruct((layers, rows, cols), jnp.float32),
            jax.ShapeDtypeStruct((8, LANES), jnp.float32),
        ),
        in_specs=[vmem, vmem],
        out_specs=(vmem, vmem),
        scratch_shapes=[
            pltpu.VMEM((XSLOTS,) + block, jnp.float32),
            pltpu.VMEM((XSLOTS,) + block, jnp.float32),
            pltpu.VMEM((slots,) + block, jnp.float32),
            pltpu.VMEM((slots, line + 1) + block[1:], jnp.float32),
            pltpu.VMEM((2 * layers, rows, LANES), jnp.float32),
            pltpu.VMEM((2 * layers, rows, LANES), jnp.float32),
            pltpu.VMEM((8, LANES), jnp.float32),
            pltpu.VMEM((8, LANES), jnp.float32),
            pltpu.VMEM((col_count - 1, 8, LANES), jnp.float32),
            pltpu.VMEM((count - 1, 8, LANES), jnp.float32),
            dma((XSLOTS,)), dma((XSLOTS,)),
            dma((slots, line)), dma((slots, line)), dma((slots, line)), dma((slots, line)),
            dma((2 * layers,)), dma((2 * layers,)),
            dma((col_count - 1,)), dma((col_count - 1,)), dma((count - 1,)), dma((count - 1,)),
            pltpu.SemaphoreType.REGULAR, pltpu.SemaphoreType.REGULAR, pltpu.SemaphoreType.REGULAR,
        ],
        compiler_params=pltpu.CompilerParams(
            collective_id=0, has_side_effects=True, vmem_limit_bytes=62 * 2**20
        ),
    )(cot, activations)


AHEAD_UNITS = 5
SEND_SLOTS = 6
ACT_SLOTS = 5
NARROW = 2
RELEASE = 3
PEAK_ROWS = 32
APPLY_ROWS = 64
STRIP_ROWS = 32
APPLY_VMEM = 62 * 2**20


def factor_kernel(
    count, col_count, cot_hbm, act_hbm, moments_hbm, squares_hbm, moment_scale, square_scale,
    grad_out, gain_out, new_moment_scale, new_square_scale, grad,
    row_values, peak, peak_rows,
    cot_raw, act_raw, narrow_act, cot_t, act_cat, xs, xr, crx, part, arr, narrow_in, held,
    own_sq, sum_sq, col_sq, dp_sq,
    ld_sem, c_in, g_out, ms_sem, mr_sem, xs_sem, xr_sem, pr_sem, cs_sem, cr_sem, rs_sem, rr_sem, ls_sem, ll_sem, fs_sem, fr_sem,
    qs_sem, qr_sem, ds_sem, dr_sem, act_free, cot_free, from_right, from_left,
):
    layers, tokens, cols = act_hbm.shape
    half = cols // 2
    line = count // 2
    pair_rows = part.shape[2]
    rows = pair_rows // 2
    slots = part.shape[0]
    chunks = half // LANES
    first_chunks = chunks - NARROW // 2
    wides = first_chunks + (layers - 1) * chunks
    items = NARROW + wides
    first_units = first_chunks + line
    layer_units = chunks + line
    units = first_units + (layers - 1) * layer_units
    all_sent = items - chunks + line - 2
    groups = col_count // 2
    pieces = cols // LANES
    features = cot_hbm.shape[2]
    me = lax.axis_index("dp")
    mine = lax.axis_index("col")
    z = me // 2
    x = me % 2
    peer = 2 * z + 1 - x
    partner = mine + 1 - 2 * (mine % 2)
    right = jnp.minimum(z + 1, line - 1) * 2 + x
    left = jnp.maximum(z - 1, 0) * 2 + x
    has_right = z < line - 1
    has_left = z > 0
    mirror = line - 1 - z
    own_half = pl.multiple_of(x * half, LANES)
    peer_half = pl.multiple_of((1 - x) * half, LANES)

    def lanes(start, width=LANES):
        return pl.ds(pl.multiple_of(start, LANES), width)

    def signal(sem, where):
        pl.semaphore_signal(
            sem, inc=1, device_id={"dp": where}, device_id_type=pl.DeviceIdType.MESH
        )

    loads = []

    def load(src, dst):
        copy = pltpu.make_async_copy(src, dst, ld_sem.at[len(loads)])
        copy.start()
        loads.append(copy)

    def block_target(place):
        after = line - 1 - z
        rising = jnp.where(place < after, line - 1 - place, place - after)
        falling = jnp.where(place < z, place, line - 1 - (place - z))
        other = jnp.where(z < line // 2, rising, falling)
        return jnp.where(place < line - 1, other, z)

    for place in range(line):
        block = lanes(block_target(place) * pair_rows, pair_rows)
        load(cot_hbm.at[0, :, block], cot_raw.at[0, :, block])
    load(act_hbm.at[0, :, pl.ds(peer_half, half)], act_raw.at[0])
    for index in range(NARROW):
        start = (index % 2) * half + (chunks - 1 - index // 2) * LANES
        load(act_hbm.at[0, :, lanes(start)], narrow_act.at[index])
    for layer in range(layers):
        if layer > 0:
            load(cot_hbm.at[layer], cot_raw.at[layer])
            load(act_hbm.at[layer, :, pl.ds(peer_half, half)], act_raw.at[layer])
        load(act_hbm.at[layer, :, pl.ds(own_half, half)], act_cat.at[layer, pl.ds(0, tokens)])

    early_loads = line + 1 + NARROW

    barrier = pltpu.get_barrier_semaphore()
    signal(barrier, peer)

    @pl.when(has_right)
    def _():
        signal(barrier, right)

    @pl.when(has_left)
    def _():
        signal(barrier, left)

    for offset in range(1, col_count):
        pl.semaphore_signal(
            barrier, inc=1, device_id={"col": lax.rem(mine + offset, col_count)},
            device_id_type=pl.DeviceIdType.MESH,
        )
    sides = has_right.astype(jnp.int32) + has_left.astype(jnp.int32)
    pl.semaphore_wait(barrier, col_count + sides)

    def remote(src, dst, send, recv, where):
        return pltpu.make_async_remote_copy(
            src_ref=src, dst_ref=dst, send_sem=send, recv_sem=recv,
            device_id={"dp": where}, device_id_type=pl.DeviceIdType.MESH,
        )

    def describe(item):
        number = item - NARROW
        narrow = item < NARROW
        later = jnp.maximum(number - first_chunks, 0)
        layer = jnp.where(number < first_chunks, 0, 1 + later // chunks)
        chunk = jnp.where(number < first_chunks, number, later % chunks)
        return layer, narrow, chunk

    def unit_base(layer):
        return jnp.where(layer == 0, 0, first_units + (layer - 1) * layer_units)

    def act_number(layer, chunk):
        return jnp.where(layer == 0, chunk, first_chunks + (layer - 1) * chunks + chunk)

    def act_copy(unit, number):
        here = unit % SEND_SLOTS
        slot = number % ACT_SLOTS
        return remote(xs.at[here], xr.at[slot], xs_sem.at[here], xr_sem.at[slot], peer)

    def cot_copy(unit, place):
        here = unit % SEND_SLOTS
        return remote(xs.at[here], crx.at[place, mine], xs_sem.at[here], pr_sem.at[place], peer)

    def col_copy(place, owner, number, where):
        return pltpu.make_async_remote_copy(
            src_ref=crx.at[place, owner], dst_ref=crx.at[place, owner],
            send_sem=cs_sem.at[place, number], recv_sem=cr_sem.at[place, owner],
            device_id={"col": where}, device_id_type=pl.DeviceIdType.MESH,
        )

    def far(index):
        return lax.rem(mine + 2 * index, col_count)

    def r_copy(slot, target):
        return remote(
            part.at[slot, target], arr.at[slot, target + 1],
            rs_sem.at[slot, target], rr_sem.at[slot, target], right,
        )

    def l_copy(slot, target):
        return remote(
            part.at[slot, target], arr.at[slot, target],
            ls_sem.at[slot, target], ll_sem.at[slot, target], left,
        )

    def n_copy(item):
        where = narrow_in.at[jnp.minimum(item, NARROW - 1)]
        return remote(held.at[item], where, fs_sem.at[item], fr_sem.at[item], peer)

    def f_copy(item, side):
        layer, narrow, chunk = describe(item)
        where = grad.at[layer, :, lanes(side * half + chunk * LANES)]
        return remote(held.at[item], where, fs_sem.at[item], fr_sem.at[item], peer)

    def exchange(item):
        @pl.when(item < NARROW)
        def _():
            n_copy(item).start()

        @pl.when(item >= NARROW)
        def _():
            f_copy(item, x).start()

    def exchanged(step):
        done = jnp.minimum(step - (line - 1), RELEASE * (step - 1 - all_sent))
        return jnp.clip(done, 0, items)

    def send(unit):
        @pl.when(unit < units)
        def _():
            layer = jnp.where(unit < first_units, 0, 1 + (unit - first_units) // layer_units)
            index = unit - unit_base(layer)
            is_cot = jnp.logical_or(index < line - 1, index == 2 * line - 2)
            here = unit % SEND_SLOTS

            @pl.when(unit >= SEND_SLOTS)
            def _():
                act_copy(unit, 0).wait_send()

            @pl.when(is_cot)
            def _():
                place = jnp.minimum(index, line - 1)
                start = block_target(place) * pair_rows + mine * LANES
                xs[here] = cot_raw[layer, :, lanes(start)].astype(jnp.float32)

                @pl.when(layer > 0)
                def _():
                    pl.semaphore_wait(cot_free.at[place], 1)

                cot_copy(unit, place).start()

            @pl.when(jnp.logical_not(is_cot))
            def _():
                chunk = jnp.where(index < 2 * line - 2, index - (line - 1), index - line)
                number = act_number(layer, chunk)
                xs[here] = act_raw[layer, :, lanes(chunk * LANES)].astype(jnp.float32)

                @pl.when(number >= ACT_SLOTS)
                def _():
                    pl.semaphore_wait(act_free.at[number % ACT_SLOTS], 1)

                act_copy(unit, number).start()

    def forward(layer, place):
        cot_copy(0, place).wait_recv()
        for index in range(1, groups):
            col_copy(place, mine, index, far(index)).start()
        col_copy(place, mine, 0, partner).start()
        send(unit_base(layer) + jnp.where(place < line - 1, place, 2 * line - 2) + AHEAD_UNITS)

    def relay(place):
        for index in range(1, groups):
            col_copy(place, far(index), groups - 1 + index, partner).wait_recv()
            col_copy(place, far(index), groups - 1 + index, partner).start()

    def prepare(layer, place):
        base = block_target(place) * pair_rows

        @pl.loop(0, col_count)
        def _(member):
            start = base + member * LANES
            value = cot_raw[layer, :, lanes(start)].astype(jnp.float32)
            cot_t[layer, lanes(start), pl.ds(0, tokens)] = value.T.astype(jnp.bfloat16)

    def absorb(layer, place):
        @pl.when(layer > 0)
        def _():
            prepare(layer, place)

        base = block_target(place) * pair_rows
        col_copy(place, partner, 0, partner).wait_recv()
        for index in range(1, groups):
            col_copy(place, lax.rem(partner + 2 * index, col_count), 0, partner).wait_recv()

        @pl.loop(0, col_count)
        def _(owner):
            source = crx[place, owner]
            cot_t[layer, lanes(base + owner * LANES), pl.ds(tokens, tokens)] = source.T.astype(jnp.bfloat16)

        for number in range(col_count - 1):
            col_copy(place, mine, number, partner).wait_send()

        @pl.when(layer < layers - 1)
        def _():
            signal(cot_free.at[place], peer)

    def take(layer, chunk):
        number = act_number(layer, chunk)
        slot = number % ACT_SLOTS
        act_copy(0, number).wait_recv()
        act_cat[layer, pl.ds(tokens, tokens), lanes(chunk * LANES)] = xr[slot].astype(jnp.bfloat16)

        @pl.when(number + ACT_SLOTS < wides)
        def _():
            signal(act_free.at[slot], peer)

        index = jnp.where(chunk < line - 1, chunk + line - 1, chunk + line)
        send(unit_base(layer) + index + AHEAD_UNITS)

    def form(item, target):
        layer, narrow, chunk = describe(item)
        here = item % slots
        at = pl.ds(pl.multiple_of(target * pair_rows, LANES), pair_rows)

        @pl.when(narrow)
        def _():
            part[here, target] = jnp.dot(
                cot_t[0, at, pl.ds(0, tokens)], narrow_act[jnp.minimum(item, NARROW - 1)],
                preferred_element_type=jnp.float32,
            )

        @pl.when(jnp.logical_not(narrow))
        def _():
            part[here, target] = jnp.dot(
                cot_t[layer, at, :], act_cat[layer, :, lanes(chunk * LANES)],
                preferred_element_type=jnp.float32,
            )

    def opens(item):
        layer, narrow, chunk = describe(item)
        return layer, jnp.logical_and(jnp.logical_not(narrow), chunk == 0)

    def ready(item, place):
        @pl.when(item == 0)
        def _():
            prepare(0, place)

        layer, first = opens(item)

        @pl.when(first)
        def _():
            if place == 0:
                @pl.when(layer == 0)
                def _():
                    for early in range(2):
                        forward(layer, early)

                for early in range(2, line - 1):
                    forward(layer, early)
                for early in range(2):
                    relay(early)
            if place == line - 1:
                relay(place)
            absorb(layer, place)

    def hop(item, stage):
        here = item % slots

        @pl.when(z <= stage)
        def _():
            target = line - 1 - stage + z
            form(item, target)
            if stage > 0:
                @pl.when(has_left)
                def _():
                    r_copy(here, target).wait_recv()
                    part[here, target] += arr[here, target + 1]

            r_copy(here, target).start()

        @pl.when(mirror <= stage)
        def _():
            target = stage - mirror
            form(item, target)
            if stage > 0:
                @pl.when(has_right)
                def _():
                    l_copy(here, target).wait_recv()
                    part[here, target] += arr[here, target]

            l_copy(here, target).start()

    def code_in(layer, kind):
        source = (moments_hbm, squares_hbm)[kind].at[layer]
        return pltpu.make_async_copy(
            source, cot_raw.at[layer, pl.ds(kind * rows, rows), pl.ds(0, cols)], c_in.at[layer, kind]
        )

    def spread_scales():
        for layer in range(layers):
            for kind in range(2):
                source = (moment_scale, square_scale)[kind]
                factor = (beta_one, beta_two)[kind]
                row = source[layer, pl.ds(mine, 1), :] * factor
                for part_at in range(0, rows, LANES):
                    tile = jnp.broadcast_to(row[:, part_at : part_at + LANES], (LANES, LANES))
                    row_values[kind, layer, part_at : part_at + LANES] = tile.T

    def begin(item):
        layer, narrow, chunk = describe(item)
        ready(item, 0)

        @pl.when(jnp.logical_not(narrow))
        def _():
            take(layer, chunk)

        @pl.when(item >= slots)
        def _():
            @pl.when(has_right)
            def _():
                pl.semaphore_wait(from_right, 1)

            @pl.when(has_left)
            def _():
                pl.semaphore_wait(from_left, 1)

        hop(item, 0)

        @pl.when(item == 1)
        def _():
            for copy in loads[early_loads:]:
                copy.wait()

        @pl.when(item == items - 2)
        def _():
            spread_scales()
            for index in range(layers):
                for kind in range(2):
                    code_in(index, kind).start()

        @pl.when(jnp.logical_and(jnp.logical_not(narrow), chunk == 0))
        def _():
            for early in range(2, line - 1):
                relay(early)

        next_layer, next_first = opens(item + 1)

        @pl.when(jnp.logical_and(next_first, jnp.logical_and(next_layer > 0, item + 1 < items)))
        def _():
            for place in range(2):
                forward(next_layer, place)

        @pl.when(jnp.logical_and(jnp.logical_not(narrow), chunk == line - 2))
        def _():
            forward(layer, line - 1)

    def middle(item, stage):
        ready(item, stage)
        hop(item, stage)

    def add_squares(value):
        rows8 = value.reshape(value.shape[0] // 8, 8, LANES)
        own_sq[...] += jnp.sum(rows8 * rows8, axis=0)

    def join_narrow():
        for item in range(NARROW):
            n_copy(item).wait_recv()
            where = lanes((item % 2) * half + (chunks - 1 - item // 2) * LANES)
            value = grad[0, :, where] + narrow_in[item]
            grad[0, :, where] = value
            add_squares(value)

    def finish(item):
        layer, narrow, chunk = describe(item)
        here = item % slots
        ready(item, line - 1)

        @pl.when(item == items - 2)
        def _():
            join_narrow()

        form(item, z)

        @pl.when(has_left)
        def _():
            r_copy(here, z).wait_recv()
            part[here, z] += arr[here, z + 1]

        @pl.when(has_right)
        def _():
            l_copy(here, z).wait_recv()
            part[here, z] += arr[here, z]

        for target in range(line):
            @pl.when(target > z)
            def _(target=target):
                r_copy(here, target).wait_send()

            @pl.when(target < z)
            def _(target=target):
                l_copy(here, target).wait_send()

        kept = pl.ds(pl.multiple_of(x * rows, 8), rows)
        held[item] = part[here, z, pl.ds(pl.multiple_of((1 - x) * rows, 8), rows)]

        @pl.when(narrow)
        def _():
            start = (item % 2) * half + (chunks - 1 - item // 2) * LANES
            grad[0, :, lanes(start)] = part[here, z, kept]

        @pl.when(jnp.logical_not(narrow))
        def _():
            grad[layer, :, lanes(own_half + chunk * LANES)] = part[here, z, kept]
            add_squares(part[here, z])

        @pl.when(item + slots < items)
        def _():
            @pl.when(has_left)
            def _():
                signal(from_right, left)

            @pl.when(has_right)
            def _():
                signal(from_left, right)

    own_sq[...] = jnp.zeros_like(own_sq)
    for unit in range(line - 1):
        loads[unit].wait()
        send(jnp.int32(unit))
    for copy in loads[line - 1 : early_loads]:
        copy.wait()
    for unit in range(line - 1, AHEAD_UNITS):
        send(jnp.int32(unit))

    @pl.loop(0, items + line)
    def _(step):
        def guard(turn, action):
            item = turn - (turn > NARROW).astype(jnp.int32)
            real = jnp.logical_and(turn >= 0, turn != NARROW)
            pl.when(jnp.logical_and(real, item < items))(lambda: action(item))

        for stage in reversed(range(1, line - 1)):
            guard(step - stage, functools.partial(middle, stage=stage))
        guard(step, begin)
        guard(step - (line - 1), finish)

        @pl.loop(exchanged(step - 1), exchanged(step))
        def _(item):
            exchange(item)

    def spread(src, landing, send_sems, recv_sems, axis, index, size):
        copies = []
        for offset in range(1, size):
            copies.append(
                pltpu.make_async_remote_copy(
                    src_ref=src, dst_ref=landing.at[offset - 1],
                    send_sem=send_sems.at[offset - 1], recv_sem=recv_sems.at[offset - 1],
                    device_id={axis: lax.rem(index + offset, size)},
                    device_id_type=pl.DeviceIdType.MESH,
                )
            )
        for copy in copies:
            copy.start()
        for copy in copies:
            copy.wait()
        total = src[...]
        for offset in range(1, size):
            total = total + landing[offset - 1]
        return total

    sum_sq[...] = spread(own_sq, col_sq, qs_sem, qr_sem, "col", mine, col_count)
    total = spread(sum_sq, dp_sq, ds_sem, dr_sem, "dp", me, count)
    total = jnp.sum(jnp.sum(total, axis=0, keepdims=True), axis=1, keepdims=True)
    rms = jnp.sqrt(total / float(layers * features * cols * col_count) + norm_eps)
    clip = jnp.minimum(1.0, 1.0 / rms)
    moment_gain = clip * (1.0 - beta_one)
    square_gain = clip * clip * (1.0 - beta_two)
    gain_out[0] = jnp.broadcast_to(moment_gain, (8, LANES))
    gain_out[1] = jnp.broadcast_to(square_gain, (8, LANES))

    for index in range(layers):
        for kind in range(2):
            code_in(index, kind).wait()

    @pl.loop(NARROW, items)
    def _(item):
        f_copy(item, 1 - x).wait_recv()

    grad_copy = pltpu.make_async_copy(grad, grad_out, g_out)
    grad_copy.start()

    def moments_of(layer, at, height, piece):
        where = lanes(piece * LANES)
        value = grad[layer, pl.ds(at, height), where]
        moment = cot_raw[layer, pl.ds(at, height), where].astype(jnp.float32)
        square = cot_raw[layer, pl.ds(pl.multiple_of(rows + at, 16), height), where].astype(jnp.float32)
        moment = moment * row_values[0, layer, pl.ds(at, height)] + moment_gain * value
        square = square * row_values[1, layer, pl.ds(at, height)] + square_gain * (value * value)
        return moment, square

    @pl.loop(0, layers * (rows // PEAK_ROWS))
    def _(index):
        layer = index // (rows // PEAK_ROWS)
        at = pl.multiple_of(index % (rows // PEAK_ROWS) * PEAK_ROWS, PEAK_ROWS)
        high_moment = jnp.zeros((PEAK_ROWS, LANES), jnp.float32)
        high_square = jnp.zeros((PEAK_ROWS, LANES), jnp.float32)
        for piece in range(pieces):
            moment, square = moments_of(layer, at, PEAK_ROWS, piece)
            high_moment = jnp.maximum(high_moment, jnp.abs(moment))
            high_square = jnp.maximum(high_square, square)
        peak[0, layer, pl.ds(at, PEAK_ROWS)] = high_moment
        peak[1, layer, pl.ds(at, PEAK_ROWS)] = high_square

    for layer in range(layers):
        for kind in range(2):
            for at in range(0, rows, LANES):
                tile = peak[kind, layer, at : at + LANES].T
                row = jnp.max(tile, axis=0, keepdims=True)
                peak_rows[mine, kind, layer : layer + 1, at : at + LANES] = row

    def peak_copy(offset):
        return pltpu.make_async_remote_copy(
            src_ref=peak_rows.at[mine], dst_ref=peak_rows.at[mine],
            send_sem=ms_sem.at[offset - 1], recv_sem=mr_sem.at[mine],
            device_id={"col": lax.rem(mine + offset, col_count)},
            device_id_type=pl.DeviceIdType.MESH,
        )

    def peak_arrival(owner):
        return pltpu.make_async_remote_copy(
            src_ref=peak_rows.at[owner], dst_ref=peak_rows.at[owner],
            send_sem=ms_sem.at[0], recv_sem=mr_sem.at[owner],
            device_id={"col": partner}, device_id_type=pl.DeviceIdType.MESH,
        )

    for offset in range(1, col_count):
        peak_copy(offset).start()

    for offset in range(1, col_count):
        peak_arrival(lax.rem(mine + offset, col_count)).wait_recv()
    for owner in range(col_count):
        for layer in range(layers):
            new_moment_scale[layer, owner : owner + 1, :] = peak_rows[owner, 0, layer : layer + 1, :]
            new_square_scale[layer, owner : owner + 1, :] = peak_rows[owner, 1, layer : layer + 1, :]

    for offset in range(1, col_count):
        peak_copy(offset).wait_send()

    @pl.loop(units - SEND_SLOTS, units)
    def _(unit):
        act_copy(unit, 0).wait_send()

    @pl.loop(0, items)
    def _(item):
        n_copy(item).wait_send()

    grad_copy.wait()


def apply_kernel(
    grad_hbm, weights_hbm, moments_hbm, squares_hbm, gain,
    moment_scale, square_scale, moment_peak, square_peak,
    new_weights, new_moments, new_squares, new_moment_scale, new_square_scale,
    grad, row_values, weights, moments, squares, in_sem, out_sem,
):
    layers, rows, cols = grad.shape
    blocks = rows // APPLY_ROWS
    correct_one = 1.0 - beta_one**STEP
    correct_two = 1.0 - beta_two**STEP

    def block_of(index):
        at = pl.multiple_of(index % blocks * APPLY_ROWS, APPLY_ROWS)
        return index // blocks, pl.ds(at, APPLY_ROWS)

    def arrivals(index):
        layer, span = block_of(index)
        sems = in_sem.at[index]
        pairs = ((grad_hbm, grad), (moments_hbm, moments), (squares_hbm, squares), (weights_hbm, weights))
        return [
            pltpu.make_async_copy(src.at[layer, span], dst.at[layer, span], sems.at[number])
            for number, (src, dst) in enumerate(pairs)
        ]

    def departures(index):
        layer, span = block_of(index)
        pairs = ((weights, new_weights), (moments, new_moments), (squares, new_squares))
        return [
            pltpu.make_async_copy(src.at[layer, span], dst.at[layer, span], out_sem.at[index, number])
            for number, (src, dst) in enumerate(pairs)
        ]

    @pl.loop(0, layers * blocks)
    def _(index):
        for copy in arrivals(index):
            copy.start()

    new_moment_scale[...] = moment_peak[...]
    new_square_scale[...] = square_peak[...]
    mine = pl.ds(lax.axis_index("col"), 1)
    for layer in range(layers):
        lines = (
            moment_scale[layer, mine] * beta_one,
            square_scale[layer, mine] * beta_two,
            1.0 / (moment_peak[layer, mine] + scale_eps),
            1.0 / (square_peak[layer, mine] + scale_eps),
        )
        for kind, row in enumerate(lines):
            for at in range(0, rows, LANES):
                tile = jnp.broadcast_to(row[:, at : at + LANES], (LANES, LANES))
                row_values[kind, layer, at : at + LANES] = tile.T

    moment_gain = gain[0, 0:1, 0:1]
    square_gain = gain[1, 0:1, 0:1]

    @pl.loop(0, layers * blocks)
    def _(index):
        layer, span = block_of(index)
        for copy in arrivals(index):
            copy.wait()

        @pl.loop(0, APPLY_ROWS // STRIP_ROWS)
        def _(strip):
            at = index % blocks * APPLY_ROWS + strip * STRIP_ROWS
            span = pl.ds(pl.multiple_of(at, STRIP_ROWS), STRIP_ROWS)
            for piece in range(cols // LANES):
                where = pl.ds(piece * LANES, LANES)
                value = grad[layer, span, where]
                moment = moments[layer, span, where].astype(jnp.float32) * row_values[0, layer, span]
                square = squares[layer, span, where].astype(jnp.float32) * row_values[1, layer, span]
                moment = moment + moment_gain * value
                square = square + square_gain * (value * value)
                moments[layer, span, where] = (moment * row_values[2, layer, span]).astype(jnp.bfloat16)
                squares[layer, span, where] = (square * row_values[3, layer, span]).astype(jnp.bfloat16)
                level = square * (1.0 / correct_two)
                ratio = moment * (1.0 / correct_one) * pl.reciprocal(level * lax.rsqrt(level) + adam_eps)
                old = weights[layer, span, where]
                weights[layer, span, where] = old - learn_rate * (decay_rate * old + ratio)

        for copy in departures(index):
            copy.start()

    @pl.loop(0, layers * blocks)
    def _(index):
        for copy in departures(index):
            copy.wait()


def factor_step(
    mesh_shape, activations, cotangent, master_weights, moment_codes, square_codes, moment_scales, square_scales
):
    count = mesh_shape["dp"]
    col_count = mesh_shape["col"]
    layers, tokens, cols = activations.shape
    line = count // 2
    features = cotangent.shape[2]
    rows = features // count
    half = cols // 2
    slots = line + 1
    blocks = layers * rows // APPLY_ROWS
    scale_shape = jax.ShapeDtypeStruct((layers, col_count, rows), jnp.float32)
    items = NARROW + layers * (half // LANES) - NARROW // 2
    piece = (tokens, LANES)
    f32, bf16 = jnp.float32, jnp.bfloat16
    moment_scales = moment_scales.transpose(0, 2, 1)
    square_scales = square_scales.transpose(0, 2, 1)
    dma = pltpu.SemaphoreType.DMA
    regular = pltpu.SemaphoreType.REGULAR
    vmem = pl.BlockSpec(memory_space=pltpu.VMEM)
    hbm = pl.BlockSpec(memory_space=pl.ANY)
    gradient, gain, moment_peak, square_peak = pl.pallas_call(
        functools.partial(factor_kernel, count, col_count),
        out_shape=(
            jax.ShapeDtypeStruct((layers, rows, cols), f32),
            jax.ShapeDtypeStruct((2, 8, LANES), f32),
            scale_shape,
            scale_shape,
        ),
        in_specs=[hbm, hbm, hbm, hbm, vmem, vmem],
        out_specs=(hbm, vmem, vmem, vmem),
        scratch_shapes=[
            pltpu.VMEM((layers, rows, cols), f32),
            pltpu.VMEM((2, layers, rows, LANES), f32),
            pltpu.VMEM((2, layers, rows, LANES), f32),
            pltpu.VMEM((col_count, 2, layers, rows), f32),
            pltpu.VMEM((layers, tokens, features), bf16),
            pltpu.VMEM((layers, tokens, half), bf16),
            pltpu.VMEM((NARROW,) + piece, bf16),
            pltpu.VMEM((layers, features, 2 * tokens), bf16),
            pltpu.VMEM((layers, 2 * tokens, half), bf16),
            pltpu.VMEM((SEND_SLOTS,) + piece, f32),
            pltpu.VMEM((ACT_SLOTS,) + piece, f32),
            pltpu.VMEM((line, col_count) + piece, f32),
            pltpu.VMEM((slots, line, 2 * rows, LANES), f32),
            pltpu.VMEM((slots, line + 1, 2 * rows, LANES), f32),
            pltpu.VMEM((NARROW, rows, LANES), f32),
            pltpu.VMEM((items, rows, LANES), f32),
            pltpu.VMEM((8, LANES), f32),
            pltpu.VMEM((8, LANES), f32),
            pltpu.VMEM((col_count - 1, 8, LANES), f32),
            pltpu.VMEM((count - 1, 8, LANES), f32),
            dma((NARROW + line + 3 * layers - 1,)),
            dma((layers, 2)), dma,
            dma((col_count - 1,)), dma((col_count,)),
            dma((SEND_SLOTS,)), dma((ACT_SLOTS,)), dma((line,)),
            dma((line, col_count - 1)), dma((line, col_count)),
            dma((slots, line)), dma((slots, line)), dma((slots, line)), dma((slots, line)),
            dma((items,)), dma((items,)),
            dma((col_count - 1,)), dma((col_count - 1,)), dma((count - 1,)), dma((count - 1,)),
            regular((ACT_SLOTS,)), regular((line,)), regular, regular,
        ],
        compiler_params=pltpu.CompilerParams(
            collective_id=0, has_side_effects=True, vmem_limit_bytes=67043328
        ),
    )(
        cotangent, activations, moment_codes, square_codes,
        moment_scales, square_scales,
    )
    outs = pl.pallas_call(
        apply_kernel,
        out_shape=(
            jax.ShapeDtypeStruct(master_weights.shape, f32),
            jax.ShapeDtypeStruct(moment_codes.shape, bf16),
            jax.ShapeDtypeStruct(square_codes.shape, bf16),
            scale_shape,
            scale_shape,
        ),
        in_specs=[hbm, hbm, hbm, hbm, vmem, vmem, vmem, vmem, vmem],
        out_specs=(hbm, hbm, hbm, vmem, vmem),
        scratch_shapes=[
            pltpu.VMEM((layers, rows, cols), f32),
            pltpu.VMEM((4, layers, rows, LANES), f32),
            pltpu.VMEM((layers, rows, cols), f32),
            pltpu.VMEM((layers, rows, cols), bf16),
            pltpu.VMEM((layers, rows, cols), bf16),
            dma((blocks, 4)), dma((blocks, 3)),
        ],
        compiler_params=pltpu.CompilerParams(vmem_limit_bytes=APPLY_VMEM),
    )(
        gradient, master_weights, moment_codes, square_codes, gain,
        moment_scales, square_scales, moment_peak, square_peak,
    )
    return outs[:3] + (outs[3].transpose(0, 2, 1), outs[4].transpose(0, 2, 1))


def fits_factors(activations, cotangent, block_count, mesh_shape):
    count = mesh_shape["dp"]
    line = count // 2
    rows = cotangent.shape[2] // count
    chunks = activations.shape[2] // (2 * LANES)
    aligned = activations.shape[1] % LANES == 0 and activations.shape[2] % (2 * LANES) == 0
    layers, tokens, cols = activations.shape
    aligned = aligned and rows % LANES == 0 and cols % LANES == 0 and block_count == mesh_shape["col"]
    roomy = layers * rows <= tokens and cols <= cotangent.shape[2]
    return aligned and roomy and line >= 3 and 2 * rows == LANES * mesh_shape["col"] and mesh_shape["col"] % 2 == 0 and chunks - NARROW // 2 > line


def local(
    mesh_shape, activations, cotangent, master_weights, moment_codes, square_codes, moment_scales, square_scales
):
    layer_count = activations.shape[0]
    shard_rows = master_weights.shape[1]
    shard_cols = master_weights.shape[2]
    block_count = moment_scales.shape[2]
    if fits_factors(activations, cotangent, block_count, mesh_shape):
        return factor_step(
            mesh_shape, activations, cotangent, master_weights, moment_codes, square_codes,
            moment_scales, square_scales,
        )
    gradient, squares = reduced_gradient(activations, cotangent, mesh_shape)
    total_sq = jnp.sum(squares)
    rms = jnp.sqrt(total_sq / float(LAYERS * KV * D) + norm_eps)
    clip_factor = jnp.minimum(1.0, 1.0 / rms)
    correct_one = 1.0 - beta_one**STEP
    correct_two = 1.0 - beta_two**STEP
    own_block = lax.axis_index("col") * shard_cols // BLOCK
    selector = (jnp.arange(block_count, dtype=jnp.int32) == own_block).astype(jnp.float32)
    outs_weights, outs_mcode, outs_scode, outs_mscale, outs_sscale = ([], [], [], [], [])
    for layer_index in range(layer_count):
        moment_scale = jnp.sum(moment_scales[layer_index] * selector, axis=1)
        square_scale = jnp.sum(square_scales[layer_index] * selector, axis=1)
        old_moment = moment_codes[layer_index].astype(jnp.float32) * moment_scale[:, None]
        old_square = square_codes[layer_index].astype(jnp.float32) * square_scale[:, None]
        grad_now = clip_factor * gradient[layer_index]
        new_moment = beta_one * old_moment + (1.0 - beta_one) * grad_now
        new_square = beta_two * old_square + (1.0 - beta_two) * grad_now * grad_now
        moment_part = jnp.max(jnp.abs(new_moment), axis=1)[:, None] * selector
        square_part = jnp.max(new_square, axis=1)[:, None] * selector
        moment, square, moment_part, square_part = (
            new_moment,
            new_square,
            moment_part,
            square_part,
        )
        moment_max, square_max = lax.pmax((moment_part, square_part), "col")
        moment_div = jnp.sum(moment_max * selector, axis=1)[:, None]
        square_div = jnp.sum(square_max * selector, axis=1)[:, None]
        moment_out = (moment / (moment_div + scale_eps)).astype(jnp.bfloat16)
        square_out = (square / (square_div + scale_eps)).astype(jnp.bfloat16)
        ratio = moment / correct_one / (jnp.sqrt(square / correct_two) + adam_eps)
        weights = master_weights[layer_index]
        results = (weights - learn_rate * (decay_rate * weights + ratio), moment_out, square_out)
        outs_weights.append(results[0])
        outs_mcode.append(results[1])
        outs_scode.append(results[2])
        outs_mscale.append(moment_max)
        outs_sscale.append(square_max)
    return (
        jnp.stack(outs_weights),
        jnp.stack(outs_mcode),
        jnp.stack(outs_scode),
        jnp.stack(outs_mscale),
        jnp.stack(outs_sscale),
    )


def solution(mesh):
    in_specs = (
        P(None, "dp", "col"),
        P(None, "dp", None),
        P(None, "dp", "col"),
        P(None, "dp", "col"),
        P(None, "dp", "col"),
        P(None, "dp", None),
        P(None, "dp", None),
    )
    out_specs = (
        P(None, "dp", "col"),
        P(None, "dp", "col"),
        P(None, "dp", "col"),
        P(None, "dp", None),
        P(None, "dp", None),
    )
    return jax.shard_map(functools.partial(local, dict(mesh.shape)), mesh=mesh, in_specs=in_specs, out_specs=out_specs, check_vma=False)
```

```python
import functools

import jax
import jax.numpy as jnp
from jax import lax
from jax.experimental import pallas as pl
from jax.experimental.pallas import tpu as pltpu
from jax.sharding import PartitionSpec as P

D = 8192
KV = 2048
BLOCK = 2048
LAYERS = 2
STEP = 10


beta_one = 0.9
beta_two = 0.999
learn_rate = 0.001
decay_rate = 0.1
adam_eps = 1e-08
scale_eps = 1e-06
norm_eps = 1e-06

LANES = 128
AHEAD = 3
XSLOTS = 4


def reduce_kernel(
    count, col_count, cot_ref, act_ref, out_ref, sq_ref,
    xs, xr, part, arr, bs, br, own_sq, sum_sq, col_sq, dp_sq,
    xs_sem, xr_sem, rs_sem, rr_sem, ls_sem, ll_sem, bs_sem, br_sem,
    cs_sem, cr_sem, ds_sem, dr_sem, x_free, from_right, from_left,
):
    layers, pairs, line, rows, tokens = cot_ref.shape
    cols = act_ref.shape[2]
    slots = part.shape[0]
    wide_per = cols // (2 * LANES) - 1
    per_layer = wide_per + 2
    period = (per_layer + 1) // 2
    items = layers * per_layer
    wides = layers * wide_per
    me = lax.axis_index("dp")
    z = me // 2
    x = me % 2
    peer = 2 * z + 1 - x
    right = jnp.minimum(z + 1, line - 1) * 2 + x
    left = jnp.maximum(z - 1, 0) * 2 + x
    has_right = z < line - 1
    has_left = z > 0
    mirror = line - 1 - z

    def signal(sem, where):
        pl.semaphore_signal(
            sem, inc=1, device_id={"dp": where}, device_id_type=pl.DeviceIdType.MESH
        )

    barrier = pltpu.get_barrier_semaphore()
    mine = lax.axis_index("col")
    for offset in range(1, count):
        signal(barrier, lax.rem(me + offset, count))
    for offset in range(1, col_count):
        pl.semaphore_signal(
            barrier, inc=1, device_id={"col": lax.rem(mine + offset, col_count)},
            device_id_type=pl.DeviceIdType.MESH,
        )
    pl.semaphore_wait(barrier, count + col_count - 2)

    def remote(src, dst, send, recv, where):
        return pltpu.make_async_remote_copy(
            src_ref=src, dst_ref=dst, send_sem=send, recv_sem=recv,
            device_id={"dp": where}, device_id_type=pl.DeviceIdType.MESH,
        )

    def describe(item):
        layer = item // per_layer
        place = item % per_layer
        narrow = place % period == 0
        wide_at = place - (place + period - 1) // period
        narrow_at = place // period
        return layer, narrow, wide_at, narrow_at

    def x_copy(number):
        slot = number % XSLOTS
        return remote(xs.at[slot], xr.at[slot], xs_sem.at[slot], xr_sem.at[slot], peer)

    def r_copy(slot, target):
        return remote(
            part.at[slot, target], arr.at[slot, target + 1],
            rs_sem.at[slot, target], rr_sem.at[slot, target], right,
        )

    def l_copy(slot, target):
        return remote(
            part.at[slot, target], arr.at[slot, target],
            ls_sem.at[slot, target], ll_sem.at[slot, target], left,
        )

    def b_copy(number):
        return remote(
            bs.at[number], br.at[number], bs_sem.at[number], br_sem.at[number], peer
        )

    def product(layer, pair, target, start, width):
        return jnp.dot(
            cot_ref[layer, pair, target],
            act_ref[layer, :, pl.ds(pl.multiple_of(start, LANES), width)],
            preferred_element_type=jnp.float32,
        )

    def send_wide(item):
        layer, narrow, wide_at, _ = describe(item)

        @pl.when(jnp.logical_not(narrow))
        def _():
            number = layer * wide_per + wide_at
            slot = number % XSLOTS

            @pl.loop(0, line)
            def _(target):
                value = product(layer, 1 - x, target, wide_at * 2 * LANES, 2 * LANES)
                xs[slot, target, 0] = value[:, :LANES]
                xs[slot, target, 1] = value[:, LANES:]

            @pl.when(number >= XSLOTS)
            def _():
                pl.semaphore_wait(x_free, 1)

            x_copy(number).start()

    def form(item):
        layer, narrow, wide_at, narrow_at = describe(item)
        here = item % slots

        @pl.when(item >= slots)
        def _():
            @pl.when(has_right)
            def _():
                pl.semaphore_wait(from_right, 1)

            @pl.when(has_left)
            def _():
                pl.semaphore_wait(from_left, 1)

        @pl.when(narrow)
        def _():
            start = wide_per * 2 * LANES + narrow_at * LANES

            @pl.loop(0, line)
            def _(target):
                part[here, target, 0] = product(layer, 0, target, start, LANES)
                part[here, target, 1] = product(layer, 1, target, start, LANES)

        @pl.when(jnp.logical_not(narrow))
        def _():
            number = layer * wide_per + wide_at
            slot = number % XSLOTS
            x_copy(number).wait()

            @pl.loop(0, line)
            def _(target):
                value = product(layer, x, target, wide_at * 2 * LANES, 2 * LANES)
                part[here, target, 0] = value[:, :LANES] + xr[slot, target, 0]
                part[here, target, 1] = value[:, LANES:] + xr[slot, target, 1]

            @pl.when(number + XSLOTS < wides)
            def _():
                signal(x_free, peer)

    def hop(item, stage):
        here = item % slots

        @pl.when(z <= stage)
        def _():
            target = line - 1 - stage + z
            if stage > 0:
                @pl.when(has_left)
                def _():
                    r_copy(here, target).wait_recv()
                    part[here, target] += arr[here, target + 1]

            r_copy(here, target).start()

        @pl.when(mirror <= stage)
        def _():
            target = stage - mirror
            if stage > 0:
                @pl.when(has_right)
                def _():
                    l_copy(here, target).wait_recv()
                    part[here, target] += arr[here, target]

            l_copy(here, target).start()

    def finish(item):
        layer, narrow, wide_at, narrow_at = describe(item)
        here = item % slots

        @pl.when(has_left)
        def _():
            r_copy(here, z).wait_recv()
            part[here, z] += arr[here, z + 1]

        @pl.when(has_right)
        def _():
            l_copy(here, z).wait_recv()
            part[here, z] += arr[here, z]

        for target in range(line):
            @pl.when(target > z)
            def _(target=target):
                r_copy(here, target).wait_send()

            @pl.when(target < z)
            def _(target=target):
                l_copy(here, target).wait_send()

        @pl.when(narrow)
        def _():
            number = layer * 2 + narrow_at
            start = wide_per * 2 * LANES + narrow_at * LANES
            bs[number] = part[here, z, 1 - x]
            b_copy(number).start()
            out_ref[layer, :, pl.ds(pl.multiple_of(start, LANES), LANES)] = part[here, z, x]

        @pl.when(jnp.logical_not(narrow))
        def _():
            for half in range(2):
                start = wide_at * 2 * LANES + half * LANES
                out_ref[layer, :, pl.ds(pl.multiple_of(start, LANES), LANES)] = part[here, z, half]

        @pl.when(item + slots < items)
        def _():
            @pl.when(has_left)
            def _():
                signal(from_right, left)

            @pl.when(has_right)
            def _():
                signal(from_left, right)

    for item in range(1, AHEAD):
        send_wide(jnp.int32(item))

    @pl.loop(0, items + line - 1)
    def _(step):
        def guard(item, action):
            pl.when(jnp.logical_and(item >= 0, item < items))(lambda: action(item))

        guard(step + AHEAD, send_wide)
        guard(step - (line - 1), finish)
        for stage in reversed(range(1, line - 1)):
            guard(step - stage, functools.partial(hop, stage=stage))

        def begin(item):
            form(item)
            hop(item, 0)

        guard(step, begin)

    for number in range(2 * layers):
        b_copy(number).wait()
        start = wide_per * 2 * LANES + (number % 2) * LANES
        out_ref[number // 2, :, start : start + LANES] += br[number]

    def square_rows(index, total):
        layer = index // (rows // 8)
        at = pl.multiple_of(index % (rows // 8) * 8, 8)
        for piece in range(cols // LANES):
            value = out_ref[layer, pl.ds(at, 8), piece * LANES : (piece + 1) * LANES]
            total = total + value * value
        return total

    def spread(src, landing, send, recv, axis, index, size):
        copies = []
        for offset in range(1, size):
            copies.append(
                pltpu.make_async_remote_copy(
                    src_ref=src, dst_ref=landing.at[offset - 1],
                    send_sem=send.at[offset - 1], recv_sem=recv.at[offset - 1],
                    device_id={axis: lax.rem(index + offset, size)},
                    device_id_type=pl.DeviceIdType.MESH,
                )
            )
        for copy in copies:
            copy.start()
        for copy in copies:
            copy.wait()
        total = src[...]
        for offset in range(1, size):
            total = total + landing[offset - 1]
        return total

    own_sq[...] = lax.fori_loop(
        0, layers * rows // 8, square_rows, jnp.zeros((8, LANES), jnp.float32)
    )
    sum_sq[...] = spread(own_sq, col_sq, cs_sem, cr_sem, "col", mine, col_count)
    sq_ref[...] = spread(sum_sq, dp_sq, ds_sem, dr_sem, "dp", me, count)


def reduced_gradient(activations, cotangent, mesh_shape):
    count = mesh_shape["dp"]
    col_count = mesh_shape["col"]
    layers, tokens, cols = activations.shape
    line = count // 2
    rows = cotangent.shape[2] // count
    slots = line + 2
    cot = cotangent.reshape(layers, tokens, line, 2, rows).transpose(0, 3, 2, 4, 1)
    block = (line, 2, rows, LANES)
    dma = pltpu.SemaphoreType.DMA
    vmem = pl.BlockSpec(memory_space=pltpu.VMEM)
    return pl.pallas_call(
        functools.partial(reduce_kernel, count, col_count),
        out_shape=(
            jax.ShapeDtypeStruct((layers, rows, cols), jnp.float32),
            jax.ShapeDtypeStruct((8, LANES), jnp.float32),
        ),
        in_specs=[vmem, vmem],
        out_specs=(vmem, vmem),
        scratch_shapes=[
            pltpu.VMEM((XSLOTS,) + block, jnp.float32),
            pltpu.VMEM((XSLOTS,) + block, jnp.float32),
            pltpu.VMEM((slots,) + block, jnp.float32),
            pltpu.VMEM((slots, line + 1) + block[1:], jnp.float32),
            pltpu.VMEM((2 * layers, rows, LANES), jnp.float32),
            pltpu.VMEM((2 * layers, rows, LANES), jnp.float32),
            pltpu.VMEM((8, LANES), jnp.float32),
            pltpu.VMEM((8, LANES), jnp.float32),
            pltpu.VMEM((col_count - 1, 8, LANES), jnp.float32),
            pltpu.VMEM((count - 1, 8, LANES), jnp.float32),
            dma((XSLOTS,)), dma((XSLOTS,)),
            dma((slots, line)), dma((slots, line)), dma((slots, line)), dma((slots, line)),
            dma((2 * layers,)), dma((2 * layers,)),
            dma((col_count - 1,)), dma((col_count - 1,)), dma((count - 1,)), dma((count - 1,)),
            pltpu.SemaphoreType.REGULAR, pltpu.SemaphoreType.REGULAR, pltpu.SemaphoreType.REGULAR,
        ],
        compiler_params=pltpu.CompilerParams(
            collective_id=0, has_side_effects=True, vmem_limit_bytes=62 * 2**20
        ),
    )(cot, activations)


AHEAD_UNITS = 5
SEND_SLOTS = 6
ACT_SLOTS = 5
NARROW = 2
RELEASE = 3
SPLITS = 2
PEAK_ROWS = 32
APPLY_ROWS = 64
STRIP_ROWS = 32
APPLY_VMEM = 62 * 2**20


def factor_kernel(
    count, col_count, cot_hbm, act_hbm, moments_hbm, squares_hbm, moment_scale, square_scale,
    grad_out, gain_out, new_moment_scale, new_square_scale, grad,
    row_values, peak, peak_rows,
    cot_raw, act_raw, narrow_act, cot_t, act_cat, xs, xr, crx, part, arr, narrow_in, held,
    own_sq, sum_sq, col_sq, dp_sq,
    ld_sem, c_in, g_out, ms_sem, mr_sem, xs_sem, xr_sem, pr_sem, cs_sem, cr_sem, rs_sem, rr_sem, ls_sem, ll_sem, fs_sem, fr_sem,
    qs_sem, qr_sem, ds_sem, dr_sem, act_free, cot_free, from_right, from_left,
):
    layers, tokens, cols = act_hbm.shape
    half = cols // 2
    line = count // 2
    pair_rows = part.shape[2]
    rows = pair_rows // 2
    slots = part.shape[0]
    chunks = half // LANES
    first_chunks = chunks - NARROW // 2
    wides = first_chunks + (layers - 1) * chunks
    items = NARROW + wides
    first_units = first_chunks + line
    layer_units = chunks + line
    units = first_units + (layers - 1) * layer_units
    all_sent = items - chunks + line - 2
    groups = col_count // 2
    pieces = cols // LANES
    features = cot_hbm.shape[2]
    me = lax.axis_index("dp")
    mine = lax.axis_index("col")
    z = me // 2
    x = me % 2
    peer = 2 * z + 1 - x
    partner = mine + 1 - 2 * (mine % 2)
    right = jnp.minimum(z + 1, line - 1) * 2 + x
    left = jnp.maximum(z - 1, 0) * 2 + x
    has_right = z < line - 1
    has_left = z > 0
    mirror = line - 1 - z
    own_half = pl.multiple_of(x * half, LANES)
    peer_half = pl.multiple_of((1 - x) * half, LANES)

    def lanes(start, width=LANES):
        return pl.ds(pl.multiple_of(start, LANES), width)

    def signal(sem, where):
        pl.semaphore_signal(
            sem, inc=1, device_id={"dp": where}, device_id_type=pl.DeviceIdType.MESH
        )

    loads = []

    def load(src, dst):
        copy = pltpu.make_async_copy(src, dst, ld_sem.at[len(loads)])
        copy.start()
        loads.append(copy)

    def block_target(place):
        after = line - 1 - z
        rising = jnp.where(place < after, line - 1 - place, place - after)
        falling = jnp.where(place < z, place, line - 1 - (place - z))
        other = jnp.where(z < line // 2, rising, falling)
        return jnp.where(place < line - 1, other, z)

    for place in range(line):
        block = lanes(block_target(place) * pair_rows, pair_rows)
        load(cot_hbm.at[0, :, block], cot_raw.at[0, :, block])
    load(act_hbm.at[0, :, pl.ds(peer_half, half)], act_raw.at[0])
    for index in range(NARROW):
        start = (index % 2) * half + (chunks - 1 - index // 2) * LANES
        load(act_hbm.at[0, :, lanes(start)], narrow_act.at[index])
    for layer in range(layers):
        if layer > 0:
            load(cot_hbm.at[layer], cot_raw.at[layer])
            load(act_hbm.at[layer, :, pl.ds(peer_half, half)], act_raw.at[layer])
        load(act_hbm.at[layer, :, pl.ds(own_half, half)], act_cat.at[layer, pl.ds(0, tokens)])

    early_loads = line + 1 + NARROW

    barrier = pltpu.get_barrier_semaphore()
    signal(barrier, peer)

    @pl.when(has_right)
    def _():
        signal(barrier, right)

    @pl.when(has_left)
    def _():
        signal(barrier, left)

    for offset in range(1, col_count):
        pl.semaphore_signal(
            barrier, inc=1, device_id={"col": lax.rem(mine + offset, col_count)},
            device_id_type=pl.DeviceIdType.MESH,
        )
    sides = has_right.astype(jnp.int32) + has_left.astype(jnp.int32)
    pl.semaphore_wait(barrier, col_count + sides)

    def remote(src, dst, send, recv, where):
        return pltpu.make_async_remote_copy(
            src_ref=src, dst_ref=dst, send_sem=send, recv_sem=recv,
            device_id={"dp": where}, device_id_type=pl.DeviceIdType.MESH,
        )

    def describe(item):
        number = item - NARROW
        narrow = item < NARROW
        later = jnp.maximum(number - first_chunks, 0)
        layer = jnp.where(number < first_chunks, 0, 1 + later // chunks)
        chunk = jnp.where(number < first_chunks, number, later % chunks)
        return layer, narrow, chunk

    def unit_base(layer):
        return jnp.where(layer == 0, 0, first_units + (layer - 1) * layer_units)

    def act_number(layer, chunk):
        return jnp.where(layer == 0, chunk, first_chunks + (layer - 1) * chunks + chunk)

    def act_copy(unit, number):
        here = unit % SEND_SLOTS
        slot = number % ACT_SLOTS
        return remote(xs.at[here], xr.at[slot], xs_sem.at[here], xr_sem.at[slot], peer)

    def cot_copy(unit, place, split):
        here = unit % SEND_SLOTS
        span = pl.ds(split * (tokens // SPLITS), tokens // SPLITS)
        return remote(
            xs.at[here, span], crx.at[place, mine, span], xs_sem.at[here], pr_sem.at[place, split], peer
        )

    def col_copy(place, owner, number, where, split):
        piece = crx.at[place, owner, pl.ds(split * (tokens // SPLITS), tokens // SPLITS)]
        return pltpu.make_async_remote_copy(
            src_ref=piece, dst_ref=piece,
            send_sem=cs_sem.at[place, number, split], recv_sem=cr_sem.at[place, owner, split],
            device_id={"col": where}, device_id_type=pl.DeviceIdType.MESH,
        )

    def far(index):
        return lax.rem(mine + 2 * index, col_count)

    def r_copy(slot, target):
        return remote(
            part.at[slot, target], arr.at[slot, target + 1],
            rs_sem.at[slot, target], rr_sem.at[slot, target], right,
        )

    def l_copy(slot, target):
        return remote(
            part.at[slot, target], arr.at[slot, target],
            ls_sem.at[slot, target], ll_sem.at[slot, target], left,
        )

    def n_copy(item):
        where = narrow_in.at[jnp.minimum(item, NARROW - 1)]
        return remote(held.at[item], where, fs_sem.at[item], fr_sem.at[item], peer)

    def f_copy(item, side):
        layer, narrow, chunk = describe(item)
        where = grad.at[layer, :, lanes(side * half + chunk * LANES)]
        return remote(held.at[item], where, fs_sem.at[item], fr_sem.at[item], peer)

    def exchange(item):
        @pl.when(item < NARROW)
        def _():
            n_copy(item).start()

        @pl.when(item >= NARROW)
        def _():
            f_copy(item, x).start()

    def exchanged(step):
        done = jnp.minimum(step - (line - 1), RELEASE * (step - 1 - all_sent))
        return jnp.clip(done, 0, items)

    def send(unit):
        @pl.when(unit < units)
        def _():
            layer = jnp.where(unit < first_units, 0, 1 + (unit - first_units) // layer_units)
            index = unit - unit_base(layer)
            mixed = index < 2 * line - 1
            is_cot = jnp.logical_and(mixed, index % 2 == 0)
            here = unit % SEND_SLOTS

            @pl.when(unit >= SEND_SLOTS)
            def _():
                act_copy(unit, 0).wait_send()

            @pl.when(is_cot)
            def _():
                place = index // 2
                start = block_target(place) * pair_rows + mine * LANES
                xs[here] = cot_raw[layer, :, lanes(start)].astype(jnp.float32)

                @pl.when(layer > 0)
                def _():
                    pl.semaphore_wait(cot_free.at[place], 1)

                for split in range(SPLITS):
                    cot_copy(unit, place, split).start()

            @pl.when(jnp.logical_not(is_cot))
            def _():
                chunk = jnp.where(mixed, index // 2, index - line)
                number = act_number(layer, chunk)
                xs[here] = act_raw[layer, :, lanes(chunk * LANES)].astype(jnp.float32)

                @pl.when(number >= ACT_SLOTS)
                def _():
                    pl.semaphore_wait(act_free.at[number % ACT_SLOTS], 1)

                act_copy(unit, number).start()

    def forward(layer, place):
        for split in range(SPLITS):
            cot_copy(0, place, split).wait_recv()
            for index in range(1, groups):
                col_copy(place, mine, index, far(index), split).start()
            col_copy(place, mine, 0, partner, split).start()
        send(unit_base(layer) + 2 * place + AHEAD_UNITS)

    def relay(place):
        for split in range(SPLITS):
            for index in range(1, groups):
                col_copy(place, far(index), groups - 1 + index, partner, split).wait_recv()
                col_copy(place, far(index), groups - 1 + index, partner, split).start()

    def prepare(layer, place):
        base = block_target(place) * pair_rows

        @pl.loop(0, col_count)
        def _(member):
            start = base + member * LANES
            value = cot_raw[layer, :, lanes(start)].astype(jnp.float32)
            cot_t[layer, lanes(start), pl.ds(0, tokens)] = value.T.astype(jnp.bfloat16)

    def absorb(layer, place):
        @pl.when(layer > 0)
        def _():
            prepare(layer, place)

        base = block_target(place) * pair_rows
        for split in range(SPLITS):
            col_copy(place, partner, 0, partner, split).wait_recv()
            for index in range(1, groups):
                col_copy(place, lax.rem(partner + 2 * index, col_count), 0, partner, split).wait_recv()

        @pl.loop(0, col_count)
        def _(owner):
            source = crx[place, owner]
            cot_t[layer, lanes(base + owner * LANES), pl.ds(tokens, tokens)] = source.T.astype(jnp.bfloat16)

        for number in range(col_count - 1):
            for split in range(SPLITS):
                col_copy(place, mine, number, partner, split).wait_send()

        @pl.when(layer < layers - 1)
        def _():
            signal(cot_free.at[place], peer)

    def take(layer, chunk):
        number = act_number(layer, chunk)
        slot = number % ACT_SLOTS
        act_copy(0, number).wait_recv()
        act_cat[layer, pl.ds(tokens, tokens), lanes(chunk * LANES)] = xr[slot].astype(jnp.bfloat16)

        @pl.when(number + ACT_SLOTS < wides)
        def _():
            signal(act_free.at[slot], peer)

        index = jnp.where(chunk < line - 1, 2 * chunk + 1, chunk + line)
        send(unit_base(layer) + index + AHEAD_UNITS)

    def form(item, target):
        layer, narrow, chunk = describe(item)
        here = item % slots
        at = pl.ds(pl.multiple_of(target * pair_rows, LANES), pair_rows)

        @pl.when(narrow)
        def _():
            part[here, target] = jnp.dot(
                cot_t[0, at, pl.ds(0, tokens)], narrow_act[jnp.minimum(item, NARROW - 1)],
                preferred_element_type=jnp.float32,
            )

        @pl.when(jnp.logical_not(narrow))
        def _():
            part[here, target] = jnp.dot(
                cot_t[layer, at, :], act_cat[layer, :, lanes(chunk * LANES)],
                preferred_element_type=jnp.float32,
            )

    def opens(item):
        layer, narrow, chunk = describe(item)
        return layer, jnp.logical_and(jnp.logical_not(narrow), chunk == 0)

    def ready(item, place):
        @pl.when(item == 0)
        def _():
            prepare(0, place)

        layer, first = opens(item)

        @pl.when(first)
        def _():
            if place == 0:
                @pl.when(layer == 0)
                def _():
                    forward(layer, 0)

            relay(place)
            absorb(layer, place)

    def hop(item, stage):
        here = item % slots

        @pl.when(z <= stage)
        def _():
            target = line - 1 - stage + z
            form(item, target)
            if stage > 0:
                @pl.when(has_left)
                def _():
                    r_copy(here, target).wait_recv()
                    part[here, target] += arr[here, target + 1]

            r_copy(here, target).start()

        @pl.when(mirror <= stage)
        def _():
            target = stage - mirror
            form(item, target)
            if stage > 0:
                @pl.when(has_right)
                def _():
                    l_copy(here, target).wait_recv()
                    part[here, target] += arr[here, target]

            l_copy(here, target).start()

    def code_in(layer, kind):
        source = (moments_hbm, squares_hbm)[kind].at[layer]
        return pltpu.make_async_copy(
            source, cot_raw.at[layer, pl.ds(kind * rows, rows), pl.ds(0, cols)], c_in.at[layer, kind]
        )

    def spread_scales():
        for layer in range(layers):
            for kind in range(2):
                source = (moment_scale, square_scale)[kind]
                factor = (beta_one, beta_two)[kind]
                row = source[layer, pl.ds(mine, 1), :] * factor
                for part_at in range(0, rows, LANES):
                    tile = jnp.broadcast_to(row[:, part_at : part_at + LANES], (LANES, LANES))
                    row_values[kind, layer, part_at : part_at + LANES] = tile.T

    def begin(item):
        layer, narrow, chunk = describe(item)
        ready(item, 0)

        @pl.when(jnp.logical_not(narrow))
        def _():
            take(layer, chunk)

        @pl.when(item >= slots)
        def _():
            @pl.when(has_right)
            def _():
                pl.semaphore_wait(from_right, 1)

            @pl.when(has_left)
            def _():
                pl.semaphore_wait(from_left, 1)

        hop(item, 0)

        @pl.when(item == 1)
        def _():
            for copy in loads[early_loads:]:
                copy.wait()

        @pl.when(item == items - 2)
        def _():
            spread_scales()
            for index in range(layers):
                for kind in range(2):
                    code_in(index, kind).start()

        @pl.when(jnp.logical_and(jnp.logical_not(narrow), chunk < line - 1))
        def _():
            forward(layer, chunk + 1)

        next_layer, next_first = opens(item + 1)

        @pl.when(jnp.logical_and(next_first, jnp.logical_and(next_layer > 0, item + 1 < items)))
        def _():
            forward(next_layer, 0)

    def middle(item, stage):
        ready(item, stage)
        hop(item, stage)

    def add_squares(value):
        rows8 = value.reshape(value.shape[0] // 8, 8, LANES)
        own_sq[...] += jnp.sum(rows8 * rows8, axis=0)

    def join_narrow():
        for item in range(NARROW):
            n_copy(item).wait_recv()
            where = lanes((item % 2) * half + (chunks - 1 - item // 2) * LANES)
            value = grad[0, :, where] + narrow_in[item]
            grad[0, :, where] = value
            add_squares(value)

    def finish(item):
        layer, narrow, chunk = describe(item)
        here = item % slots
        ready(item, line - 1)

        @pl.when(item == items - 2)
        def _():
            join_narrow()

        form(item, z)

        @pl.when(has_left)
        def _():
            r_copy(here, z).wait_recv()
            part[here, z] += arr[here, z + 1]

        @pl.when(has_right)
        def _():
            l_copy(here, z).wait_recv()
            part[here, z] += arr[here, z]

        for target in range(line):
            @pl.when(target > z)
            def _(target=target):
                r_copy(here, target).wait_send()

            @pl.when(target < z)
            def _(target=target):
                l_copy(here, target).wait_send()

        kept = pl.ds(pl.multiple_of(x * rows, 8), rows)
        held[item] = part[here, z, pl.ds(pl.multiple_of((1 - x) * rows, 8), rows)]

        @pl.when(narrow)
        def _():
            start = (item % 2) * half + (chunks - 1 - item // 2) * LANES
            grad[0, :, lanes(start)] = part[here, z, kept]

        @pl.when(jnp.logical_not(narrow))
        def _():
            grad[layer, :, lanes(own_half + chunk * LANES)] = part[here, z, kept]
            add_squares(part[here, z])

        @pl.when(item + slots < items)
        def _():
            @pl.when(has_left)
            def _():
                signal(from_right, left)

            @pl.when(has_right)
            def _():
                signal(from_left, right)

    own_sq[...] = jnp.zeros_like(own_sq)
    loads[0].wait()
    send(jnp.int32(0))
    for copy in loads[1:early_loads]:
        copy.wait()
    for unit in range(1, AHEAD_UNITS):
        send(jnp.int32(unit))

    @pl.loop(0, items + line)
    def _(step):
        def guard(turn, action):
            item = turn - (turn > NARROW).astype(jnp.int32)
            real = jnp.logical_and(turn >= 0, turn != NARROW)
            pl.when(jnp.logical_and(real, item < items))(lambda: action(item))

        for stage in range(1, line - 1):
            guard(step - stage, functools.partial(middle, stage=stage))
        guard(step, begin)
        guard(step - (line - 1), finish)

        @pl.loop(exchanged(step - 1), exchanged(step))
        def _(item):
            exchange(item)

    def spread(src, landing, send_sems, recv_sems, axis, index, size):
        copies = []
        for offset in range(1, size):
            copies.append(
                pltpu.make_async_remote_copy(
                    src_ref=src, dst_ref=landing.at[offset - 1],
                    send_sem=send_sems.at[offset - 1], recv_sem=recv_sems.at[offset - 1],
                    device_id={axis: lax.rem(index + offset, size)},
                    device_id_type=pl.DeviceIdType.MESH,
                )
            )
        for copy in copies:
            copy.start()
        for copy in copies:
            copy.wait()
        total = src[...]
        for offset in range(1, size):
            total = total + landing[offset - 1]
        return total

    sum_sq[...] = spread(own_sq, col_sq, qs_sem, qr_sem, "col", mine, col_count)
    total = spread(sum_sq, dp_sq, ds_sem, dr_sem, "dp", me, count)
    total = jnp.sum(jnp.sum(total, axis=0, keepdims=True), axis=1, keepdims=True)
    rms = jnp.sqrt(total / float(layers * features * cols * col_count) + norm_eps)
    clip = jnp.minimum(1.0, 1.0 / rms)
    moment_gain = clip * (1.0 - beta_one)
    square_gain = clip * clip * (1.0 - beta_two)
    gain_out[0] = jnp.broadcast_to(moment_gain, (8, LANES))
    gain_out[1] = jnp.broadcast_to(square_gain, (8, LANES))

    for index in range(layers):
        for kind in range(2):
            code_in(index, kind).wait()

    @pl.loop(NARROW, items)
    def _(item):
        f_copy(item, 1 - x).wait_recv()

    grad_copy = pltpu.make_async_copy(grad, grad_out, g_out)
    grad_copy.start()

    def moments_of(layer, at, height, piece):
        where = lanes(piece * LANES)
        value = grad[layer, pl.ds(at, height), where]
        moment = cot_raw[layer, pl.ds(at, height), where].astype(jnp.float32)
        square = cot_raw[layer, pl.ds(pl.multiple_of(rows + at, 16), height), where].astype(jnp.float32)
        moment = moment * row_values[0, layer, pl.ds(at, height)] + moment_gain * value
        square = square * row_values[1, layer, pl.ds(at, height)] + square_gain * (value * value)
        return moment, square

    @pl.loop(0, layers * (rows // PEAK_ROWS))
    def _(index):
        layer = index // (rows // PEAK_ROWS)
        at = pl.multiple_of(index % (rows // PEAK_ROWS) * PEAK_ROWS, PEAK_ROWS)
        high_moment = jnp.zeros((PEAK_ROWS, LANES), jnp.float32)
        high_square = jnp.zeros((PEAK_ROWS, LANES), jnp.float32)
        for piece in range(pieces):
            moment, square = moments_of(layer, at, PEAK_ROWS, piece)
            high_moment = jnp.maximum(high_moment, jnp.abs(moment))
            high_square = jnp.maximum(high_square, square)
        peak[0, layer, pl.ds(at, PEAK_ROWS)] = high_moment
        peak[1, layer, pl.ds(at, PEAK_ROWS)] = high_square

    for layer in range(layers):
        for kind in range(2):
            for at in range(0, rows, LANES):
                tile = peak[kind, layer, at : at + LANES].T
                row = jnp.max(tile, axis=0, keepdims=True)
                peak_rows[mine, kind, layer : layer + 1, at : at + LANES] = row

    def peak_copy(offset):
        return pltpu.make_async_remote_copy(
            src_ref=peak_rows.at[mine], dst_ref=peak_rows.at[mine],
            send_sem=ms_sem.at[offset - 1], recv_sem=mr_sem.at[mine],
            device_id={"col": lax.rem(mine + offset, col_count)},
            device_id_type=pl.DeviceIdType.MESH,
        )

    def peak_arrival(owner):
        return pltpu.make_async_remote_copy(
            src_ref=peak_rows.at[owner], dst_ref=peak_rows.at[owner],
            send_sem=ms_sem.at[0], recv_sem=mr_sem.at[owner],
            device_id={"col": partner}, device_id_type=pl.DeviceIdType.MESH,
        )

    for offset in range(1, col_count):
        peak_copy(offset).start()

    for offset in range(1, col_count):
        peak_arrival(lax.rem(mine + offset, col_count)).wait_recv()
    for owner in range(col_count):
        for layer in range(layers):
            new_moment_scale[layer, owner : owner + 1, :] = peak_rows[owner, 0, layer : layer + 1, :]
            new_square_scale[layer, owner : owner + 1, :] = peak_rows[owner, 1, layer : layer + 1, :]

    for offset in range(1, col_count):
        peak_copy(offset).wait_send()

    @pl.loop(units - SEND_SLOTS, units)
    def _(unit):
        act_copy(unit, 0).wait_send()

    @pl.loop(0, items)
    def _(item):
        n_copy(item).wait_send()

    grad_copy.wait()


def apply_kernel(
    grad_hbm, weights_hbm, moments_hbm, squares_hbm, gain,
    moment_scale, square_scale, moment_peak, square_peak,
    new_weights, new_moments, new_squares, new_moment_scale, new_square_scale,
    grad, row_values, weights, moments, squares, in_sem, out_sem,
):
    layers, rows, cols = grad.shape
    blocks = rows // APPLY_ROWS
    correct_one = 1.0 - beta_one**STEP
    correct_two = 1.0 - beta_two**STEP

    def block_of(index):
        at = pl.multiple_of(index % blocks * APPLY_ROWS, APPLY_ROWS)
        return index // blocks, pl.ds(at, APPLY_ROWS)

    def arrivals(index):
        layer, span = block_of(index)
        sems = in_sem.at[index]
        pairs = ((grad_hbm, grad), (moments_hbm, moments), (squares_hbm, squares), (weights_hbm, weights))
        return [
            pltpu.make_async_copy(src.at[layer, span], dst.at[layer, span], sems.at[number])
            for number, (src, dst) in enumerate(pairs)
        ]

    def departures(index):
        layer, span = block_of(index)
        pairs = ((weights, new_weights), (moments, new_moments), (squares, new_squares))
        return [
            pltpu.make_async_copy(src.at[layer, span], dst.at[layer, span], out_sem.at[index, number])
            for number, (src, dst) in enumerate(pairs)
        ]

    @pl.loop(0, layers * blocks)
    def _(index):
        for copy in arrivals(index):
            copy.start()

    new_moment_scale[...] = moment_peak[...]
    new_square_scale[...] = square_peak[...]
    mine = pl.ds(lax.axis_index("col"), 1)
    for layer in range(layers):
        lines = (
            moment_scale[layer, mine] * beta_one,
            square_scale[layer, mine] * beta_two,
            1.0 / (moment_peak[layer, mine] + scale_eps),
            1.0 / (square_peak[layer, mine] + scale_eps),
        )
        for kind, row in enumerate(lines):
            for at in range(0, rows, LANES):
                tile = jnp.broadcast_to(row[:, at : at + LANES], (LANES, LANES))
                row_values[kind, layer, at : at + LANES] = tile.T

    moment_gain = gain[0, 0:1, 0:1]
    square_gain = gain[1, 0:1, 0:1]

    @pl.loop(0, layers * blocks)
    def _(index):
        layer, span = block_of(index)
        for copy in arrivals(index):
            copy.wait()

        @pl.loop(0, APPLY_ROWS // STRIP_ROWS)
        def _(strip):
            at = index % blocks * APPLY_ROWS + strip * STRIP_ROWS
            span = pl.ds(pl.multiple_of(at, STRIP_ROWS), STRIP_ROWS)
            for piece in range(cols // LANES):
                where = pl.ds(piece * LANES, LANES)
                value = grad[layer, span, where]
                moment = moments[layer, span, where].astype(jnp.float32) * row_values[0, layer, span]
                square = squares[layer, span, where].astype(jnp.float32) * row_values[1, layer, span]
                moment = moment + moment_gain * value
                square = square + square_gain * (value * value)
                moments[layer, span, where] = (moment * row_values[2, layer, span]).astype(jnp.bfloat16)
                squares[layer, span, where] = (square * row_values[3, layer, span]).astype(jnp.bfloat16)
                level = square * (1.0 / correct_two)
                ratio = moment * (1.0 / correct_one) * pl.reciprocal(level * lax.rsqrt(level) + adam_eps)
                old = weights[layer, span, where]
                weights[layer, span, where] = old - learn_rate * (decay_rate * old + ratio)

        for copy in departures(index):
            copy.start()

    @pl.loop(0, layers * blocks)
    def _(index):
        for copy in departures(index):
            copy.wait()


def factor_step(
    mesh_shape, activations, cotangent, master_weights, moment_codes, square_codes, moment_scales, square_scales
):
    count = mesh_shape["dp"]
    col_count = mesh_shape["col"]
    layers, tokens, cols = activations.shape
    line = count // 2
    features = cotangent.shape[2]
    rows = features // count
    half = cols // 2
    slots = line + 1
    blocks = layers * rows // APPLY_ROWS
    scale_shape = jax.ShapeDtypeStruct((layers, col_count, rows), jnp.float32)
    items = NARROW + layers * (half // LANES) - NARROW // 2
    piece = (tokens, LANES)
    f32, bf16 = jnp.float32, jnp.bfloat16
    moment_scales = moment_scales.transpose(0, 2, 1)
    square_scales = square_scales.transpose(0, 2, 1)
    dma = pltpu.SemaphoreType.DMA
    regular = pltpu.SemaphoreType.REGULAR
    vmem = pl.BlockSpec(memory_space=pltpu.VMEM)
    hbm = pl.BlockSpec(memory_space=pl.ANY)
    gradient, gain, moment_peak, square_peak = pl.pallas_call(
        functools.partial(factor_kernel, count, col_count),
        out_shape=(
            jax.ShapeDtypeStruct((layers, rows, cols), f32),
            jax.ShapeDtypeStruct((2, 8, LANES), f32),
            scale_shape,
            scale_shape,
        ),
        in_specs=[hbm, hbm, hbm, hbm, vmem, vmem],
        out_specs=(hbm, vmem, vmem, vmem),
        scratch_shapes=[
            pltpu.VMEM((layers, rows, cols), f32),
            pltpu.VMEM((2, layers, rows, LANES), f32),
            pltpu.VMEM((2, layers, rows, LANES), f32),
            pltpu.VMEM((col_count, 2, layers, rows), f32),
            pltpu.VMEM((layers, tokens, features), bf16),
            pltpu.VMEM((layers, tokens, half), bf16),
            pltpu.VMEM((NARROW,) + piece, bf16),
            pltpu.VMEM((layers, features, 2 * tokens), bf16),
            pltpu.VMEM((layers, 2 * tokens, half), bf16),
            pltpu.VMEM((SEND_SLOTS,) + piece, f32),
            pltpu.VMEM((ACT_SLOTS,) + piece, f32),
            pltpu.VMEM((line, col_count) + piece, f32),
            pltpu.VMEM((slots, line, 2 * rows, LANES), f32),
            pltpu.VMEM((slots, line + 1, 2 * rows, LANES), f32),
            pltpu.VMEM((NARROW, rows, LANES), f32),
            pltpu.VMEM((items, rows, LANES), f32),
            pltpu.VMEM((8, LANES), f32),
            pltpu.VMEM((8, LANES), f32),
            pltpu.VMEM((col_count - 1, 8, LANES), f32),
            pltpu.VMEM((count - 1, 8, LANES), f32),
            dma((NARROW + line + 3 * layers - 1,)),
            dma((layers, 2)), dma,
            dma((col_count - 1,)), dma((col_count,)),
            dma((SEND_SLOTS,)), dma((ACT_SLOTS,)), dma((line, SPLITS)),
            dma((line, col_count - 1, SPLITS)), dma((line, col_count, SPLITS)),
            dma((slots, line)), dma((slots, line)), dma((slots, line)), dma((slots, line)),
            dma((items,)), dma((items,)),
            dma((col_count - 1,)), dma((col_count - 1,)), dma((count - 1,)), dma((count - 1,)),
            regular((ACT_SLOTS,)), regular((line,)), regular, regular,
        ],
        compiler_params=pltpu.CompilerParams(
            collective_id=0, has_side_effects=True, vmem_limit_bytes=67043328
        ),
    )(
        cotangent, activations, moment_codes, square_codes,
        moment_scales, square_scales,
    )
    outs = pl.pallas_call(
        apply_kernel,
        out_shape=(
            jax.ShapeDtypeStruct(master_weights.shape, f32),
            jax.ShapeDtypeStruct(moment_codes.shape, bf16),
            jax.ShapeDtypeStruct(square_codes.shape, bf16),
            scale_shape,
            scale_shape,
        ),
        in_specs=[hbm, hbm, hbm, hbm, vmem, vmem, vmem, vmem, vmem],
        out_specs=(hbm, hbm, hbm, vmem, vmem),
        scratch_shapes=[
            pltpu.VMEM((layers, rows, cols), f32),
            pltpu.VMEM((4, layers, rows, LANES), f32),
            pltpu.VMEM((layers, rows, cols), f32),
            pltpu.VMEM((layers, rows, cols), bf16),
            pltpu.VMEM((layers, rows, cols), bf16),
            dma((blocks, 4)), dma((blocks, 3)),
        ],
        compiler_params=pltpu.CompilerParams(vmem_limit_bytes=APPLY_VMEM),
    )(
        gradient, master_weights, moment_codes, square_codes, gain,
        moment_scales, square_scales, moment_peak, square_peak,
    )
    return outs[:3] + (outs[3].transpose(0, 2, 1), outs[4].transpose(0, 2, 1))


def fits_factors(activations, cotangent, block_count, mesh_shape):
    count = mesh_shape["dp"]
    line = count // 2
    rows = cotangent.shape[2] // count
    chunks = activations.shape[2] // (2 * LANES)
    aligned = activations.shape[1] % LANES == 0 and activations.shape[2] % (2 * LANES) == 0
    layers, tokens, cols = activations.shape
    aligned = aligned and rows % LANES == 0 and cols % LANES == 0 and block_count == mesh_shape["col"]
    roomy = layers * rows <= tokens and cols <= cotangent.shape[2]
    return aligned and roomy and line >= 3 and 2 * rows == LANES * mesh_shape["col"] and mesh_shape["col"] % 2 == 0 and activations.shape[1] % (8 * SPLITS) == 0 and chunks - NARROW // 2 > line


def local(
    mesh_shape, activations, cotangent, master_weights, moment_codes, square_codes, moment_scales, square_scales
):
    layer_count = activations.shape[0]
    shard_rows = master_weights.shape[1]
    shard_cols = master_weights.shape[2]
    block_count = moment_scales.shape[2]
    if fits_factors(activations, cotangent, block_count, mesh_shape):
        return factor_step(
            mesh_shape, activations, cotangent, master_weights, moment_codes, square_codes,
            moment_scales, square_scales,
        )
    gradient, squares = reduced_gradient(activations, cotangent, mesh_shape)
    total_sq = jnp.sum(squares)
    rms = jnp.sqrt(total_sq / float(LAYERS * KV * D) + norm_eps)
    clip_factor = jnp.minimum(1.0, 1.0 / rms)
    correct_one = 1.0 - beta_one**STEP
    correct_two = 1.0 - beta_two**STEP
    own_block = lax.axis_index("col") * shard_cols // BLOCK
    selector = (jnp.arange(block_count, dtype=jnp.int32) == own_block).astype(jnp.float32)
    outs_weights, outs_mcode, outs_scode, outs_mscale, outs_sscale = ([], [], [], [], [])
    for layer_index in range(layer_count):
        moment_scale = jnp.sum(moment_scales[layer_index] * selector, axis=1)
        square_scale = jnp.sum(square_scales[layer_index] * selector, axis=1)
        old_moment = moment_codes[layer_index].astype(jnp.float32) * moment_scale[:, None]
        old_square = square_codes[layer_index].astype(jnp.float32) * square_scale[:, None]
        grad_now = clip_factor * gradient[layer_index]
        new_moment = beta_one * old_moment + (1.0 - beta_one) * grad_now
        new_square = beta_two * old_square + (1.0 - beta_two) * grad_now * grad_now
        moment_part = jnp.max(jnp.abs(new_moment), axis=1)[:, None] * selector
        square_part = jnp.max(new_square, axis=1)[:, None] * selector
        moment, square, moment_part, square_part = (
            new_moment,
            new_square,
            moment_part,
            square_part,
        )
        moment_max, square_max = lax.pmax((moment_part, square_part), "col")
        moment_div = jnp.sum(moment_max * selector, axis=1)[:, None]
        square_div = jnp.sum(square_max * selector, axis=1)[:, None]
        moment_out = (moment / (moment_div + scale_eps)).astype(jnp.bfloat16)
        square_out = (square / (square_div + scale_eps)).astype(jnp.bfloat16)
        ratio = moment / correct_one / (jnp.sqrt(square / correct_two) + adam_eps)
        weights = master_weights[layer_index]
        results = (weights - learn_rate * (decay_rate * weights + ratio), moment_out, square_out)
        outs_weights.append(results[0])
        outs_mcode.append(results[1])
        outs_scode.append(results[2])
        outs_mscale.append(moment_max)
        outs_sscale.append(square_max)
    return (
        jnp.stack(outs_weights),
        jnp.stack(outs_mcode),
        jnp.stack(outs_scode),
        jnp.stack(outs_mscale),
        jnp.stack(outs_sscale),
    )


def solution(mesh):
    in_specs = (
        P(None, "dp", "col"),
        P(None, "dp", None),
        P(None, "dp", "col"),
        P(None, "dp", "col"),
        P(None, "dp", "col"),
        P(None, "dp", None),
        P(None, "dp", None),
    )
    out_specs = (
        P(None, "dp", "col"),
        P(None, "dp", "col"),
        P(None, "dp", "col"),
        P(None, "dp", None),
        P(None, "dp", None),
    )
    return jax.shard_map(functools.partial(local, dict(mesh.shape)), mesh=mesh, in_specs=in_specs, out_specs=out_specs, check_vma=False)
```

```python
import functools

import jax
import jax.numpy as jnp
from jax import lax
from jax.experimental import pallas as pl
from jax.experimental.pallas import tpu as pltpu
from jax.sharding import PartitionSpec as P

D = 8192
KV = 2048
BLOCK = 2048
LAYERS = 2
STEP = 10


beta_one = 0.9
beta_two = 0.999
learn_rate = 0.001
decay_rate = 0.1
adam_eps = 1e-08
scale_eps = 1e-06
norm_eps = 1e-06

LANES = 128
AHEAD = 3
XSLOTS = 4


def reduce_kernel(
    count, col_count, cot_ref, act_ref, out_ref, sq_ref,
    xs, xr, part, arr, bs, br, own_sq, sum_sq, col_sq, dp_sq,
    xs_sem, xr_sem, rs_sem, rr_sem, ls_sem, ll_sem, bs_sem, br_sem,
    cs_sem, cr_sem, ds_sem, dr_sem, x_free, from_right, from_left,
):
    layers, pairs, line, rows, tokens = cot_ref.shape
    cols = act_ref.shape[2]
    slots = part.shape[0]
    wide_per = cols // (2 * LANES) - 1
    per_layer = wide_per + 2
    period = (per_layer + 1) // 2
    items = layers * per_layer
    wides = layers * wide_per
    me = lax.axis_index("dp")
    z = me // 2
    x = me % 2
    peer = 2 * z + 1 - x
    right = jnp.minimum(z + 1, line - 1) * 2 + x
    left = jnp.maximum(z - 1, 0) * 2 + x
    has_right = z < line - 1
    has_left = z > 0
    mirror = line - 1 - z

    def signal(sem, where):
        pl.semaphore_signal(
            sem, inc=1, device_id={"dp": where}, device_id_type=pl.DeviceIdType.MESH
        )

    barrier = pltpu.get_barrier_semaphore()
    mine = lax.axis_index("col")
    for offset in range(1, count):
        signal(barrier, lax.rem(me + offset, count))
    for offset in range(1, col_count):
        pl.semaphore_signal(
            barrier, inc=1, device_id={"col": lax.rem(mine + offset, col_count)},
            device_id_type=pl.DeviceIdType.MESH,
        )
    pl.semaphore_wait(barrier, count + col_count - 2)

    def remote(src, dst, send, recv, where):
        return pltpu.make_async_remote_copy(
            src_ref=src, dst_ref=dst, send_sem=send, recv_sem=recv,
            device_id={"dp": where}, device_id_type=pl.DeviceIdType.MESH,
        )

    def describe(item):
        layer = item // per_layer
        place = item % per_layer
        narrow = place % period == 0
        wide_at = place - (place + period - 1) // period
        narrow_at = place // period
        return layer, narrow, wide_at, narrow_at

    def x_copy(number):
        slot = number % XSLOTS
        return remote(xs.at[slot], xr.at[slot], xs_sem.at[slot], xr_sem.at[slot], peer)

    def r_copy(slot, target):
        return remote(
            part.at[slot, target], arr.at[slot, target + 1],
            rs_sem.at[slot, target], rr_sem.at[slot, target], right,
        )

    def l_copy(slot, target):
        return remote(
            part.at[slot, target], arr.at[slot, target],
            ls_sem.at[slot, target], ll_sem.at[slot, target], left,
        )

    def b_copy(number):
        return remote(
            bs.at[number], br.at[number], bs_sem.at[number], br_sem.at[number], peer
        )

    def product(layer, pair, target, start, width):
        return jnp.dot(
            cot_ref[layer, pair, target],
            act_ref[layer, :, pl.ds(pl.multiple_of(start, LANES), width)],
            preferred_element_type=jnp.float32,
        )

    def send_wide(item):
        layer, narrow, wide_at, _ = describe(item)

        @pl.when(jnp.logical_not(narrow))
        def _():
            number = layer * wide_per + wide_at
            slot = number % XSLOTS

            @pl.loop(0, line)
            def _(target):
                value = product(layer, 1 - x, target, wide_at * 2 * LANES, 2 * LANES)
                xs[slot, target, 0] = value[:, :LANES]
                xs[slot, target, 1] = value[:, LANES:]

            @pl.when(number >= XSLOTS)
            def _():
                pl.semaphore_wait(x_free, 1)

            x_copy(number).start()

    def form(item):
        layer, narrow, wide_at, narrow_at = describe(item)
        here = item % slots

        @pl.when(item >= slots)
        def _():
            @pl.when(has_right)
            def _():
                pl.semaphore_wait(from_right, 1)

            @pl.when(has_left)
            def _():
                pl.semaphore_wait(from_left, 1)

        @pl.when(narrow)
        def _():
            start = wide_per * 2 * LANES + narrow_at * LANES

            @pl.loop(0, line)
            def _(target):
                part[here, target, 0] = product(layer, 0, target, start, LANES)
                part[here, target, 1] = product(layer, 1, target, start, LANES)

        @pl.when(jnp.logical_not(narrow))
        def _():
            number = layer * wide_per + wide_at
            slot = number % XSLOTS
            x_copy(number).wait()

            @pl.loop(0, line)
            def _(target):
                value = product(layer, x, target, wide_at * 2 * LANES, 2 * LANES)
                part[here, target, 0] = value[:, :LANES] + xr[slot, target, 0]
                part[here, target, 1] = value[:, LANES:] + xr[slot, target, 1]

            @pl.when(number + XSLOTS < wides)
            def _():
                signal(x_free, peer)

    def hop(item, stage):
        here = item % slots

        @pl.when(z <= stage)
        def _():
            target = line - 1 - stage + z
            if stage > 0:
                @pl.when(has_left)
                def _():
                    r_copy(here, target).wait_recv()
                    part[here, target] += arr[here, target + 1]

            r_copy(here, target).start()

        @pl.when(mirror <= stage)
        def _():
            target = stage - mirror
            if stage > 0:
                @pl.when(has_right)
                def _():
                    l_copy(here, target).wait_recv()
                    part[here, target] += arr[here, target]

            l_copy(here, target).start()

    def finish(item):
        layer, narrow, wide_at, narrow_at = describe(item)
        here = item % slots

        @pl.when(has_left)
        def _():
            r_copy(here, z).wait_recv()
            part[here, z] += arr[here, z + 1]

        @pl.when(has_right)
        def _():
            l_copy(here, z).wait_recv()
            part[here, z] += arr[here, z]

        for target in range(line):
            @pl.when(target > z)
            def _(target=target):
                r_copy(here, target).wait_send()

            @pl.when(target < z)
            def _(target=target):
                l_copy(here, target).wait_send()

        @pl.when(narrow)
        def _():
            number = layer * 2 + narrow_at
            start = wide_per * 2 * LANES + narrow_at * LANES
            bs[number] = part[here, z, 1 - x]
            b_copy(number).start()
            out_ref[layer, :, pl.ds(pl.multiple_of(start, LANES), LANES)] = part[here, z, x]

        @pl.when(jnp.logical_not(narrow))
        def _():
            for half in range(2):
                start = wide_at * 2 * LANES + half * LANES
                out_ref[layer, :, pl.ds(pl.multiple_of(start, LANES), LANES)] = part[here, z, half]

        @pl.when(item + slots < items)
        def _():
            @pl.when(has_left)
            def _():
                signal(from_right, left)

            @pl.when(has_right)
            def _():
                signal(from_left, right)

    for item in range(1, AHEAD):
        send_wide(jnp.int32(item))

    @pl.loop(0, items + line - 1)
    def _(step):
        def guard(item, action):
            pl.when(jnp.logical_and(item >= 0, item < items))(lambda: action(item))

        guard(step + AHEAD, send_wide)
        guard(step - (line - 1), finish)
        for stage in reversed(range(1, line - 1)):
            guard(step - stage, functools.partial(hop, stage=stage))

        def begin(item):
            form(item)
            hop(item, 0)

        guard(step, begin)

    for number in range(2 * layers):
        b_copy(number).wait()
        start = wide_per * 2 * LANES + (number % 2) * LANES
        out_ref[number // 2, :, start : start + LANES] += br[number]

    def square_rows(index, total):
        layer = index // (rows // 8)
        at = pl.multiple_of(index % (rows // 8) * 8, 8)
        for piece in range(cols // LANES):
            value = out_ref[layer, pl.ds(at, 8), piece * LANES : (piece + 1) * LANES]
            total = total + value * value
        return total

    def spread(src, landing, send, recv, axis, index, size):
        copies = []
        for offset in range(1, size):
            copies.append(
                pltpu.make_async_remote_copy(
                    src_ref=src, dst_ref=landing.at[offset - 1],
                    send_sem=send.at[offset - 1], recv_sem=recv.at[offset - 1],
                    device_id={axis: lax.rem(index + offset, size)},
                    device_id_type=pl.DeviceIdType.MESH,
                )
            )
        for copy in copies:
            copy.start()
        for copy in copies:
            copy.wait()
        total = src[...]
        for offset in range(1, size):
            total = total + landing[offset - 1]
        return total

    own_sq[...] = lax.fori_loop(
        0, layers * rows // 8, square_rows, jnp.zeros((8, LANES), jnp.float32)
    )
    sum_sq[...] = spread(own_sq, col_sq, cs_sem, cr_sem, "col", mine, col_count)
    sq_ref[...] = spread(sum_sq, dp_sq, ds_sem, dr_sem, "dp", me, count)


def reduced_gradient(activations, cotangent, mesh_shape):
    count = mesh_shape["dp"]
    col_count = mesh_shape["col"]
    layers, tokens, cols = activations.shape
    line = count // 2
    rows = cotangent.shape[2] // count
    slots = line + 2
    cot = cotangent.reshape(layers, tokens, line, 2, rows).transpose(0, 3, 2, 4, 1)
    block = (line, 2, rows, LANES)
    dma = pltpu.SemaphoreType.DMA
    vmem = pl.BlockSpec(memory_space=pltpu.VMEM)
    return pl.pallas_call(
        functools.partial(reduce_kernel, count, col_count),
        out_shape=(
            jax.ShapeDtypeStruct((layers, rows, cols), jnp.float32),
            jax.ShapeDtypeStruct((8, LANES), jnp.float32),
        ),
        in_specs=[vmem, vmem],
        out_specs=(vmem, vmem),
        scratch_shapes=[
            pltpu.VMEM((XSLOTS,) + block, jnp.float32),
            pltpu.VMEM((XSLOTS,) + block, jnp.float32),
            pltpu.VMEM((slots,) + block, jnp.float32),
            pltpu.VMEM((slots, line + 1) + block[1:], jnp.float32),
            pltpu.VMEM((2 * layers, rows, LANES), jnp.float32),
            pltpu.VMEM((2 * layers, rows, LANES), jnp.float32),
            pltpu.VMEM((8, LANES), jnp.float32),
            pltpu.VMEM((8, LANES), jnp.float32),
            pltpu.VMEM((col_count - 1, 8, LANES), jnp.float32),
            pltpu.VMEM((count - 1, 8, LANES), jnp.float32),
            dma((XSLOTS,)), dma((XSLOTS,)),
            dma((slots, line)), dma((slots, line)), dma((slots, line)), dma((slots, line)),
            dma((2 * layers,)), dma((2 * layers,)),
            dma((col_count - 1,)), dma((col_count - 1,)), dma((count - 1,)), dma((count - 1,)),
            pltpu.SemaphoreType.REGULAR, pltpu.SemaphoreType.REGULAR, pltpu.SemaphoreType.REGULAR,
        ],
        compiler_params=pltpu.CompilerParams(
            collective_id=0, has_side_effects=True, vmem_limit_bytes=62 * 2**20
        ),
    )(cot, activations)


AHEAD_UNITS = 5
SEND_SLOTS = 6
ACT_SLOTS = 5
NARROW = 2
RELEASE = 3
SPLITS = 2
PEAK_ROWS = 32
APPLY_ROWS = 64
STRIP_ROWS = 32
APPLY_VMEM = 62 * 2**20


def factor_kernel(
    count, col_count, cot_hbm, act_hbm, moments_hbm, squares_hbm, moment_scale, square_scale,
    grad_out, gain_out, new_moment_scale, new_square_scale, grad,
    scales, row_values, peak, peak_rows,
    cot_raw, act_raw, narrow_act, cot_t, act_cat, xs, xr, crx, part, arr, narrow_in, held,
    own_sq, sum_sq, col_sq, dp_sq,
    ld_sem, c_in, g_out, ms_sem, mr_sem, xs_sem, xr_sem, pr_sem, cs_sem, cr_sem, rs_sem, rr_sem, ls_sem, ll_sem, fs_sem, fr_sem,
    qs_sem, qr_sem, ds_sem, dr_sem, act_free, cot_free, from_right, from_left,
):
    layers, tokens, cols = act_hbm.shape
    half = cols // 2
    line = count // 2
    pair_rows = part.shape[2]
    rows = pair_rows // 2
    slots = part.shape[0]
    chunks = half // LANES
    first_chunks = chunks - NARROW // 2
    wides = first_chunks + (layers - 1) * chunks
    items = NARROW + wides
    first_units = first_chunks + line
    layer_units = chunks + line
    units = first_units + (layers - 1) * layer_units
    all_sent = items - chunks + line - 2
    groups = col_count // 2
    pieces = cols // LANES
    features = cot_hbm.shape[2]
    me = lax.axis_index("dp")
    mine = lax.axis_index("col")
    z = me // 2
    x = me % 2
    peer = 2 * z + 1 - x
    partner = mine + 1 - 2 * (mine % 2)
    right = jnp.minimum(z + 1, line - 1) * 2 + x
    left = jnp.maximum(z - 1, 0) * 2 + x
    has_right = z < line - 1
    has_left = z > 0
    mirror = line - 1 - z
    own_half = pl.multiple_of(x * half, LANES)
    peer_half = pl.multiple_of((1 - x) * half, LANES)

    def lanes(start, width=LANES):
        return pl.ds(pl.multiple_of(start, LANES), width)

    def signal(sem, where):
        pl.semaphore_signal(
            sem, inc=1, device_id={"dp": where}, device_id_type=pl.DeviceIdType.MESH
        )

    loads = []

    def load(src, dst):
        copy = pltpu.make_async_copy(src, dst, ld_sem.at[len(loads)])
        copy.start()
        loads.append(copy)

    def block_target(place):
        after = line - 1 - z
        rising = jnp.where(place < after, line - 1 - place, place - after)
        falling = jnp.where(place < z, place, line - 1 - (place - z))
        other = jnp.where(z < line // 2, rising, falling)
        return jnp.where(place < line - 1, other, z)

    for place in range(line):
        block = lanes(block_target(place) * pair_rows, pair_rows)
        load(cot_hbm.at[0, :, block], cot_raw.at[0, :, block])
    load(act_hbm.at[0, :, pl.ds(peer_half, half)], act_raw.at[0])
    for index in range(NARROW):
        start = (index % 2) * half + (chunks - 1 - index // 2) * LANES
        load(act_hbm.at[0, :, lanes(start)], narrow_act.at[index])
    for layer in range(layers):
        if layer > 0:
            load(cot_hbm.at[layer], cot_raw.at[layer])
            load(act_hbm.at[layer, :, pl.ds(peer_half, half)], act_raw.at[layer])
        load(act_hbm.at[layer, :, pl.ds(own_half, half)], act_cat.at[layer, pl.ds(0, tokens)])
    load(moment_scale, scales.at[0])
    load(square_scale, scales.at[1])

    early_loads = line + 1 + NARROW

    barrier = pltpu.get_barrier_semaphore()
    signal(barrier, peer)

    @pl.when(has_right)
    def _():
        signal(barrier, right)

    @pl.when(has_left)
    def _():
        signal(barrier, left)

    for offset in range(1, col_count):
        pl.semaphore_signal(
            barrier, inc=1, device_id={"col": lax.rem(mine + offset, col_count)},
            device_id_type=pl.DeviceIdType.MESH,
        )
    sides = has_right.astype(jnp.int32) + has_left.astype(jnp.int32)
    pl.semaphore_wait(barrier, col_count + sides)

    def remote(src, dst, send, recv, where):
        return pltpu.make_async_remote_copy(
            src_ref=src, dst_ref=dst, send_sem=send, recv_sem=recv,
            device_id={"dp": where}, device_id_type=pl.DeviceIdType.MESH,
        )

    def describe(item):
        number = item - NARROW
        narrow = item < NARROW
        later = jnp.maximum(number - first_chunks, 0)
        layer = jnp.where(number < first_chunks, 0, 1 + later // chunks)
        chunk = jnp.where(number < first_chunks, number, later % chunks)
        return layer, narrow, chunk

    def unit_base(layer):
        return jnp.where(layer == 0, 0, first_units + (layer - 1) * layer_units)

    def act_number(layer, chunk):
        return jnp.where(layer == 0, chunk, first_chunks + (layer - 1) * chunks + chunk)

    def act_copy(unit, number):
        here = unit % SEND_SLOTS
        slot = number % ACT_SLOTS
        return remote(xs.at[here], xr.at[slot], xs_sem.at[here], xr_sem.at[slot], peer)

    def cot_copy(unit, place, split):
        here = unit % SEND_SLOTS
        span = pl.ds(split * (tokens // SPLITS), tokens // SPLITS)
        return remote(
            xs.at[here, span], crx.at[place, mine, span], xs_sem.at[here], pr_sem.at[place, split], peer
        )

    def col_copy(place, owner, number, where, split):
        piece = crx.at[place, owner, pl.ds(split * (tokens // SPLITS), tokens // SPLITS)]
        return pltpu.make_async_remote_copy(
            src_ref=piece, dst_ref=piece,
            send_sem=cs_sem.at[place, number, split], recv_sem=cr_sem.at[place, owner, split],
            device_id={"col": where}, device_id_type=pl.DeviceIdType.MESH,
        )

    def far(index):
        return lax.rem(mine + 2 * index, col_count)

    def r_copy(slot, target):
        return remote(
            part.at[slot, target], arr.at[slot, target + 1],
            rs_sem.at[slot, target], rr_sem.at[slot, target], right,
        )

    def l_copy(slot, target):
        return remote(
            part.at[slot, target], arr.at[slot, target],
            ls_sem.at[slot, target], ll_sem.at[slot, target], left,
        )

    def n_copy(item):
        where = narrow_in.at[jnp.minimum(item, NARROW - 1)]
        return remote(held.at[item], where, fs_sem.at[item], fr_sem.at[item], peer)

    def f_copy(item, side):
        layer, narrow, chunk = describe(item)
        where = grad.at[layer, :, lanes(side * half + chunk * LANES)]
        return remote(held.at[item], where, fs_sem.at[item], fr_sem.at[item], peer)

    def exchange(item):
        @pl.when(item < NARROW)
        def _():
            n_copy(item).start()

        @pl.when(item >= NARROW)
        def _():
            f_copy(item, x).start()

    def exchanged(step):
        done = jnp.minimum(step - (line - 1), RELEASE * (step - 1 - all_sent))
        return jnp.clip(done, 0, items)

    def send(unit):
        @pl.when(unit < units)
        def _():
            layer = jnp.where(unit < first_units, 0, 1 + (unit - first_units) // layer_units)
            index = unit - unit_base(layer)
            mixed = index < 2 * line - 1
            is_cot = jnp.logical_and(mixed, index % 2 == 0)
            here = unit % SEND_SLOTS

            @pl.when(unit >= SEND_SLOTS)
            def _():
                act_copy(unit, 0).wait_send()

            @pl.when(is_cot)
            def _():
                place = index // 2
                start = block_target(place) * pair_rows + mine * LANES
                xs[here] = cot_raw[layer, :, lanes(start)].astype(jnp.float32)

                @pl.when(layer > 0)
                def _():
                    pl.semaphore_wait(cot_free.at[place], 1)

                for split in range(SPLITS):
                    cot_copy(unit, place, split).start()

            @pl.when(jnp.logical_not(is_cot))
            def _():
                chunk = jnp.where(mixed, index // 2, index - line)
                number = act_number(layer, chunk)
                xs[here] = act_raw[layer, :, lanes(chunk * LANES)].astype(jnp.float32)

                @pl.when(number >= ACT_SLOTS)
                def _():
                    pl.semaphore_wait(act_free.at[number % ACT_SLOTS], 1)

                act_copy(unit, number).start()

    def forward(layer, place):
        for split in range(SPLITS):
            cot_copy(0, place, split).wait_recv()
            for index in range(1, groups):
                col_copy(place, mine, index, far(index), split).start()
            col_copy(place, mine, 0, partner, split).start()
        send(unit_base(layer) + 2 * place + AHEAD_UNITS)

    def relay(place):
        for split in range(SPLITS):
            for index in range(1, groups):
                col_copy(place, far(index), groups - 1 + index, partner, split).wait_recv()
                col_copy(place, far(index), groups - 1 + index, partner, split).start()

    def prepare(layer, place):
        base = block_target(place) * pair_rows

        @pl.loop(0, col_count)
        def _(member):
            start = base + member * LANES
            value = cot_raw[layer, :, lanes(start)].astype(jnp.float32)
            cot_t[layer, lanes(start), pl.ds(0, tokens)] = value.T.astype(jnp.bfloat16)

    def absorb(layer, place):
        @pl.when(layer > 0)
        def _():
            prepare(layer, place)

        base = block_target(place) * pair_rows
        for split in range(SPLITS):
            col_copy(place, partner, 0, partner, split).wait_recv()
            for index in range(1, groups):
                col_copy(place, lax.rem(partner + 2 * index, col_count), 0, partner, split).wait_recv()

        @pl.loop(0, col_count)
        def _(owner):
            source = crx[place, owner]
            cot_t[layer, lanes(base + owner * LANES), pl.ds(tokens, tokens)] = source.T.astype(jnp.bfloat16)

        for number in range(col_count - 1):
            for split in range(SPLITS):
                col_copy(place, mine, number, partner, split).wait_send()

        @pl.when(layer < layers - 1)
        def _():
            signal(cot_free.at[place], peer)

    def take(layer, chunk):
        number = act_number(layer, chunk)
        slot = number % ACT_SLOTS
        act_copy(0, number).wait_recv()
        act_cat[layer, pl.ds(tokens, tokens), lanes(chunk * LANES)] = xr[slot].astype(jnp.bfloat16)

        @pl.when(number + ACT_SLOTS < wides)
        def _():
            signal(act_free.at[slot], peer)

        index = jnp.where(chunk < line - 1, 2 * chunk + 1, chunk + line)
        send(unit_base(layer) + index + AHEAD_UNITS)

    def form(item, target):
        layer, narrow, chunk = describe(item)
        here = item % slots
        at = pl.ds(pl.multiple_of(target * pair_rows, LANES), pair_rows)

        @pl.when(narrow)
        def _():
            part[here, target] = jnp.dot(
                cot_t[0, at, pl.ds(0, tokens)], narrow_act[jnp.minimum(item, NARROW - 1)],
                preferred_element_type=jnp.float32,
            )

        @pl.when(jnp.logical_not(narrow))
        def _():
            part[here, target] = jnp.dot(
                cot_t[layer, at, :], act_cat[layer, :, lanes(chunk * LANES)],
                preferred_element_type=jnp.float32,
            )

    def opens(item):
        layer, narrow, chunk = describe(item)
        return layer, jnp.logical_and(jnp.logical_not(narrow), chunk == 0)

    def ready(item, place):
        @pl.when(item == 0)
        def _():
            prepare(0, place)

        layer, first = opens(item)

        @pl.when(first)
        def _():
            if place == 0:
                @pl.when(layer == 0)
                def _():
                    forward(layer, 0)

            relay(place)
            absorb(layer, place)

    def hop(item, stage):
        here = item % slots

        @pl.when(z <= stage)
        def _():
            target = line - 1 - stage + z
            form(item, target)
            if stage > 0:
                @pl.when(has_left)
                def _():
                    r_copy(here, target).wait_recv()
                    part[here, target] += arr[here, target + 1]

            r_copy(here, target).start()

        @pl.when(mirror <= stage)
        def _():
            target = stage - mirror
            form(item, target)
            if stage > 0:
                @pl.when(has_right)
                def _():
                    l_copy(here, target).wait_recv()
                    part[here, target] += arr[here, target]

            l_copy(here, target).start()

    def code_in(layer, kind):
        source = (moments_hbm, squares_hbm)[kind].at[layer]
        return pltpu.make_async_copy(
            source, cot_raw.at[layer, pl.ds(kind * rows, rows), pl.ds(0, cols)], c_in.at[layer, kind]
        )

    def spread_scales():
        for layer in range(layers):
            for kind in range(2):
                factor = (beta_one, beta_two)[kind]
                row = scales[kind, layer, pl.ds(mine, 1), :] * factor
                for part_at in range(0, rows, LANES):
                    tile = jnp.broadcast_to(row[:, part_at : part_at + LANES], (LANES, LANES))
                    row_values[kind, layer, part_at : part_at + LANES] = tile.T

    def begin(item):
        layer, narrow, chunk = describe(item)
        ready(item, 0)

        @pl.when(jnp.logical_not(narrow))
        def _():
            take(layer, chunk)

        @pl.when(item >= slots)
        def _():
            @pl.when(has_right)
            def _():
                pl.semaphore_wait(from_right, 1)

            @pl.when(has_left)
            def _():
                pl.semaphore_wait(from_left, 1)

        hop(item, 0)

        @pl.when(item == 1)
        def _():
            for copy in loads[early_loads:]:
                copy.wait()

        @pl.when(item == items - 2)
        def _():
            spread_scales()
            for index in range(layers):
                for kind in range(2):
                    code_in(index, kind).start()

        @pl.when(jnp.logical_and(jnp.logical_not(narrow), chunk < line - 1))
        def _():
            forward(layer, chunk + 1)

        next_layer, next_first = opens(item + 1)

        @pl.when(jnp.logical_and(next_first, jnp.logical_and(next_layer > 0, item + 1 < items)))
        def _():
            forward(next_layer, 0)

    def middle(item, stage):
        ready(item, stage)
        hop(item, stage)

    def add_squares(value):
        rows8 = value.reshape(value.shape[0] // 8, 8, LANES)
        own_sq[...] += jnp.sum(rows8 * rows8, axis=0)

    def join_narrow():
        for item in range(NARROW):
            n_copy(item).wait_recv()
            where = lanes((item % 2) * half + (chunks - 1 - item // 2) * LANES)
            value = grad[0, :, where] + narrow_in[item]
            grad[0, :, where] = value
            add_squares(value)

    def finish(item):
        layer, narrow, chunk = describe(item)
        here = item % slots
        ready(item, line - 1)

        @pl.when(item == items - 2)
        def _():
            join_narrow()

        form(item, z)

        @pl.when(has_left)
        def _():
            r_copy(here, z).wait_recv()
            part[here, z] += arr[here, z + 1]

        @pl.when(has_right)
        def _():
            l_copy(here, z).wait_recv()
            part[here, z] += arr[here, z]

        for target in range(line):
            @pl.when(target > z)
            def _(target=target):
                r_copy(here, target).wait_send()

            @pl.when(target < z)
            def _(target=target):
                l_copy(here, target).wait_send()

        kept = pl.ds(pl.multiple_of(x * rows, 8), rows)
        held[item] = part[here, z, pl.ds(pl.multiple_of((1 - x) * rows, 8), rows)]

        @pl.when(narrow)
        def _():
            start = (item % 2) * half + (chunks - 1 - item // 2) * LANES
            grad[0, :, lanes(start)] = part[here, z, kept]

        @pl.when(jnp.logical_not(narrow))
        def _():
            grad[layer, :, lanes(own_half + chunk * LANES)] = part[here, z, kept]
            add_squares(part[here, z])

        @pl.when(item + slots < items)
        def _():
            @pl.when(has_left)
            def _():
                signal(from_right, left)

            @pl.when(has_right)
            def _():
                signal(from_left, right)

    own_sq[...] = jnp.zeros_like(own_sq)
    loads[0].wait()
    send(jnp.int32(0))
    for copy in loads[1:early_loads]:
        copy.wait()
    for unit in range(1, AHEAD_UNITS):
        send(jnp.int32(unit))

    @pl.loop(0, items + line)
    def _(step):
        def guard(turn, action):
            item = turn - (turn > NARROW).astype(jnp.int32)
            real = jnp.logical_and(turn >= 0, turn != NARROW)
            pl.when(jnp.logical_and(real, item < items))(lambda: action(item))

        for stage in range(1, line - 1):
            guard(step - stage, functools.partial(middle, stage=stage))
        guard(step, begin)
        guard(step - (line - 1), finish)

        @pl.loop(exchanged(step - 1), exchanged(step))
        def _(item):
            exchange(item)

    def spread(src, landing, send_sems, recv_sems, axis, index, size):
        copies = []
        for offset in range(1, size):
            copies.append(
                pltpu.make_async_remote_copy(
                    src_ref=src, dst_ref=landing.at[offset - 1],
                    send_sem=send_sems.at[offset - 1], recv_sem=recv_sems.at[offset - 1],
                    device_id={axis: lax.rem(index + offset, size)},
                    device_id_type=pl.DeviceIdType.MESH,
                )
            )
        for copy in copies:
            copy.start()
        for copy in copies:
            copy.wait()
        total = src[...]
        for offset in range(1, size):
            total = total + landing[offset - 1]
        return total

    sum_sq[...] = spread(own_sq, col_sq, qs_sem, qr_sem, "col", mine, col_count)
    total = spread(sum_sq, dp_sq, ds_sem, dr_sem, "dp", me, count)
    total = jnp.sum(jnp.sum(total, axis=0, keepdims=True), axis=1, keepdims=True)
    rms = jnp.sqrt(total / float(layers * features * cols * col_count) + norm_eps)
    clip = jnp.minimum(1.0, 1.0 / rms)
    moment_gain = clip * (1.0 - beta_one)
    square_gain = clip * clip * (1.0 - beta_two)
    gain_out[0] = jnp.broadcast_to(moment_gain, (8, LANES))
    gain_out[1] = jnp.broadcast_to(square_gain, (8, LANES))

    for index in range(layers):
        for kind in range(2):
            code_in(index, kind).wait()

    @pl.loop(NARROW, items)
    def _(item):
        f_copy(item, 1 - x).wait_recv()

    grad_copy = pltpu.make_async_copy(grad, grad_out, g_out)
    grad_copy.start()

    def moments_of(layer, at, height, piece):
        where = lanes(piece * LANES)
        value = grad[layer, pl.ds(at, height), where]
        moment = cot_raw[layer, pl.ds(at, height), where].astype(jnp.float32)
        square = cot_raw[layer, pl.ds(pl.multiple_of(rows + at, 16), height), where].astype(jnp.float32)
        moment = moment * row_values[0, layer, pl.ds(at, height)] + moment_gain * value
        square = square * row_values[1, layer, pl.ds(at, height)] + square_gain * (value * value)
        return moment, square

    @pl.loop(0, layers * (rows // PEAK_ROWS))
    def _(index):
        layer = index // (rows // PEAK_ROWS)
        at = pl.multiple_of(index % (rows // PEAK_ROWS) * PEAK_ROWS, PEAK_ROWS)
        high_moment = jnp.zeros((PEAK_ROWS, LANES), jnp.float32)
        high_square = jnp.zeros((PEAK_ROWS, LANES), jnp.float32)
        for piece in range(pieces):
            moment, square = moments_of(layer, at, PEAK_ROWS, piece)
            high_moment = jnp.maximum(high_moment, jnp.abs(moment))
            high_square = jnp.maximum(high_square, square)
        peak[0, layer, pl.ds(at, PEAK_ROWS)] = high_moment
        peak[1, layer, pl.ds(at, PEAK_ROWS)] = high_square

    for layer in range(layers):
        for kind in range(2):
            for at in range(0, rows, LANES):
                tile = peak[kind, layer, at : at + LANES].T
                row = jnp.max(tile, axis=0, keepdims=True)
                peak_rows[mine, kind, layer : layer + 1, at : at + LANES] = row

    def peak_copy(offset):
        return pltpu.make_async_remote_copy(
            src_ref=peak_rows.at[mine], dst_ref=peak_rows.at[mine],
            send_sem=ms_sem.at[offset - 1], recv_sem=mr_sem.at[mine],
            device_id={"col": lax.rem(mine + offset, col_count)},
            device_id_type=pl.DeviceIdType.MESH,
        )

    def peak_arrival(owner):
        return pltpu.make_async_remote_copy(
            src_ref=peak_rows.at[owner], dst_ref=peak_rows.at[owner],
            send_sem=ms_sem.at[0], recv_sem=mr_sem.at[owner],
            device_id={"col": partner}, device_id_type=pl.DeviceIdType.MESH,
        )

    for offset in range(1, col_count):
        peak_copy(offset).start()

    for offset in range(1, col_count):
        peak_arrival(lax.rem(mine + offset, col_count)).wait_recv()
    for owner in range(col_count):
        for layer in range(layers):
            new_moment_scale[layer, owner : owner + 1, :] = peak_rows[owner, 0, layer : layer + 1, :]
            new_square_scale[layer, owner : owner + 1, :] = peak_rows[owner, 1, layer : layer + 1, :]

    for offset in range(1, col_count):
        peak_copy(offset).wait_send()

    @pl.loop(units - SEND_SLOTS, units)
    def _(unit):
        act_copy(unit, 0).wait_send()

    @pl.loop(0, items)
    def _(item):
        n_copy(item).wait_send()

    grad_copy.wait()


def apply_kernel(
    grad_hbm, weights_hbm, moments_hbm, squares_hbm, gain_hbm,
    moment_scale_hbm, square_scale_hbm, moment_peak_hbm, square_peak_hbm,
    new_weights, new_moments, new_squares, new_moment_scale, new_square_scale,
    gain, moment_scale, square_scale, moment_peak, square_peak,
    grad, row_values, weights, moments, squares, in_sem, out_sem, small_in, small_out,
):
    layers, rows, cols = grad.shape
    blocks = rows // APPLY_ROWS
    correct_one = 1.0 - beta_one**STEP
    correct_two = 1.0 - beta_two**STEP

    def block_of(index):
        at = pl.multiple_of(index % blocks * APPLY_ROWS, APPLY_ROWS)
        return index // blocks, pl.ds(at, APPLY_ROWS)

    def arrivals(index):
        layer, span = block_of(index)
        sems = in_sem.at[index]
        pairs = ((grad_hbm, grad), (moments_hbm, moments), (squares_hbm, squares), (weights_hbm, weights))
        return [
            pltpu.make_async_copy(src.at[layer, span], dst.at[layer, span], sems.at[number])
            for number, (src, dst) in enumerate(pairs)
        ]

    def departures(index):
        layer, span = block_of(index)
        pairs = ((weights, new_weights), (moments, new_moments), (squares, new_squares))
        return [
            pltpu.make_async_copy(src.at[layer, span], dst.at[layer, span], out_sem.at[index, number])
            for number, (src, dst) in enumerate(pairs)
        ]

    small = [
        pltpu.make_async_copy(src, dst, small_in.at[number])
        for number, (src, dst) in enumerate((
            (gain_hbm, gain), (moment_scale_hbm, moment_scale), (square_scale_hbm, square_scale),
            (moment_peak_hbm, moment_peak), (square_peak_hbm, square_peak),
        ))
    ]
    results = [
        pltpu.make_async_copy(moment_peak, new_moment_scale, small_out.at[0]),
        pltpu.make_async_copy(square_peak, new_square_scale, small_out.at[1]),
    ]
    for copy in small:
        copy.start()

    @pl.loop(0, layers * blocks)
    def _(index):
        for copy in arrivals(index):
            copy.start()

    for copy in small:
        copy.wait()
    for copy in results:
        copy.start()
    mine = pl.ds(lax.axis_index("col"), 1)
    for layer in range(layers):
        lines = (
            moment_scale[layer, mine] * beta_one,
            square_scale[layer, mine] * beta_two,
            1.0 / (moment_peak[layer, mine] + scale_eps),
            1.0 / (square_peak[layer, mine] + scale_eps),
        )
        for kind, row in enumerate(lines):
            for at in range(0, rows, LANES):
                tile = jnp.broadcast_to(row[:, at : at + LANES], (LANES, LANES))
                row_values[kind, layer, at : at + LANES] = tile.T

    moment_gain = gain[0, 0:1, 0:1]
    square_gain = gain[1, 0:1, 0:1]

    @pl.loop(0, layers * blocks)
    def _(index):
        layer, span = block_of(index)
        for copy in arrivals(index):
            copy.wait()

        @pl.loop(0, APPLY_ROWS // STRIP_ROWS)
        def _(strip):
            at = index % blocks * APPLY_ROWS + strip * STRIP_ROWS
            span = pl.ds(pl.multiple_of(at, STRIP_ROWS), STRIP_ROWS)
            for piece in range(cols // LANES):
                where = pl.ds(piece * LANES, LANES)
                value = grad[layer, span, where]
                moment = moments[layer, span, where].astype(jnp.float32) * row_values[0, layer, span]
                square = squares[layer, span, where].astype(jnp.float32) * row_values[1, layer, span]
                moment = moment + moment_gain * value
                square = square + square_gain * (value * value)
                moments[layer, span, where] = (moment * row_values[2, layer, span]).astype(jnp.bfloat16)
                squares[layer, span, where] = (square * row_values[3, layer, span]).astype(jnp.bfloat16)
                level = square * (1.0 / correct_two)
                ratio = moment * (1.0 / correct_one) * pl.reciprocal(level * lax.rsqrt(level) + adam_eps)
                old = weights[layer, span, where]
                weights[layer, span, where] = old - learn_rate * (decay_rate * old + ratio)

        for copy in departures(index):
            copy.start()

    @pl.loop(0, layers * blocks)
    def _(index):
        for copy in departures(index):
            copy.wait()

    for copy in results:
        copy.wait()


def factor_step(
    mesh_shape, activations, cotangent, master_weights, moment_codes, square_codes, moment_scales, square_scales
):
    count = mesh_shape["dp"]
    col_count = mesh_shape["col"]
    layers, tokens, cols = activations.shape
    line = count // 2
    features = cotangent.shape[2]
    rows = features // count
    half = cols // 2
    slots = line + 1
    blocks = layers * rows // APPLY_ROWS
    scale_shape = jax.ShapeDtypeStruct((layers, col_count, rows), jnp.float32)
    items = NARROW + layers * (half // LANES) - NARROW // 2
    piece = (tokens, LANES)
    f32, bf16 = jnp.float32, jnp.bfloat16
    moment_scales = moment_scales.transpose(0, 2, 1)
    square_scales = square_scales.transpose(0, 2, 1)
    dma = pltpu.SemaphoreType.DMA
    regular = pltpu.SemaphoreType.REGULAR
    vmem = pl.BlockSpec(memory_space=pltpu.VMEM)
    hbm = pl.BlockSpec(memory_space=pl.ANY)
    gradient, gain, moment_peak, square_peak = pl.pallas_call(
        functools.partial(factor_kernel, count, col_count),
        out_shape=(
            jax.ShapeDtypeStruct((layers, rows, cols), f32),
            jax.ShapeDtypeStruct((2, 8, LANES), f32),
            scale_shape,
            scale_shape,
        ),
        in_specs=[hbm] * 6,
        out_specs=(hbm, vmem, vmem, vmem),
        scratch_shapes=[
            pltpu.VMEM((layers, rows, cols), f32),
            pltpu.VMEM((2, layers, col_count, rows), f32),
            pltpu.VMEM((2, layers, rows, LANES), f32),
            pltpu.VMEM((2, layers, rows, LANES), f32),
            pltpu.VMEM((col_count, 2, layers, rows), f32),
            pltpu.VMEM((layers, tokens, features), bf16),
            pltpu.VMEM((layers, tokens, half), bf16),
            pltpu.VMEM((NARROW,) + piece, bf16),
            pltpu.VMEM((layers, features, 2 * tokens), bf16),
            pltpu.VMEM((layers, 2 * tokens, half), bf16),
            pltpu.VMEM((SEND_SLOTS,) + piece, f32),
            pltpu.VMEM((ACT_SLOTS,) + piece, f32),
            pltpu.VMEM((line, col_count) + piece, f32),
            pltpu.VMEM((slots, line, 2 * rows, LANES), f32),
            pltpu.VMEM((slots, line + 1, 2 * rows, LANES), f32),
            pltpu.VMEM((NARROW, rows, LANES), f32),
            pltpu.VMEM((items, rows, LANES), f32),
            pltpu.VMEM((8, LANES), f32),
            pltpu.VMEM((8, LANES), f32),
            pltpu.VMEM((col_count - 1, 8, LANES), f32),
            pltpu.VMEM((count - 1, 8, LANES), f32),
            dma((NARROW + line + 3 * layers + 1,)),
            dma((layers, 2)), dma,
            dma((col_count - 1,)), dma((col_count,)),
            dma((SEND_SLOTS,)), dma((ACT_SLOTS,)), dma((line, SPLITS)),
            dma((line, col_count - 1, SPLITS)), dma((line, col_count, SPLITS)),
            dma((slots, line)), dma((slots, line)), dma((slots, line)), dma((slots, line)),
            dma((items,)), dma((items,)),
            dma((col_count - 1,)), dma((col_count - 1,)), dma((count - 1,)), dma((count - 1,)),
            regular((ACT_SLOTS,)), regular((line,)), regular, regular,
        ],
        compiler_params=pltpu.CompilerParams(
            collective_id=0, has_side_effects=True, vmem_limit_bytes=67043328
        ),
    )(
        cotangent, activations, moment_codes, square_codes,
        moment_scales, square_scales,
    )
    outs = pl.pallas_call(
        apply_kernel,
        out_shape=(
            jax.ShapeDtypeStruct(master_weights.shape, f32),
            jax.ShapeDtypeStruct(moment_codes.shape, bf16),
            jax.ShapeDtypeStruct(square_codes.shape, bf16),
            scale_shape,
            scale_shape,
        ),
        in_specs=[hbm] * 9,
        out_specs=(hbm,) * 5,
        scratch_shapes=[
            pltpu.VMEM((2, 8, LANES), f32),
            pltpu.VMEM(scale_shape.shape, f32),
            pltpu.VMEM(scale_shape.shape, f32),
            pltpu.VMEM(scale_shape.shape, f32),
            pltpu.VMEM(scale_shape.shape, f32),
            pltpu.VMEM((layers, rows, cols), f32),
            pltpu.VMEM((4, layers, rows, LANES), f32),
            pltpu.VMEM((layers, rows, cols), f32),
            pltpu.VMEM((layers, rows, cols), bf16),
            pltpu.VMEM((layers, rows, cols), bf16),
            dma((blocks, 4)), dma((blocks, 3)), dma((5,)), dma((2,)),
        ],
        compiler_params=pltpu.CompilerParams(vmem_limit_bytes=APPLY_VMEM),
    )(
        gradient, master_weights, moment_codes, square_codes, gain,
        moment_scales, square_scales, moment_peak, square_peak,
    )
    return outs[:3] + (outs[3].transpose(0, 2, 1), outs[4].transpose(0, 2, 1))


def fits_factors(activations, cotangent, block_count, mesh_shape):
    count = mesh_shape["dp"]
    line = count // 2
    rows = cotangent.shape[2] // count
    chunks = activations.shape[2] // (2 * LANES)
    aligned = activations.shape[1] % LANES == 0 and activations.shape[2] % (2 * LANES) == 0
    layers, tokens, cols = activations.shape
    aligned = aligned and rows % LANES == 0 and cols % LANES == 0 and block_count == mesh_shape["col"]
    roomy = layers * rows <= tokens and cols <= cotangent.shape[2]
    return aligned and roomy and line >= 3 and 2 * rows == LANES * mesh_shape["col"] and mesh_shape["col"] % 2 == 0 and activations.shape[1] % (8 * SPLITS) == 0 and chunks - NARROW // 2 > line


def local(
    mesh_shape, activations, cotangent, master_weights, moment_codes, square_codes, moment_scales, square_scales
):
    layer_count = activations.shape[0]
    shard_rows = master_weights.shape[1]
    shard_cols = master_weights.shape[2]
    block_count = moment_scales.shape[2]
    if fits_factors(activations, cotangent, block_count, mesh_shape):
        return factor_step(
            mesh_shape, activations, cotangent, master_weights, moment_codes, square_codes,
            moment_scales, square_scales,
        )
    gradient, squares = reduced_gradient(activations, cotangent, mesh_shape)
    total_sq = jnp.sum(squares)
    rms = jnp.sqrt(total_sq / float(LAYERS * KV * D) + norm_eps)
    clip_factor = jnp.minimum(1.0, 1.0 / rms)
    correct_one = 1.0 - beta_one**STEP
    correct_two = 1.0 - beta_two**STEP
    own_block = lax.axis_index("col") * shard_cols // BLOCK
    selector = (jnp.arange(block_count, dtype=jnp.int32) == own_block).astype(jnp.float32)
    outs_weights, outs_mcode, outs_scode, outs_mscale, outs_sscale = ([], [], [], [], [])
    for layer_index in range(layer_count):
        moment_scale = jnp.sum(moment_scales[layer_index] * selector, axis=1)
        square_scale = jnp.sum(square_scales[layer_index] * selector, axis=1)
        old_moment = moment_codes[layer_index].astype(jnp.float32) * moment_scale[:, None]
        old_square = square_codes[layer_index].astype(jnp.float32) * square_scale[:, None]
        grad_now = clip_factor * gradient[layer_index]
        new_moment = beta_one * old_moment + (1.0 - beta_one) * grad_now
        new_square = beta_two * old_square + (1.0 - beta_two) * grad_now * grad_now
        moment_part = jnp.max(jnp.abs(new_moment), axis=1)[:, None] * selector
        square_part = jnp.max(new_square, axis=1)[:, None] * selector
        moment, square, moment_part, square_part = (
            new_moment,
            new_square,
            moment_part,
            square_part,
        )
        moment_max, square_max = lax.pmax((moment_part, square_part), "col")
        moment_div = jnp.sum(moment_max * selector, axis=1)[:, None]
        square_div = jnp.sum(square_max * selector, axis=1)[:, None]
        moment_out = (moment / (moment_div + scale_eps)).astype(jnp.bfloat16)
        square_out = (square / (square_div + scale_eps)).astype(jnp.bfloat16)
        ratio = moment / correct_one / (jnp.sqrt(square / correct_two) + adam_eps)
        weights = master_weights[layer_index]
        results = (weights - learn_rate * (decay_rate * weights + ratio), moment_out, square_out)
        outs_weights.append(results[0])
        outs_mcode.append(results[1])
        outs_scode.append(results[2])
        outs_mscale.append(moment_max)
        outs_sscale.append(square_max)
    return (
        jnp.stack(outs_weights),
        jnp.stack(outs_mcode),
        jnp.stack(outs_scode),
        jnp.stack(outs_mscale),
        jnp.stack(outs_sscale),
    )


def solution(mesh):
    in_specs = (
        P(None, "dp", "col"),
        P(None, "dp", None),
        P(None, "dp", "col"),
        P(None, "dp", "col"),
        P(None, "dp", "col"),
        P(None, "dp", None),
        P(None, "dp", None),
    )
    out_specs = (
        P(None, "dp", "col"),
        P(None, "dp", "col"),
        P(None, "dp", "col"),
        P(None, "dp", None),
        P(None, "dp", None),
    )
    return jax.shard_map(functools.partial(local, dict(mesh.shape)), mesh=mesh, in_specs=in_specs, out_specs=out_specs, check_vma=False)
```
